32 devices in a mesh: dp: 2 (over x), cp: 16 (over z, y, core).
Axes of the slice: x: 2, y: 2, z: 4, core: 2. Of those that a mesh axis runs over, the one named last changes fastest.
Arguments:
- image: bfloat16 [2, 6144, 3072], P('dp', 'cp'), parts along dimension 0
- text: bfloat16 [2, 256, 3072], P('dp'), parts along dimension 0
- cond_vec: bfloat16 [2, 3072], P('dp'), parts along dimension 0
- image_ids: int32 [12288, 3], P(('dp', 'cp')), parts along dimension 0
- img_w_mod: bfloat16 [3072, 18432], replicated
- img_b_mod: bfloat16 [18432], replicated
- img_w_qkv: bfloat16 [3072, 9216], replicated
- img_b_qkv: bfloat16 [9216], replicated
- img_q_gain: bfloat16 [128], replicated
- img_k_gain: bfloat16 [128], replicated
- img_w_proj: bfloat16 [3072, 3072], replicated
- img_b_proj: bfloat16 [3072], replicated
- img_w_fc1: bfloat16 [3072, 12288], replicated
- img_b_fc1: bfloat16 [12288], replicated
- img_w_fc2: bfloat16 [12288, 3072], replicated
- img_b_fc2: bfloat16 [3072], replicated
- txt_w_mod: bfloat16 [3072, 18432], replicated
- txt_b_mod: bfloat16 [18432], replicated
- txt_w_qkv: bfloat16 [3072, 9216], replicated
- txt_b_qkv: bfloat16 [9216], replicated
- txt_q_gain: bfloat16 [128], replicated
- txt_k_gain: bfloat16 [128], replicated
- txt_w_proj: bfloat16 [3072, 3072], replicated
- txt_b_proj: bfloat16 [3072], replicated
- txt_w_fc1: bfloat16 [3072, 12288], replicated
- txt_b_fc1: bfloat16 [12288], replicated
- txt_w_fc2: bfloat16 [12288, 3072], replicated
- txt_b_fc2: bfloat16 [3072], replicated
Outputs:
- output 1: bfloat16 [2, 6144, 3072], P('dp', 'cp'), parts along dimension 0
- output 2: bfloat16 [2, 256, 3072], P('dp'), parts along dimension 0
There are 2 independent parts. The reference program is written for one: setup_inputs(seed, part) draws one part's arguments, and reference() takes and returns one part's arrays. A program takes and returns all parts, laid end to end along the dimension named above; an argument that names none is the same for every part.
All inputs are finite; a program needn't handle non-finite values.
Results may differ from the reference program's by a relative error of at most 0.00561117.
Values are sent between devices in bfloat16 or wider.
A program may use at most 2.75 GiB of HBM per device.

```python
import jax
import jax.numpy as jnp
from jax import lax

BATCH = 1
IMG_LEN = 6144
TXT = 256
D = 3072
FF = 12288
HEADS = 24
HEAD = 128
REGIONS = 32
ROPE_T = HEAD // 8
ROPE_S = (HEAD - ROPE_T) // 2
EPS = 1e-6
THETA = 10000.0
SCALE = HEAD ** -0.5
PARAM_NAMES = ['w_mod', 'b_mod', 'w_qkv', 'b_qkv', 'q_gain', 'k_gain', 'w_proj', 'b_proj', 'w_fc1', 'b_fc1', 'w_fc2', 'b_fc2']


def draw_ids(ids_key):
    key_frame, key_corner, key_offset = jax.random.split(ids_key, 3)
    region_of = (jnp.arange(IMG_LEN) * REGIONS) // IMG_LEN
    frame_ids = jax.random.randint(key_frame, (REGIONS, 1), 0, 4)
    corner_ids = jax.random.randint(key_corner, (REGIONS, 2), 0, 96)
    offsets = jax.random.randint(key_offset, (IMG_LEN, 2), 0, 32)
    grid_ids = corner_ids[region_of] + offsets
    return jnp.concatenate([frame_ids[region_of], grid_ids], axis=1).astype(jnp.int32)


def scaled_normal(sub_key, shape, scale):
    return jax.random.normal(sub_key, shape, jnp.float32) * scale


def draw_branch(branch_key):
    keys = jax.random.split(branch_key, 12)
    drawn = [
        scaled_normal(keys[0], (D, 6 * D), D ** -0.5),
        scaled_normal(keys[1], (6 * D,), 0.4),
        scaled_normal(keys[2], (D, 3 * D), D ** -0.5),
        scaled_normal(keys[3], (3 * D,), 0.4),
        1.0 + scaled_normal(keys[4], (HEAD,), 0.5),
        1.0 + scaled_normal(keys[5], (HEAD,), 0.5),
        scaled_normal(keys[6], (D, D), D ** -0.5),
        scaled_normal(keys[7], (D,), 0.4),
        scaled_normal(keys[8], (D, FF), D ** -0.5),
        scaled_normal(keys[9], (FF,), 0.4),
        scaled_normal(keys[10], (FF, D), FF ** -0.5),
        scaled_normal(keys[11], (D,), 0.4),
    ]
    return [item.astype(jnp.bfloat16) for item in drawn]


def setup_inputs(seed: int = 0, part: int = 0) -> dict:
    part_key = jax.random.fold_in(jax.random.key(seed), part)
    key_field, key_noise, key_text, key_cond, key_ids = jax.random.split(part_key, 5)
    region_of = (jnp.arange(IMG_LEN) * REGIONS) // IMG_LEN
    field = jax.random.normal(key_field, (BATCH, REGIONS, D), jnp.float32)
    noise = jax.random.normal(key_noise, (BATCH, IMG_LEN, D), jnp.float32)
    image = (field[:, region_of, :] + 0.5 * noise).astype(jnp.bfloat16)
    text = jax.random.normal(key_text, (BATCH, TXT, D), jnp.float32).astype(jnp.bfloat16)
    cond_vec = jax.random.normal(key_cond, (BATCH, D), jnp.float32).astype(jnp.bfloat16)
    image_ids = draw_ids(key_ids)
    result = {'image': image, 'text': text, 'cond_vec': cond_vec, 'image_ids': image_ids}
    key_img, key_txt = jax.random.split(jax.random.key(seed + 1))
    for name, value in zip(PARAM_NAMES, draw_branch(key_img)):
        result['img_' + name] = value
    for name, value in zip(PARAM_NAMES, draw_branch(key_txt)):
        result['txt_' + name] = value
    return result


def layer_norm(x):
    mean_x = jnp.mean(x, axis=-1, keepdims=True)
    centered = x - mean_x
    var_x = jnp.mean(centered * centered, axis=-1, keepdims=True)
    return centered * lax.rsqrt(var_x + EPS)


def head_norm(x, gain):
    mean_sq = jnp.mean(x * x, axis=-1, keepdims=True)
    return x * lax.rsqrt(mean_sq + EPS) * gain.astype(jnp.float32)


def rope_angles(pos_ids):
    positions = pos_ids.astype(jnp.float32)
    pieces = []
    for axis_idx, width in enumerate((ROPE_T, ROPE_S, ROPE_S)):
        omega = THETA ** (-jnp.arange(0, width, 2, dtype=jnp.float32) / width)
        pieces.append(positions[:, axis_idx:axis_idx + 1] * omega[None, :])
    return jnp.concatenate(pieces, axis=-1)


def apply_rope(x, cos_a, sin_a):
    pairs = x.reshape(x.shape[:-1] + (x.shape[-1] // 2, 2))
    even = pairs[..., 0]
    odd = pairs[..., 1]
    turned = jnp.stack([cos_a * even - sin_a * odd, sin_a * even + cos_a * odd], axis=-1)
    return turned.reshape(x.shape)


def modulation(cond_act, w_mod, b_mod):
    mod_all = jnp.dot(cond_act, w_mod, preferred_element_type=jnp.float32) + b_mod.astype(jnp.float32)
    return jnp.split(mod_all[:, None, :], 6, axis=-1)


def branch_qkv(x, mod_rows, w_qkv, b_qkv, q_gain, k_gain):
    normed = ((1.0 + mod_rows[1]) * layer_norm(x.astype(jnp.float32)) + mod_rows[0]).astype(jnp.bfloat16)
    qkv_proj = jnp.dot(normed, w_qkv, preferred_element_type=jnp.float32) + b_qkv.astype(jnp.float32)
    qkv_proj = qkv_proj.reshape(x.shape[0], x.shape[1], 3, HEADS, HEAD)
    query = head_norm(qkv_proj[:, :, 0], q_gain)
    keys = head_norm(qkv_proj[:, :, 1], k_gain)
    values = qkv_proj[:, :, 2].astype(jnp.bfloat16)
    return query, keys, values


def branch_out(x, attn_part, mod_rows, w_proj, b_proj, w_fc1, b_fc1, w_fc2, b_fc2):
    proj_out = jnp.dot(attn_part, w_proj, preferred_element_type=jnp.float32) + b_proj.astype(jnp.float32)
    resid_mid = x.astype(jnp.float32) + mod_rows[2] * proj_out
    normed = ((1.0 + mod_rows[4]) * layer_norm(resid_mid) + mod_rows[3]).astype(jnp.bfloat16)
    hidden = jnp.dot(normed, w_fc1, preferred_element_type=jnp.float32) + b_fc1.astype(jnp.float32)
    hidden = jax.nn.gelu(hidden, approximate=True).astype(jnp.bfloat16)
    mlp_out = jnp.dot(hidden, w_fc2, preferred_element_type=jnp.float32) + b_fc2.astype(jnp.float32)
    return (resid_mid + mod_rows[5] * mlp_out).astype(jnp.bfloat16)


def head_attention(operands):
    q_head, k_head, v_head = operands
    scores = jnp.einsum('bqd,bkd->bqk', q_head.astype(jnp.float32), k_head.astype(jnp.float32)) * SCALE
    peak = jnp.max(scores, axis=-1, keepdims=True)
    exp_w = jnp.exp(scores - peak)
    total = jnp.sum(exp_w, axis=-1, keepdims=True)
    out_head = jnp.einsum('bqk,bkd->bqd', exp_w.astype(jnp.bfloat16).astype(jnp.float32), v_head.astype(jnp.float32)) / total
    return out_head.astype(jnp.bfloat16)


def heads_first(tensor):
    return jnp.moveaxis(tensor, 2, 0)


def reference(image, text, cond_vec, image_ids, img_w_mod, img_b_mod, img_w_qkv, img_b_qkv, img_q_gain, img_k_gain, img_w_proj, img_b_proj, img_w_fc1, img_b_fc1, img_w_fc2, img_b_fc2, txt_w_mod, txt_b_mod, txt_w_qkv, txt_b_qkv, txt_q_gain, txt_k_gain, txt_w_proj, txt_b_proj, txt_w_fc1, txt_b_fc1, txt_w_fc2, txt_b_fc2):
    cond_act = jax.nn.silu(cond_vec.astype(jnp.float32)).astype(jnp.bfloat16)
    img_mods = modulation(cond_act, img_w_mod, img_b_mod)
    txt_mods = modulation(cond_act, txt_w_mod, txt_b_mod)
    img_q, img_k, img_v = branch_qkv(image, img_mods, img_w_qkv, img_b_qkv, img_q_gain, img_k_gain)
    txt_q, txt_k, txt_v = branch_qkv(text, txt_mods, txt_w_qkv, txt_b_qkv, txt_q_gain, txt_k_gain)
    angles = rope_angles(image_ids)
    cos_a = jnp.cos(angles)[None, :, None, :]
    sin_a = jnp.sin(angles)[None, :, None, :]
    img_q = apply_rope(img_q, cos_a, sin_a).astype(jnp.bfloat16)
    img_k = apply_rope(img_k, cos_a, sin_a).astype(jnp.bfloat16)
    joint_q = jnp.concatenate([txt_q.astype(jnp.bfloat16), img_q], axis=1)
    joint_k = jnp.concatenate([txt_k.astype(jnp.bfloat16), img_k], axis=1)
    joint_v = jnp.concatenate([txt_v, img_v], axis=1)
    attn_heads = lax.map(head_attention, (heads_first(joint_q), heads_first(joint_k), heads_first(joint_v)))
    attn_out = jnp.moveaxis(attn_heads, 0, 2).reshape(BATCH, TXT + IMG_LEN, D)
    text_out = branch_out(text, attn_out[:, :TXT], txt_mods, txt_w_proj, txt_b_proj, txt_w_fc1, txt_b_fc1, txt_w_fc2, txt_b_fc2)
    image_out = branch_out(image, attn_out[:, TXT:], img_mods, img_w_proj, img_b_proj, img_w_fc1, img_b_fc1, img_w_fc2, img_b_fc2)
    return image_out, text_out
```

```python
import functools

import jax
import jax.numpy as jnp
from jax import lax
from jax.experimental import pallas as pl
from jax.experimental.pallas import tpu as pltpu
from jax.sharding import PartitionSpec as P

EPS = 1e-6
THETA = 10000.0
F32 = jnp.float32
BF16 = jnp.bfloat16
HD = 128
NCHIP = 8
NDEV = 16
VM = pl.BlockSpec(memory_space=pltpu.VMEM)
ANY = pl.BlockSpec(memory_space=pl.ANY)
MESH = pl.DeviceIdType.MESH
VMEM_LIMIT = 67043328


def dot(a, b):
    return jnp.dot(a, b, preferred_element_type=F32)


def dot_t(a, b):
    return lax.dot_general(a, b, (((1,), (1,)), ((), ())), preferred_element_type=F32)


def mod_kernel(cond_ref, wi_hbm, wt_hbm, out_ref, wi, wt, mine, lsem, ssem, rsem):
    me = lax.axis_index("cp")
    cols = wi.shape[1]
    n_row = cols // 128
    base = pl.multiple_of(me * cols, 128)
    ci = pltpu.make_async_copy(wi_hbm.at[:, pl.ds(base, cols)], wi, lsem.at[0])
    ct = pltpu.make_async_copy(wt_hbm.at[:, pl.ds(base, cols)], wt, lsem.at[1])
    ci.start()
    ct.start()
    barrier = pltpu.get_barrier_semaphore()
    for r in range(1, NDEV):
        peer = lax.rem(me + r, NDEV)
        pl.semaphore_signal(barrier, inc=1, device_id={"cp": peer}, device_id_type=MESH)
    c = cond_ref[...].astype(F32)
    act = (c * jax.nn.sigmoid(c)).astype(BF16)
    act = jnp.broadcast_to(act, (16, act.shape[1]))
    mine[...] = jnp.zeros_like(mine)
    ci.wait()
    ri = dot(act, wi[...])
    for i in range(n_row):
        mine[pl.ds(i, 1), :] = ri[0:1, i * 128:(i + 1) * 128]
    ct.wait()
    rt = dot(act, wt[...])
    for i in range(n_row):
        mine[pl.ds(n_row + i, 1), :] = rt[0:1, i * 128:(i + 1) * 128]
    out_ref[me] = mine[...]
    pl.semaphore_wait(barrier, NDEV - 1)
    copies = []
    for r in range(1, NDEV):
        peer = lax.rem(me + r, NDEV)
        cp = pltpu.make_async_remote_copy(
            src_ref=mine, dst_ref=out_ref.at[me], send_sem=ssem.at[r], recv_sem=rsem.at[r],
            device_id={"cp": peer}, device_id_type=MESH)
        cp.start()
        copies.append(cp)
    for cp in copies:
        cp.wait()


def modulation(cond_vec, w_img, w_txt):
    d, total = w_img.shape
    cols = total // NDEV
    n_row = cols // 128
    pad = -(-2 * n_row // 8) * 8
    out = pl.pallas_call(
        mod_kernel,
        out_shape=jax.ShapeDtypeStruct((NDEV, pad, 128), F32),
        in_specs=[VM, ANY, ANY],
        out_specs=VM,
        scratch_shapes=[
            pltpu.VMEM((d, cols), BF16), pltpu.VMEM((d, cols), BF16), pltpu.VMEM((pad, 128), F32),
            pltpu.SemaphoreType.DMA((2,)), pltpu.SemaphoreType.DMA((NDEV,)), pltpu.SemaphoreType.DMA((NDEV,)),
        ],
        compiler_params=pltpu.CompilerParams(collective_id=0, has_side_effects=True, vmem_limit_bytes=32 * 2**20),
        cost_estimate=pl.CostEstimate(flops=4 * d * cols * 16, bytes_accessed=4 * d * cols, transcendentals=0),
        name="mod",
    )(cond_vec, w_img, w_txt)
    img = out[:, :n_row].reshape(total)
    txt = out[:, n_row:2 * n_row].reshape(total)
    return img, txt


def ln_mod_rows(x, scale1p, shift):
    xf = x.astype(F32)
    mean = jnp.mean(xf, axis=-1, keepdims=True)
    cent = xf - mean
    var = jnp.mean(cent * cent, axis=-1, keepdims=True)
    return scale1p * (cent * lax.rsqrt(var + EPS)) + shift


def main_kernel(cfg, x_ref, xt_ref, mi_ref, mt_ref, wi_hbm, wt_hbm, bi_ref, bt_ref, gi_ref, gt_ref,
                cos_ref, se_ref, so_ref, o_hbm, ot_ref,
                u, w, ks, vs, qs, kb, vb, qb, s0, s1, mx0, mx1, ost, otmp,
                wsem, ssem, rsem, fssem, frsem, ossem, orsem):
    tok, txt, d_in, heads, ck = cfg
    hd_all = heads * HD
    nj = heads // NCHIP
    half = tok * NCHIP
    me = lax.axis_index("cp")
    chip, core = me // 2, me % 2
    sib = chip * 2 + (1 - core)

    def dev(c):
        return {"cp": c * 2 + core}

    barrier = pltpu.get_barrier_semaphore()
    for r in range(1, NCHIP):
        pl.semaphore_signal(barrier, inc=1, device_id=dev(lax.rem(chip + r, NCHIP)), device_id_type=MESH)
    pl.semaphore_signal(barrier, inc=1, device_id={"cp": sib}, device_id_type=MESH)

    wide = 4 * HD
    steps = []
    for j in range(nj):
        for kind in (1, 2, 0):
            for hf in range(2):
                steps.append(("img", kind, j, hf))
    for kind in (1, 2, 0):
        steps.append(("txt", kind, 0, 0))
    nslot = w.shape[0]

    def copies_of(n):
        where, kind, j, hf = steps[n]
        slot = n % nslot
        if where == "img":
            off = kind * hd_all + j * NCHIP * HD + hf * wide
            return [pltpu.make_async_copy(wi_hbm.at[:, pl.ds(off, wide)], w.at[slot], wsem.at[slot, 0])]
        out = []
        for jj in range(nj):
            off = pl.multiple_of(kind * hd_all + (jj * NCHIP + chip) * HD, HD)
            out.append(pltpu.make_async_copy(
                wt_hbm.at[:, pl.ds(off, HD)], w.at[slot, :, pl.ds(jj * HD, HD)], wsem.at[slot, jj]))
        return out

    for n in range(nslot - 1):
        for c in copies_of(n):
            c.start()

    rb = 16

    def ln_into(src, dst, m_ref, rows):
        shift = m_ref[0:1, :]
        scale = 1.0 + m_ref[1:2, :]

        def body(i, carry):
            sl = pl.ds(pl.multiple_of(i * rb, rb), rb)
            dst[sl, :] = ln_mod_rows(src[sl, :], scale, shift).astype(BF16)
            return carry
        lax.fori_loop(0, rows // rb, body, 0)

    ln_into(x_ref, u, mi_ref, tok)
    pl.semaphore_wait(barrier, NCHIP)

    def sends(kind, j):
        src, dst = ((qs, qb), (ks, kb), (vs, vb))[kind]
        out = []
        for r in range(1, NCHIP):
            c = lax.rem(chip + r, NCHIP)
            if kind == 0:
                d = dst.at[j, pl.ds(txt + chip * tok, tok)]
            elif kind == 1:
                d = dst.at[j, pl.ds(txt + core * half + chip * tok, tok)]
            else:
                d = dst.at[j, :, pl.ds(pl.multiple_of(txt + core * half + chip * tok, 128), tok)]
            out.append(pltpu.make_async_remote_copy(
                src_ref=src.at[j * NCHIP + c], dst_ref=d, send_sem=ssem.at[kind, j, r], recv_sem=rsem.at[kind, j, r],
                device_id=dev(c), device_id_type=MESH))
        return out

    def norm_rope(y, gain, cos, se, so, rope):
        ms = jnp.mean(y * y, axis=-1, keepdims=True)
        y = y * lax.rsqrt(ms + EPS) * gain
        if rope:
            y = y * cos + pltpu.roll(y, HD - 1, 1) * se + pltpu.roll(y, 1, 1) * so
        return y

    def img_step(n):
        _, kind, j, hf = steps[n]
        slot = n % nslot

        def body(i, carry):
            col = pl.multiple_of(i * 2 * HD, 2 * HD)
            boff = pl.multiple_of(kind * hd_all + j * NCHIP * HD + hf * wide + col, 2 * HD)
            y2 = dot(u[0:tok, :], w[slot, :, pl.ds(col, 2 * HD)])
            y2 = y2 + bi_ref[0:1, pl.ds(boff, 2 * HD)].astype(F32)
            for hh in range(2):
                head = j * NCHIP + hf * 4 + i * 2 + hh
                y = y2[:, hh * HD:(hh + 1) * HD]
                if kind == 2:
                    vs[head] = y.T.astype(BF16)
                else:
                    gain = gi_ref[kind:kind + 1, :].astype(F32)
                    y = norm_rope(y, gain, cos_ref[...], se_ref[...], so_ref[...], True)
                    (qs, ks)[kind][head] = y.astype(BF16)
            return carry
        lax.fori_loop(0, 2, body, 0)

    def txt_step(n):
        _, kind, _, _ = steps[n]
        slot = n % nslot
        y3 = dot(u[0:txt, :], w[slot, :, 0:nj * HD])
        for j in range(nj):
            boff = pl.multiple_of(kind * hd_all + (j * NCHIP + chip) * HD, HD)
            y = y3[:, j * HD:(j + 1) * HD] + bt_ref[0:1, pl.ds(boff, HD)].astype(F32)
            if kind == 2:
                vb[j, :, 0:txt] = y.T.astype(BF16)
            else:
                gain = gt_ref[kind:kind + 1, :].astype(F32)
                y = norm_rope(y, gain, None, None, None, False).astype(BF16)
                (qb, kb)[kind][j, 0:txt] = y

    def own_copy(kind, j):
        src = (qs, ks, vs)[kind]
        v = src[j * NCHIP + chip]
        if kind == 0:
            qb[j, pl.ds(txt + chip * tok, tok)] = v
        elif kind == 1:
            kb[j, pl.ds(txt + core * half + chip * tok, tok)] = v
        else:
            vb[j, :, pl.ds(pl.multiple_of(txt + core * half + chip * tok, 128), tok)] = v

    all_sends = []
    for n in range(len(steps)):
        nxt = n + nslot - 1
        if nxt < len(steps):
            for c in copies_of(nxt):
                c.start()
        for c in copies_of(n):
            c.wait()
        where, kind, j, hf = steps[n]
        if where == "img":
            img_step(n)
            if hf == 1:
                own_copy(kind, j)
                new = sends(kind, j)
                for c in new:
                    c.start()
                all_sends += new
        else:
            if kind == 1:
                ln_into(xt_ref, u, mt_ref, txt)
            txt_step(n)

    scale2 = (HD ** -0.5) * 1.4426950408889634
    keys = txt + 2 * half
    nchunk = keys // ck
    qt = 256
    ntile = (txt + half) // qt
    group = 2 * tok // qt
    ngroup = NCHIP // 2

    def tile_start(t):
        g = (t - 1) // group
        plane = lax.rem(chip // 2 + 1 + g, ngroup)
        row = txt + plane * (2 * tok) + lax.rem(t - 1, group) * qt
        return pl.multiple_of(jnp.where(t == 0, 0, row), 128)

    def qk(j, q, i, s_ref, mx):
        sl = pl.ds(pl.multiple_of(i * ck, ck), ck)
        s = dot_t(kb[j, sl], q)
        s_ref[sl, :] = s
        return jnp.maximum(mx, jnp.max(s.reshape(ck // 8, 8, qt), axis=0))

    def sm(j, i, s_ref, m, lsum, acc):
        sl = pl.ds(pl.multiple_of(i * ck, ck), ck)
        p = jnp.exp2((s_ref[sl, :] - m) * scale2)
        lsum = lsum + jnp.sum(p.reshape(ck // 8, 8, qt), axis=0)
        acc = acc + dot(vb[j, :, sl], p.astype(BF16))
        return lsum, acc

    def new_max():
        return jnp.full((8, qt), -jnp.inf, F32)

    def o_refs(j, c):
        src = ost.at[j, pl.ds(pl.multiple_of(c * tok, 128), tok)]
        dst = o_hbm.at[:, pl.ds(pl.multiple_of((j * NCHIP + chip) * HD, HD), HD)]
        return src, dst

    def o_remote(j, c):
        src, dst = o_refs(j, c)
        return pltpu.make_async_remote_copy(
            src_ref=src, dst_ref=dst, send_sem=ossem.at[j, c], recv_sem=orsem.at[j, chip],
            device_id=dev(c), device_id_type=MESH)

    def o_local(j):
        return pltpu.make_async_copy(*o_refs(j, chip), ossem.at[j, chip])

    def o_send(j, g):
        plane = lax.rem(chip // 2 + 1 + g, ngroup)
        for y in range(2):
            c = plane * 2 + y

            @pl.when(c != chip)
            def _():
                o_remote(j, c).start()

            @pl.when(c == chip)
            def _():
                o_local(j).start()

    def finish(j, t, lsum, acc):
        tot = jnp.sum(lsum, axis=0, keepdims=True)
        o = (acc / tot).T.astype(BF16)

        @pl.when(t == 0)
        def _():
            otmp[...] = o
            ot_ref[j] = otmp[pl.ds(pl.multiple_of(core * (txt // 2), 8), txt // 2), :]

        @pl.when(t > 0)
        def _():
            ost[j, pl.ds(pl.multiple_of(tile_start(t) - txt, 128), qt)] = o

            @pl.when(lax.rem(t, group) == 0)
            def _():
                o_send(j, t // group - 1)

    def pair(j, t, s_cur, mx_cur, s_nxt, mx_nxt, has_next):
        m = jnp.max(mx_cur[...], axis=0, keepdims=True)
        lsum = jnp.zeros((8, qt), F32)
        acc = jnp.zeros((HD, qt), F32)
        if has_next:
            q = qb[j, pl.ds(tile_start(t + 1), qt)]

            def body(i, carry):
                lsum, acc, mx = carry
                mx = qk(j, q, i, s_nxt, mx)
                lsum, acc = sm(j, i, s_cur, m, lsum, acc)
                return lsum, acc, mx
            lsum, acc, mx = lax.fori_loop(0, nchunk, body, (lsum, acc, new_max()))
            mx_nxt[...] = mx
        else:
            def body(i, carry):
                return sm(j, i, s_cur, m, *carry)
            lsum, acc = lax.fori_loop(0, nchunk, body, (lsum, acc))
        finish(j, t, lsum, acc)

    for j in range(nj):
        recv = {kind: sends(kind, j) for kind in (0, 1, 2)}
        fwd = []
        for kind in (1, 2):
            for c in recv[kind]:
                c.wait_recv()
            if kind == 1:
                ref = kb.at[j, pl.ds(txt + core * half, half)]
            else:
                ref = vb.at[j, :, pl.ds(pl.multiple_of(txt + core * half, 128), half)]
            f = pltpu.make_async_remote_copy(
                src_ref=ref, dst_ref=ref, send_sem=fssem.at[kind - 1, j], recv_sem=frsem.at[kind - 1, j],
                device_id={"cp": sib}, device_id_type=MESH)
            f.start()
            fwd.append(f)
        for c in recv[0]:
            c.wait_recv()
        for f in fwd:
            f.wait()

        q = qb[j, 0:qt]

        def first(i, mx):
            return qk(j, q, i, s0, mx)
        mx0[...] = lax.fori_loop(0, nchunk, first, new_max())

        def two(i, carry):
            pair(j, 2 * i, s0, mx0, s1, mx1, True)
            pair(j, 2 * i + 1, s1, mx1, s0, mx0, True)
            return carry
        lax.fori_loop(0, (ntile - 1) // 2, two, 0)
        pair(j, jnp.int32(ntile - 1), s0, mx0, s1, mx1, False)

    for c in all_sends:
        c.wait_send()
    for j in range(nj):
        o_local(j).wait()
        for r in range(1, NCHIP):
            c = lax.rem(chip + r, NCHIP)
            o_remote(j, c).wait_send()
            src, _ = o_refs(j, c)
            arrived = o_hbm.at[:, pl.ds(pl.multiple_of((j * NCHIP + c) * HD, HD), HD)]
            pltpu.make_async_remote_copy(
                src_ref=src, dst_ref=arrived, send_sem=ossem.at[j, c], recv_sem=orsem.at[j, c],
                device_id=dev(c), device_id_type=MESH).wait_recv()


def attention(image, text, m_img, m_txt, w_img, w_txt, b_img, b_txt, g_img, g_txt, cos, se, so):
    tok, d_in = image.shape
    txt = text.shape[0]
    hd_all = w_img.shape[1] // 3
    heads = hd_all // HD
    nj = heads // NCHIP
    half = tok * NCHIP
    keys = txt + 2 * half
    ck = 1280 if keys % 1280 == 0 else 256
    nslot = 3
    cfg = (tok, txt, d_in, heads, ck)
    dma = pltpu.SemaphoreType.DMA
    flops = 2 * tok * d_in * 3 * hd_all + 4 * nj * HD * (half + txt) * keys
    return pl.pallas_call(
        functools.partial(main_kernel, cfg),
        out_shape=(jax.ShapeDtypeStruct((tok, hd_all), BF16), jax.ShapeDtypeStruct((nj, txt // 2, HD), BF16)),
        in_specs=[VM, VM, VM, VM, ANY, ANY] + [VM] * 7,
        out_specs=(ANY, VM),
        scratch_shapes=[
            pltpu.VMEM((max(tok, txt), d_in), BF16),
            pltpu.VMEM((nslot, d_in, 4 * HD), BF16),
            pltpu.VMEM((heads, tok, HD), BF16),
            pltpu.VMEM((heads, HD, tok), BF16),
            pltpu.VMEM((heads, tok, HD), BF16),
            pltpu.VMEM((nj, keys, HD), BF16),
            pltpu.VMEM((nj, HD, keys), BF16),
            pltpu.VMEM((nj, txt + half, HD), BF16),
            pltpu.VMEM((keys, 256), F32),
            pltpu.VMEM((keys, 256), F32),
            pltpu.VMEM((8, 256), F32),
            pltpu.VMEM((8, 256), F32),
            pltpu.VMEM((nj, half, HD), BF16),
            pltpu.VMEM((txt, HD), BF16),
            dma((nslot, nj)), dma((3, nj, NCHIP)), dma((3, nj, NCHIP)), dma((2, nj)), dma((2, nj)),
            dma((nj, NCHIP)), dma((nj, NCHIP)),
        ],
        compiler_params=pltpu.CompilerParams(collective_id=1, has_side_effects=True, vmem_limit_bytes=VMEM_LIMIT),
        cost_estimate=pl.CostEstimate(flops=flops, bytes_accessed=2 * d_in * 3 * hd_all, transcendentals=0),
        name="attn",
    )(image, text, m_img, m_txt, w_img, w_txt, b_img, b_txt, g_img, g_txt, cos, se, so)


def proj_kernel(o_ref, x_ref, m_ref, w_ref, b_ref, h_ref, z_ref):
    i = pl.program_id(0)
    nb = w_ref.shape[1]
    col = pl.multiple_of(i * nb, nb)
    sl = pl.ds(col, nb)
    y = dot(o_ref[...], w_ref[...]) + b_ref[0:1, sl].astype(F32)
    h_ref[:, sl] = x_ref[:, sl].astype(F32) + m_ref[2:3, sl] * y

    @pl.when(i == pl.num_programs(0) - 1)
    def _():
        shift, scale = m_ref[3:4, :], 1.0 + m_ref[4:5, :]
        rb = 16

        def body(k, carry):
            rows = pl.ds(pl.multiple_of(k * rb, rb), rb)
            z_ref[rows, :] = ln_mod_rows(h_ref[rows, :], scale, shift).astype(BF16)
            return carry
        lax.fori_loop(0, h_ref.shape[0] // rb, body, 0)


def out_proj(o, x, mods, w, b):
    tok, d = x.shape
    nb = 512
    full = lambda i: (0, 0)
    return pl.pallas_call(
        proj_kernel,
        grid=(d // nb,),
        out_shape=(jax.ShapeDtypeStruct((tok, d), F32), jax.ShapeDtypeStruct((tok, d), BF16)),
        in_specs=[pl.BlockSpec((tok, o.shape[1]), full), pl.BlockSpec((tok, d), full), pl.BlockSpec(mods.shape, full),
                  pl.BlockSpec((w.shape[0], nb), lambda i: (0, i)), pl.BlockSpec(b.shape, full)],
        out_specs=(pl.BlockSpec((tok, d), full), pl.BlockSpec((tok, d), full)),
        compiler_params=pltpu.CompilerParams(dimension_semantics=("arbitrary",), vmem_limit_bytes=48 * 2**20),
        cost_estimate=pl.CostEstimate(flops=2 * tok * d * d, bytes_accessed=2 * d * d, transcendentals=0),
        name="img_proj",
    )(o, x, mods, w, b)


def gelu(x):
    return 0.5 * x * (1.0 + jnp.tanh(0.7978845608028654 * (x + 0.044715 * (x * x * x))))


def ffn_kernel(last, z_ref, h_ref, m_ref, w1_ref, b1_ref, w2_ref, b2_ref, *rest):
    i = pl.program_id(0)
    n = pl.num_programs(0)
    if last:
        acc_in, out_ref, acc = rest
    else:
        (acc,) = rest
        acc_in = None
    a = dot(z_ref[...], w1_ref[...]) + b1_ref[...].astype(F32)
    a = gelu(a).astype(BF16)

    @pl.when(i == 0)
    def _():
        base = b2_ref[...].astype(F32) if acc_in is None else acc_in[...]
        acc[...] = base + dot(a, w2_ref[...])

    @pl.when(i > 0)
    def _():
        acc[...] += dot(a, w2_ref[...])

    if last:
        @pl.when(i == n - 1)
        def _():
            out_ref[...] = (h_ref[...] + m_ref[5:6, :] * acc[...]).astype(BF16)


def ffn(z, h, mods, w1, b1, w2, b2, lo, hi, acc_in=None):
    tok, d = z.shape
    ff = w1.shape[1]
    nb = 512
    lo, hi = lo // nb, hi // nb
    full = lambda i: (0, 0)
    last = acc_in is not None
    specs = [pl.BlockSpec((tok, d), full), pl.BlockSpec((tok, d), full), pl.BlockSpec(mods.shape, full),
             pl.BlockSpec((d, nb), lambda i: (0, i + lo)), pl.BlockSpec((1, nb), lambda i: (0, i + lo)),
             pl.BlockSpec((nb, d), lambda i: (i + lo, 0)), pl.BlockSpec((1, d), full)]
    args = [z, h, mods, w1, b1, w2, b2]
    if last:
        specs.append(pl.BlockSpec((tok, d), full))
        args.append(acc_in)
    return pl.pallas_call(
        functools.partial(ffn_kernel, last),
        grid=(hi - lo,),
        out_shape=jax.ShapeDtypeStruct((tok, d), BF16 if last else F32),
        in_specs=specs,
        out_specs=pl.BlockSpec((tok, d), full),
        scratch_shapes=[pltpu.VMEM((tok, d), F32)] if last else [],
        compiler_params=pltpu.CompilerParams(dimension_semantics=("arbitrary",), vmem_limit_bytes=VMEM_LIMIT),
        cost_estimate=pl.CostEstimate(flops=4 * tok * d * (hi - lo) * nb, bytes_accessed=4 * d * (hi - lo) * nb,
                                      transcendentals=tok * (hi - lo) * nb),
        name="img_ffn",
    )(*args)


def txt_kernel(og_ref, x_ref, m_ref, wp_hbm, bp_ref, w1_hbm, b1_ref, w2_hbm, h_ref, part_ref,
               o, h, wp, w1, w2, z, a, sem, psem):
    me = lax.axis_index("cp")
    txt, d = x_ref.shape
    fb = w1.shape[1]
    nj = og_ref.shape[1]
    nb = wp.shape[2]
    c1 = pltpu.make_async_copy(w1_hbm.at[:, pl.ds(pl.multiple_of(me * fb, 128), fb)], w1, sem.at[0])
    c2 = pltpu.make_async_copy(w2_hbm.at[pl.ds(pl.multiple_of(me * fb, 128), fb), :], w2, sem.at[1])

    def cp(i, slot):
        return pltpu.make_async_copy(wp_hbm.at[:, pl.ds(pl.multiple_of(i * nb, nb), nb)], wp.at[slot], psem.at[slot])

    nstep = d // nb
    cp(0, 0).start()
    c1.start()
    c2.start()
    rows = txt // 2
    for c in range(NCHIP):
        for k in range(2):
            for j in range(nj):
                o[k * rows:(k + 1) * rows, (j * NCHIP + c) * HD:(j * NCHIP + c + 1) * HD] = og_ref[c * 2 + k, j]

    def body(i, carry):
        slot = lax.rem(i, 2)

        @pl.when(i + 1 < nstep)
        def _():
            cp(i + 1, 1 - slot).start()
        cp(i, slot).wait()
        sl = pl.ds(pl.multiple_of(i * nb, nb), nb)
        y = dot(o[...], wp[slot]) + bp_ref[0:1, sl].astype(F32)
        h[:, sl] = x_ref[:, sl].astype(F32) + m_ref[2:3, sl] * y
        return carry
    lax.fori_loop(0, nstep, body, 0)
    shift, scale = m_ref[3:4, :], 1.0 + m_ref[4:5, :]
    rb = 16

    def lnb(k, carry):
        r = pl.ds(pl.multiple_of(k * rb, rb), rb)
        z[r, :] = ln_mod_rows(h[r, :], scale, shift).astype(BF16)
        return carry
    lax.fori_loop(0, txt // rb, lnb, 0)
    h_ref[...] = h[pl.ds(pl.multiple_of(me * (txt // NDEV), 8), txt // NDEV), :]
    c1.wait()
    y = dot(z[...], w1[...]) + b1_ref[0:1, pl.ds(pl.multiple_of(me * fb, 128), fb)].astype(F32)
    a[...] = gelu(y).astype(BF16)
    c2.wait()

    def fc2(i, carry):
        sl = pl.ds(pl.multiple_of(i * nb, nb), nb)
        part_ref[:, sl] = dot(a[...], w2[:, sl])
        return carry
    lax.fori_loop(0, nstep, fc2, 0)


def text_mlp(og, x, mods, wp, bp, w1, b1, w2):
    txt, d = x.shape
    ff = w1.shape[1]
    fb = ff // NDEV
    nb = 512
    dma = pltpu.SemaphoreType.DMA
    return pl.pallas_call(
        txt_kernel,
        out_shape=(jax.ShapeDtypeStruct((txt // NDEV, d), F32), jax.ShapeDtypeStruct((txt, d), F32)),
        in_specs=[VM, VM, VM, ANY, VM, ANY, VM, ANY],
        out_specs=(VM, VM),
        scratch_shapes=[
            pltpu.VMEM((txt, wp.shape[0]), BF16), pltpu.VMEM((txt, d), F32), pltpu.VMEM((2, wp.shape[0], nb), BF16),
            pltpu.VMEM((d, fb), BF16), pltpu.VMEM((fb, d), BF16), pltpu.VMEM((txt, d), BF16), pltpu.VMEM((txt, fb), BF16),
            dma((2,)), dma((2,)),
        ],
        compiler_params=pltpu.CompilerParams(vmem_limit_bytes=48 * 2**20),
        cost_estimate=pl.CostEstimate(flops=2 * txt * d * (d + 2 * fb), bytes_accessed=2 * d * (d + 2 * fb), transcendentals=0),
        name="txt_mlp",
    )(og, x, mods, wp, bp, w1, b1, w2)


def rope_tables(ids):
    d_t = HD // 8
    d_s = (HD - d_t) // 2
    pos = ids.astype(F32)
    lanes = []
    for axis, width in enumerate((d_t, d_s, d_s)):
        omega = THETA ** (-jnp.arange(0, width, 2, dtype=F32) / width)
        lanes.append(pos[:, axis:axis + 1] * jnp.repeat(omega, 2)[None, :])
    ang = jnp.concatenate(lanes, axis=-1)
    odd = (jnp.arange(HD) % 2).astype(F32)[None, :]
    sin = jnp.sin(ang)
    return jnp.cos(ang), -sin * (1.0 - odd), sin * odd


def device_fn(image, text, cond_vec, image_ids, *weights):
    (wm, bm, wqkv, bqkv, qg, kg, wp, bp, w1, b1, w2, b2) = weights[:12]
    (twm, tbm, twqkv, tbqkv, tqg, tkg, twp, tbp, tw1, tb1, tw2, tb2) = weights[12:]
    x, xt = image[0], text[0]
    d = x.shape[1]
    row = lambda v: v[None, :]
    m_img, m_txt = modulation(cond_vec, wm, twm)
    m_img = (m_img + bm.astype(F32)).reshape(6, d)
    m_txt = (m_txt + tbm.astype(F32)).reshape(6, d)
    cos, se, so = rope_tables(image_ids)
    o_img, o_txt = attention(x, xt, m_img, m_txt, wqkv, twqkv, row(bqkv), row(tbqkv),
                             jnp.stack([qg, kg]), jnp.stack([tqg, tkg]), cos, se, so)
    og = lax.all_gather(o_txt, "cp")
    h, z = out_proj(o_img, x, m_img, wp, row(bp))
    ht, part = text_mlp(og, xt, m_txt, twp, row(tbp), tw1, row(tb1), tw2)
    ff = w1.shape[1]
    acc = ffn(z, h, m_img, w1, row(b1), w2, row(b2), 0, ff // 2)
    red = lax.psum_scatter(part, "cp", scatter_dimension=0, tiled=True)
    rows = (ht + m_txt[5:6] * (red + tb2.astype(F32)[None, :])).astype(BF16)
    text_out = lax.all_gather(rows, "cp", tiled=True)
    image_out = ffn(z, h, m_img, w1, row(b1), w2, row(b2), ff // 2, ff, acc)
    return image_out[None], text_out[None]


def solution(mesh):
    act = P("dp", "cp", None)
    txt = P("dp", None, None)
    in_specs = (act, txt, P("dp", None), P(("dp", "cp"), None)) + (P(),) * 24
    return jax.shard_map(device_fn, mesh=mesh, in_specs=in_specs, out_specs=(act, txt), check_vma=False)
```

```python
import functools

import jax
import jax.numpy as jnp
from jax import lax
from jax.experimental import pallas as pl
from jax.experimental.pallas import tpu as pltpu
from jax.sharding import PartitionSpec as P

EPS = 1e-6
THETA = 10000.0
F32 = jnp.float32
BF16 = jnp.bfloat16
HD = 128
NCHIP = 8
NDEV = 16
VM = pl.BlockSpec(memory_space=pltpu.VMEM)
ANY = pl.BlockSpec(memory_space=pl.ANY)
MESH = pl.DeviceIdType.MESH
VMEM_LIMIT = 67043328


def dot(a, b):
    return jnp.dot(a, b, preferred_element_type=F32)


def dot_t(a, b):
    return lax.dot_general(a, b, (((1,), (1,)), ((), ())), preferred_element_type=F32)


def mod_kernel(cond_ref, wi_hbm, wt_hbm, out_ref, wi, wt, mine, lsem, ssem, rsem):
    me = lax.axis_index("cp")
    cols = wi.shape[1]
    n_row = cols // 128
    base = pl.multiple_of(me * cols, 128)
    ci = pltpu.make_async_copy(wi_hbm.at[:, pl.ds(base, cols)], wi, lsem.at[0])
    ct = pltpu.make_async_copy(wt_hbm.at[:, pl.ds(base, cols)], wt, lsem.at[1])
    ci.start()
    ct.start()
    barrier = pltpu.get_barrier_semaphore()
    for r in range(1, NDEV):
        peer = lax.rem(me + r, NDEV)
        pl.semaphore_signal(barrier, inc=1, device_id={"cp": peer}, device_id_type=MESH)
    c = cond_ref[...].astype(F32)
    act = (c * jax.nn.sigmoid(c)).astype(BF16)
    act = jnp.broadcast_to(act, (16, act.shape[1]))
    mine[...] = jnp.zeros_like(mine)
    ci.wait()
    ri = dot(act, wi[...])
    for i in range(n_row):
        mine[pl.ds(i, 1), :] = ri[0:1, i * 128:(i + 1) * 128]
    ct.wait()
    rt = dot(act, wt[...])
    for i in range(n_row):
        mine[pl.ds(n_row + i, 1), :] = rt[0:1, i * 128:(i + 1) * 128]
    out_ref[me] = mine[...]
    pl.semaphore_wait(barrier, NDEV - 1)
    copies = []
    for r in range(1, NDEV):
        peer = lax.rem(me + r, NDEV)
        cp = pltpu.make_async_remote_copy(
            src_ref=mine, dst_ref=out_ref.at[me], send_sem=ssem.at[r], recv_sem=rsem.at[r],
            device_id={"cp": peer}, device_id_type=MESH)
        cp.start()
        copies.append(cp)
    for cp in copies:
        cp.wait()


def modulation(cond_vec, w_img, w_txt):
    d, total = w_img.shape
    cols = total // NDEV
    n_row = cols // 128
    pad = -(-2 * n_row // 8) * 8
    out = pl.pallas_call(
        mod_kernel,
        out_shape=jax.ShapeDtypeStruct((NDEV, pad, 128), F32),
        in_specs=[VM, ANY, ANY],
        out_specs=VM,
        scratch_shapes=[
            pltpu.VMEM((d, cols), BF16), pltpu.VMEM((d, cols), BF16), pltpu.VMEM((pad, 128), F32),
            pltpu.SemaphoreType.DMA((2,)), pltpu.SemaphoreType.DMA((NDEV,)), pltpu.SemaphoreType.DMA((NDEV,)),
        ],
        compiler_params=pltpu.CompilerParams(collective_id=0, has_side_effects=True, vmem_limit_bytes=32 * 2**20),
        cost_estimate=pl.CostEstimate(flops=4 * d * cols * 16, bytes_accessed=4 * d * cols, transcendentals=0),
        name="mod",
    )(cond_vec, w_img, w_txt)
    img = out[:, :n_row].reshape(total)
    txt = out[:, n_row:2 * n_row].reshape(total)
    return img, txt


def ln_mod_rows(x, scale1p, shift):
    xf = x.astype(F32)
    mean = jnp.mean(xf, axis=-1, keepdims=True)
    cent = xf - mean
    var = jnp.mean(cent * cent, axis=-1, keepdims=True)
    return scale1p * (cent * lax.rsqrt(var + EPS)) + shift


def main_kernel(cfg, x_ref, xt_ref, mi_ref, mt_ref, wi_hbm, wt_hbm, bi_ref, bt_ref, gi_ref, gt_ref,
                cos_ref, se_ref, so_ref, o_hbm, ot_ref,
                u, w, ks, vs, qs, kb, vb, qb, s0, s1, mx0, mx1, ost, otmp,
                wsem, ssem, rsem, fssem, frsem, ossem, orsem):
    tok, txt, d_in, heads, ck = cfg
    hd_all = heads * HD
    nj = heads // NCHIP
    half = tok * NCHIP
    me = lax.axis_index("cp")
    chip, core = me // 2, me % 2
    sib = chip * 2 + (1 - core)

    def dev(c):
        return {"cp": c * 2 + core}

    barrier = pltpu.get_barrier_semaphore()
    for r in range(1, NCHIP):
        pl.semaphore_signal(barrier, inc=1, device_id=dev(lax.rem(chip + r, NCHIP)), device_id_type=MESH)
    pl.semaphore_signal(barrier, inc=1, device_id={"cp": sib}, device_id_type=MESH)

    wide = 4 * HD
    steps = []
    for j in range(nj):
        for kind in (1, 2, 0):
            for hf in range(2):
                steps.append(("img", kind, j, hf))
    for kind in (1, 2, 0):
        steps.append(("txt", kind, 0, 0))
    nslot = w.shape[0]

    def copies_of(n):
        where, kind, j, hf = steps[n]
        slot = n % nslot
        if where == "img":
            off = kind * hd_all + j * NCHIP * HD + hf * wide
            return [pltpu.make_async_copy(wi_hbm.at[:, pl.ds(off, wide)], w.at[slot], wsem.at[slot, 0])]
        out = []
        for jj in range(nj):
            off = pl.multiple_of(kind * hd_all + (jj * NCHIP + chip) * HD, HD)
            out.append(pltpu.make_async_copy(
                wt_hbm.at[:, pl.ds(off, HD)], w.at[slot, :, pl.ds(jj * HD, HD)], wsem.at[slot, jj]))
        return out

    for n in range(nslot - 1):
        for c in copies_of(n):
            c.start()

    rb = 16

    def ln_into(src, dst, m_ref, rows):
        shift = m_ref[0:1, :]
        scale = 1.0 + m_ref[1:2, :]

        def body(i, carry):
            sl = pl.ds(pl.multiple_of(i * rb, rb), rb)
            dst[sl, :] = ln_mod_rows(src[sl, :], scale, shift).astype(BF16)
            return carry
        lax.fori_loop(0, rows // rb, body, 0)

    ln_into(x_ref, u, mi_ref, tok)
    pl.semaphore_wait(barrier, NCHIP)

    def sends(kind, j):
        src, dst = ((qs, qb), (ks, kb), (vs, vb))[kind]
        out = []
        for r in range(1, NCHIP):
            c = lax.rem(chip + r, NCHIP)
            if kind == 0:
                d = dst.at[j, pl.ds(txt + chip * tok, tok)]
            elif kind == 1:
                d = dst.at[j, pl.ds(txt + core * half + chip * tok, tok)]
            else:
                d = dst.at[j, :, pl.ds(pl.multiple_of(txt + core * half + chip * tok, 128), tok)]
            out.append(pltpu.make_async_remote_copy(
                src_ref=src.at[j * NCHIP + c], dst_ref=d, send_sem=ssem.at[kind, j, r], recv_sem=rsem.at[kind, j, r],
                device_id=dev(c), device_id_type=MESH))
        return out

    def norm_rope(y, gain, cos, se, so, rope):
        ms = jnp.mean(y * y, axis=-1, keepdims=True)
        y = y * lax.rsqrt(ms + EPS) * gain
        if rope:
            y = y * cos + pltpu.roll(y, HD - 1, 1) * se + pltpu.roll(y, 1, 1) * so
        return y

    def img_step(n):
        _, kind, j, hf = steps[n]
        slot = n % nslot

        def body(i, carry):
            col = pl.multiple_of(i * 2 * HD, 2 * HD)
            boff = pl.multiple_of(kind * hd_all + j * NCHIP * HD + hf * wide + col, 2 * HD)
            y2 = dot(u[0:tok, :], w[slot, :, pl.ds(col, 2 * HD)])
            y2 = y2 + bi_ref[0:1, pl.ds(boff, 2 * HD)].astype(F32)
            for hh in range(2):
                head = j * NCHIP + hf * 4 + i * 2 + hh
                y = y2[:, hh * HD:(hh + 1) * HD]
                if kind == 2:
                    vs[head] = y.T.astype(BF16)
                else:
                    gain = gi_ref[kind:kind + 1, :].astype(F32)
                    y = norm_rope(y, gain, cos_ref[...], se_ref[...], so_ref[...], True)
                    (qs, ks)[kind][head] = y.astype(BF16)
            return carry
        lax.fori_loop(0, 2, body, 0)

    def txt_step(n):
        _, kind, _, _ = steps[n]
        slot = n % nslot
        y3 = dot(u[0:txt, :], w[slot, :, 0:nj * HD])
        for j in range(nj):
            boff = pl.multiple_of(kind * hd_all + (j * NCHIP + chip) * HD, HD)
            y = y3[:, j * HD:(j + 1) * HD] + bt_ref[0:1, pl.ds(boff, HD)].astype(F32)
            if kind == 2:
                vb[j, :, 0:txt] = y.T.astype(BF16)
            else:
                gain = gt_ref[kind:kind + 1, :].astype(F32)
                y = norm_rope(y, gain, None, None, None, False).astype(BF16)
                (qb, kb)[kind][j, 0:txt] = y

    def own_copy(kind, j):
        src = (qs, ks, vs)[kind]
        v = src[j * NCHIP + chip]
        if kind == 0:
            qb[j, pl.ds(txt + chip * tok, tok)] = v
        elif kind == 1:
            kb[j, pl.ds(txt + core * half + chip * tok, tok)] = v
        else:
            vb[j, :, pl.ds(pl.multiple_of(txt + core * half + chip * tok, 128), tok)] = v

    all_sends = []
    for n in range(len(steps)):
        nxt = n + nslot - 1
        if nxt < len(steps):
            for c in copies_of(nxt):
                c.start()
        for c in copies_of(n):
            c.wait()
        where, kind, j, hf = steps[n]
        if where == "img":
            img_step(n)
            if hf == 1:
                own_copy(kind, j)
                new = sends(kind, j)
                for c in new:
                    c.start()
                all_sends += new
        else:
            if kind == 1:
                ln_into(xt_ref, u, mt_ref, txt)
            txt_step(n)

    scale2 = (HD ** -0.5) * 1.4426950408889634
    keys = txt + 2 * half
    nchunk = keys // ck
    qt = 256
    ntile = (txt + half) // qt
    group = 2 * tok // qt
    ngroup = NCHIP // 2

    def tile_start(t):
        g = (t - 1) // group
        plane = lax.rem(chip // 2 + 1 + g, ngroup)
        row = txt + plane * (2 * tok) + lax.rem(t - 1, group) * qt
        return pl.multiple_of(jnp.where(t == 0, 0, row), 128)

    def qk(j, q, i, s_ref, mx):
        sl = pl.ds(pl.multiple_of(i * ck, ck), ck)
        s = dot_t(kb[j, sl], q)
        s_ref[sl, :] = s
        return jnp.maximum(mx, jnp.max(s.reshape(ck // 8, 8, qt), axis=0))

    def sm(j, i, s_ref, m, lsum, acc):
        sl = pl.ds(pl.multiple_of(i * ck, ck), ck)
        p = jnp.exp2((s_ref[sl, :] - m) * scale2)
        lsum = lsum + jnp.sum(p.reshape(ck // 8, 8, qt), axis=0)
        acc = acc + dot(vb[j, :, sl], p.astype(BF16))
        return lsum, acc

    def new_max():
        return jnp.full((8, qt), -jnp.inf, F32)

    def o_refs(j, c):
        src = ost.at[j, pl.ds(pl.multiple_of(c * tok, 128), tok)]
        dst = o_hbm.at[:, pl.ds(pl.multiple_of((j * NCHIP + chip) * HD, HD), HD)]
        return src, dst

    def o_remote(j, c):
        src, dst = o_refs(j, c)
        return pltpu.make_async_remote_copy(
            src_ref=src, dst_ref=dst, send_sem=ossem.at[j, c], recv_sem=orsem.at[j, chip],
            device_id=dev(c), device_id_type=MESH)

    def o_local(j):
        return pltpu.make_async_copy(*o_refs(j, chip), ossem.at[j, chip])

    def o_send(j, g):
        plane = lax.rem(chip // 2 + 1 + g, ngroup)
        for y in range(2):
            c = plane * 2 + y

            @pl.when(c != chip)
            def _():
                o_remote(j, c).start()

            @pl.when(c == chip)
            def _():
                o_local(j).start()

    def finish(j, t, lsum, acc):
        tot = jnp.sum(lsum, axis=0, keepdims=True)
        o = (acc / tot).T.astype(BF16)

        @pl.when(t == 0)
        def _():
            otmp[...] = o
            ot_ref[j] = otmp[pl.ds(pl.multiple_of(core * (txt // 2), 8), txt // 2), :]

        @pl.when(t > 0)
        def _():
            ost[j, pl.ds(pl.multiple_of(tile_start(t) - txt, 128), qt)] = o

            @pl.when(lax.rem(t, group) == 0)
            def _():
                o_send(j, t // group - 1)

    def pair(j, t, s_cur, mx_cur, s_nxt, mx_nxt, has_next):
        m = jnp.max(mx_cur[...], axis=0, keepdims=True)
        lsum = jnp.zeros((8, qt), F32)
        acc = jnp.zeros((HD, qt), F32)
        if has_next:
            q = qb[j, pl.ds(tile_start(t + 1), qt)]

            def body(i, carry):
                lsum, acc, mx = carry
                mx = qk(j, q, i, s_nxt, mx)
                lsum, acc = sm(j, i, s_cur, m, lsum, acc)
                return lsum, acc, mx
            lsum, acc, mx = lax.fori_loop(0, nchunk, body, (lsum, acc, new_max()))
            mx_nxt[...] = mx
        else:
            def body(i, carry):
                return sm(j, i, s_cur, m, *carry)
            lsum, acc = lax.fori_loop(0, nchunk, body, (lsum, acc))
        finish(j, t, lsum, acc)

    for j in range(nj):
        recv = {kind: sends(kind, j) for kind in (0, 1, 2)}
        fwd = []
        for kind in (1, 2):
            for c in recv[kind]:
                c.wait_recv()
            if kind == 1:
                ref = kb.at[j, pl.ds(txt + core * half, half)]
            else:
                ref = vb.at[j, :, pl.ds(pl.multiple_of(txt + core * half, 128), half)]
            f = pltpu.make_async_remote_copy(
                src_ref=ref, dst_ref=ref, send_sem=fssem.at[kind - 1, j], recv_sem=frsem.at[kind - 1, j],
                device_id={"cp": sib}, device_id_type=MESH)
            f.start()
            fwd.append(f)
        for c in recv[0]:
            c.wait_recv()
        for f in fwd:
            f.wait()

        q = qb[j, 0:qt]

        def first(i, mx):
            return qk(j, q, i, s0, mx)
        mx0[...] = lax.fori_loop(0, nchunk, first, new_max())

        def two(i, carry):
            pair(j, 2 * i, s0, mx0, s1, mx1, True)
            pair(j, 2 * i + 1, s1, mx1, s0, mx0, True)
            return carry
        lax.fori_loop(0, (ntile - 1) // 2, two, 0)
        pair(j, jnp.int32(ntile - 1), s0, mx0, s1, mx1, False)

    for c in all_sends:
        c.wait_send()
    for j in range(nj):
        o_local(j).wait()
        for r in range(1, NCHIP):
            c = lax.rem(chip + r, NCHIP)
            o_remote(j, c).wait_send()
            src, _ = o_refs(j, c)
            arrived = o_hbm.at[:, pl.ds(pl.multiple_of((j * NCHIP + c) * HD, HD), HD)]
            pltpu.make_async_remote_copy(
                src_ref=src, dst_ref=arrived, send_sem=ossem.at[j, c], recv_sem=orsem.at[j, c],
                device_id=dev(c), device_id_type=MESH).wait_recv()


def attention(image, text, m_img, m_txt, w_img, w_txt, b_img, b_txt, g_img, g_txt, cos, se, so):
    tok, d_in = image.shape
    txt = text.shape[0]
    hd_all = w_img.shape[1] // 3
    heads = hd_all // HD
    nj = heads // NCHIP
    half = tok * NCHIP
    keys = txt + 2 * half
    ck = 1280 if keys % 1280 == 0 else 256
    nslot = 3
    cfg = (tok, txt, d_in, heads, ck)
    dma = pltpu.SemaphoreType.DMA
    flops = 2 * tok * d_in * 3 * hd_all + 4 * nj * HD * (half + txt) * keys
    return pl.pallas_call(
        functools.partial(main_kernel, cfg),
        out_shape=(jax.ShapeDtypeStruct((tok, hd_all), BF16), jax.ShapeDtypeStruct((nj, txt // 2, HD), BF16)),
        in_specs=[VM, VM, VM, VM, ANY, ANY] + [VM] * 7,
        out_specs=(ANY, VM),
        scratch_shapes=[
            pltpu.VMEM((max(tok, txt), d_in), BF16),
            pltpu.VMEM((nslot, d_in, 4 * HD), BF16),
            pltpu.VMEM((heads, tok, HD), BF16),
            pltpu.VMEM((heads, HD, tok), BF16),
            pltpu.VMEM((heads, tok, HD), BF16),
            pltpu.VMEM((nj, keys, HD), BF16),
            pltpu.VMEM((nj, HD, keys), BF16),
            pltpu.VMEM((nj, txt + half, HD), BF16),
            pltpu.VMEM((keys, 256), F32),
            pltpu.VMEM((keys, 256), F32),
            pltpu.VMEM((8, 256), F32),
            pltpu.VMEM((8, 256), F32),
            pltpu.VMEM((nj, half, HD), BF16),
            pltpu.VMEM((txt, HD), BF16),
            dma((nslot, nj)), dma((3, nj, NCHIP)), dma((3, nj, NCHIP)), dma((2, nj)), dma((2, nj)),
            dma((nj, NCHIP)), dma((nj, NCHIP)),
        ],
        compiler_params=pltpu.CompilerParams(collective_id=1, has_side_effects=True, vmem_limit_bytes=VMEM_LIMIT),
        cost_estimate=pl.CostEstimate(flops=flops, bytes_accessed=2 * d_in * 3 * hd_all, transcendentals=0),
        name="attn",
    )(image, text, m_img, m_txt, w_img, w_txt, b_img, b_txt, g_img, g_txt, cos, se, so)


def gelu(x):
    return x * (0.5 * (1.0 + jnp.tanh(0.7978845608028654 * (x + 0.044715 * (x * x * x)))))


def out_kernel(cfg, o_hbm, x_hbm, xt_hbm, ot_ref, mi_ref, mt_ref, wp_hbm, w1_hbm, w2_hbm, twp_hbm, tw1_hbm, tw2_hbm,
               bp_ref, b1_ref, b2_ref, tbp_ref, tb1_ref, tb2_ref, out_ref, tout_ref,
               wa, wb, o, x, h, z, acc, a0, a1, o_t, x_t, h_t, z_t, a_t, part, rs, row,
               asem, bsem, lsem, ossem, orsem, pssem, prsem, rssem, rrsem, fssem, frsem):
    tok, txt, d, ff, s1, s2 = cfg
    me = lax.axis_index("cp")
    chip, core = me // 2, me % 2
    sib = chip * 2 + (1 - core)
    rows = txt // 2
    piece = rows // NCHIP
    nb = wa.shape[2]
    na = wa.shape[0]
    np_ = d // nb
    nf = ff // nb
    ft = ff // NCHIP
    nt = ft // nb
    nj = ot_ref.shape[0]

    def dev(c):
        return {"cp": c * 2 + core}

    off = pl.multiple_of(chip * ft, nb)
    segs_a = ((np_, wp_hbm, 0), (s1, w1_hbm, 0), (np_, twp_hbm, 0), (nt, tw1_hbm, off), (nf - s1, w1_hbm, s1 * nb))
    segs_b = ((s1, w2_hbm, 0), (nt, tw2_hbm, off), (nf - s1, w2_hbm, s1 * nb))

    def start(p, segs, is_a):
        lo = 0
        for n, ref, base in segs:
            @pl.when((p >= lo) & (p < lo + n))
            def _(lo=lo, ref=ref, base=base):
                sl = pl.ds(pl.multiple_of(base + (p - lo) * nb, nb), nb)
                slot = lax.rem(p, na)
                if is_a:
                    pltpu.make_async_copy(ref.at[:, sl], wa.at[slot], asem.at[slot]).start()
                else:
                    pltpu.make_async_copy(ref.at[sl, :], wb.at[slot], bsem.at[slot]).start()
            lo += n

    def get_a(p):
        start(p + na - 1, segs_a, True)
        slot = lax.rem(p, na)
        pltpu.make_async_copy(w1_hbm.at[:, 0:nb], wa.at[slot], asem.at[slot]).wait()
        return slot

    def get_b(p):
        start(p + na - 1, segs_b, False)
        slot = lax.rem(p, na)
        pltpu.make_async_copy(w2_hbm.at[0:nb, :], wb.at[slot], bsem.at[slot]).wait()
        return slot

    load_o = pltpu.make_async_copy(o_hbm, o, lsem.at[0])
    load_x = pltpu.make_async_copy(x_hbm, x, lsem.at[1])
    load_t = pltpu.make_async_copy(xt_hbm.at[pl.ds(pl.multiple_of(core * rows, 8), rows), :], x_t, lsem.at[2])
    load_o.start()
    start(jnp.int32(0), segs_a, True)
    load_x.start()
    for p in range(1, na - 1):
        start(jnp.int32(p), segs_a, True)
    for p in range(na - 1):
        start(jnp.int32(p), segs_b, False)
    load_t.start()

    barrier = pltpu.get_barrier_semaphore()
    for r in range(1, NCHIP):
        pl.semaphore_signal(barrier, inc=1, device_id=dev(lax.rem(chip + r, NCHIP)), device_id_type=MESH)
    pl.semaphore_signal(barrier, inc=1, device_id={"cp": sib}, device_id_type=MESH)
    pl.semaphore_wait(barrier, NCHIP)

    def o_copy(j, r, c_src, c_dst):
        return pltpu.make_async_remote_copy(
            src_ref=ot_ref.at[j], dst_ref=o_t.at[:, pl.ds(pl.multiple_of((j * NCHIP + c_src) * HD, HD), HD)],
            send_sem=ossem.at[j, r], recv_sem=orsem.at[j, r], device_id=dev(c_dst), device_id_type=MESH)

    for j in range(nj):
        for r in range(1, NCHIP):
            o_copy(j, r, chip, lax.rem(chip + r, NCHIP)).start()
        o_t[:, pl.ds(pl.multiple_of((j * NCHIP + chip) * HD, HD), HD)] = ot_ref[j]

    load_o.wait()
    load_x.wait()

    def proj(p, carry):
        slot = get_a(p)
        sl = pl.ds(pl.multiple_of(p * nb, nb), nb)
        y = dot(o[...], wa[slot]) + bp_ref[0:1, sl].astype(F32)
        h[:, sl] = x[:, sl].astype(F32) + mi_ref[2:3, sl] * y
        return carry
    lax.fori_loop(0, np_, proj, 0)

    def ln2(src, dst, m_ref, n):
        shift, scale = m_ref[3:4, :], 1.0 + m_ref[4:5, :]
        rb = 16

        def body(i, carry):
            r = pl.ds(pl.multiple_of(i * rb, rb), rb)
            dst[r, :] = ln_mod_rows(src[r, :], scale, shift).astype(BF16)
            return carry
        lax.fori_loop(0, n // rb, body, 0)

    ln2(h, z, mi_ref, tok)
    acc[...] = jnp.broadcast_to(b2_ref[...].astype(F32), acc.shape)

    def mlp(i, pa, pb, a_new, a_old):
        slot_b = get_b(pb)
        slot_a = get_a(pa)
        sl = pl.ds(pl.multiple_of(i * nb, nb), nb)
        a_new[...] = gelu(dot(z[...], wa[slot_a]) + b1_ref[0:1, sl].astype(F32)).astype(BF16)
        acc[...] += dot(a_old[...], wb[slot_b])

    def mlp_range(lo, hi, da, db):
        def two(k, carry):
            i = lo + 2 * k
            mlp(i, i + da, i - 1 + db, a1, a0)
            mlp(i + 1, i + 1 + da, i + db, a0, a1)
            return carry
        lax.fori_loop(0, (hi - lo) // 2, two, 0)

    slot = get_a(jnp.int32(np_))
    a0[...] = gelu(dot(z[...], wa[slot]) + b1_ref[0:1, 0:nb].astype(F32)).astype(BF16)
    mlp_range(1, s1, np_, 0)
    slot = get_b(jnp.int32(s1 - 1))
    acc[...] += dot(a0[...], wb[slot])

    load_t.wait()
    for j in range(nj):
        for r in range(1, NCHIP):
            o_copy(j, r, lax.rem(chip + NCHIP - r, NCHIP), chip).wait_recv()
    pa = np_ + s1

    def tproj(k, carry):
        slot = get_a(pa + k)
        sl = pl.ds(pl.multiple_of(k * nb, nb), nb)
        y = dot(o_t[...], wa[slot]) + tbp_ref[0:1, sl].astype(F32)
        h_t[:, sl] = x_t[:, sl].astype(F32) + mt_ref[2:3, sl] * y
        return carry
    lax.fori_loop(0, np_, tproj, 0)
    ln2(h_t, z_t, mt_ref, rows)

    for k in range(nt):
        slot = get_a(jnp.int32(pa + np_ + k))
        y = dot(z_t[...], wa[slot]) + tb1_ref[0:1, pl.ds(pl.multiple_of(off + k * nb, nb), nb)].astype(F32)
        a_t[:, k * nb:(k + 1) * nb] = gelu(y).astype(BF16)
    for k in range(nt):
        slot = get_b(jnp.int32(s1 + k))
        y = dot(a_t[:, k * nb:(k + 1) * nb], wb[slot])
        part[...] = y if k == 0 else part[...] + y

    def p_copy(r, c_src, c_dst):
        return pltpu.make_async_remote_copy(
            src_ref=part.at[pl.ds(pl.multiple_of(c_dst * piece, 8), piece), :], dst_ref=rs.at[c_src],
            send_sem=pssem.at[r], recv_sem=prsem.at[r], device_id=dev(c_dst), device_id_type=MESH)

    for r in range(1, NCHIP):
        p_copy(r, chip, lax.rem(chip + r, NCHIP)).start()
    mine = pl.ds(pl.multiple_of(chip * piece, 8), piece)
    rs[chip] = part[mine, :]

    da, db = np_ + np_ + nt, nt
    slot = get_a(jnp.int32(s1 + da))
    sl = slice(s1 * nb, (s1 + 1) * nb)
    a0[...] = gelu(dot(z[...], wa[slot]) + b1_ref[0:1, sl].astype(F32)).astype(BF16)
    mlp_range(s1 + 1, s2, da, db)

    for r in range(1, NCHIP):
        p_copy(r, lax.rem(chip + NCHIP - r, NCHIP), chip).wait_recv()
    tot = rs[0]
    for c in range(1, NCHIP):
        tot = tot + rs[c]
    y = h_t[mine, :] + mt_ref[5:6, :] * (tot + tb2_ref[...].astype(F32))
    row[...] = y.astype(BF16)

    def r_copy(r, c_src, c_dst):
        return pltpu.make_async_remote_copy(
            src_ref=row, dst_ref=tout_ref.at[pl.ds(pl.multiple_of(core * rows + c_src * piece, 8), piece), :],
            send_sem=rssem.at[r], recv_sem=rrsem.at[r], device_id=dev(c_dst), device_id_type=MESH)

    for r in range(1, NCHIP):
        r_copy(r, chip, lax.rem(chip + r, NCHIP)).start()
    tout_ref[pl.ds(pl.multiple_of(core * rows + chip * piece, 8), piece), :] = row[...]

    mlp_range(s2, nf, da, db)

    for r in range(1, NCHIP):
        r_copy(r, lax.rem(chip + NCHIP - r, NCHIP), chip).wait_recv()
    ref = tout_ref.at[pl.ds(pl.multiple_of(core * rows, 8), rows), :]
    fwd = pltpu.make_async_remote_copy(src_ref=ref, dst_ref=ref, send_sem=fssem, recv_sem=frsem,
                                       device_id={"cp": sib}, device_id_type=MESH)
    fwd.start()

    slot = get_b(jnp.int32(nf - 1 + db))
    y = acc[...] + dot((a0 if (nf - 1 - s1) % 2 == 0 else a1)[...], wb[slot])
    out_ref[...] = (h[...] + mi_ref[5:6, :] * y).astype(BF16)

    fwd.wait()
    for j in range(nj):
        for r in range(1, NCHIP):
            o_copy(j, r, chip, lax.rem(chip + r, NCHIP)).wait_send()
    for r in range(1, NCHIP):
        c = lax.rem(chip + r, NCHIP)
        p_copy(r, chip, c).wait_send()
        r_copy(r, chip, c).wait_send()


def output(o_img, image, text, o_txt, m_img, m_txt, wp, w1, w2, twp, tw1, tw2, *biases):
    tok, d = image.shape
    txt = text.shape[0]
    ff = w1.shape[1]
    nb = 512
    nf = ff // nb
    s1 = 3 if nf > 8 else 1
    s2 = 18 if nf > 8 else 4
    na = 3
    rows = txt // 2
    ft = ff // NCHIP
    nj = o_txt.shape[0]
    dma = pltpu.SemaphoreType.DMA
    flops = 2 * tok * d * (d + 2 * ff) + 2 * rows * d * (d + 2 * ft)
    return pl.pallas_call(
        functools.partial(out_kernel, (tok, txt, d, ff, s1, s2)),
        out_shape=(jax.ShapeDtypeStruct((tok, d), BF16), jax.ShapeDtypeStruct((txt, d), BF16)),
        in_specs=[ANY, ANY, ANY, VM, VM, VM] + [ANY] * 6 + [VM] * 6,
        out_specs=(VM, VM),
        scratch_shapes=[
            pltpu.VMEM((na, d, nb), BF16), pltpu.VMEM((na, nb, d), BF16),
            pltpu.VMEM((tok, d), BF16), pltpu.VMEM((tok, d), BF16), pltpu.VMEM((tok, d), F32), pltpu.VMEM((tok, d), BF16),
            pltpu.VMEM((tok, d), F32), pltpu.VMEM((tok, nb), BF16), pltpu.VMEM((tok, nb), BF16),
            pltpu.VMEM((rows, d), BF16), pltpu.VMEM((rows, d), BF16), pltpu.VMEM((rows, d), F32), pltpu.VMEM((rows, d), BF16),
            pltpu.VMEM((rows, ft), BF16), pltpu.VMEM((rows, d), F32), pltpu.VMEM((NCHIP, rows // NCHIP, d), F32),
            pltpu.VMEM((rows // NCHIP, d), BF16),
            dma((na,)), dma((na,)), dma((3,)), dma((nj, NCHIP)), dma((nj, NCHIP)), dma((NCHIP,)), dma((NCHIP,)),
            dma((NCHIP,)), dma((NCHIP,)), dma, dma,
        ],
        compiler_params=pltpu.CompilerParams(collective_id=2, has_side_effects=True, vmem_limit_bytes=VMEM_LIMIT),
        cost_estimate=pl.CostEstimate(flops=flops, bytes_accessed=2 * d * (d + 2 * ff), transcendentals=0),
        name="out",
    )(o_img, image, text, o_txt, m_img, m_txt, wp, w1, w2, twp, tw1, tw2, *biases)


def rope_tables(ids):
    d_t = HD // 8
    d_s = (HD - d_t) // 2
    pos = ids.astype(F32)
    lanes = []
    for axis, width in enumerate((d_t, d_s, d_s)):
        omega = THETA ** (-jnp.arange(0, width, 2, dtype=F32) / width)
        lanes.append(pos[:, axis:axis + 1] * jnp.repeat(omega, 2)[None, :])
    ang = jnp.concatenate(lanes, axis=-1)
    odd = (jnp.arange(HD) % 2).astype(F32)[None, :]
    sin = jnp.sin(ang)
    return jnp.cos(ang), -sin * (1.0 - odd), sin * odd


def device_fn(image, text, cond_vec, image_ids, *weights):
    (wm, bm, wqkv, bqkv, qg, kg, wp, bp, w1, b1, w2, b2) = weights[:12]
    (twm, tbm, twqkv, tbqkv, tqg, tkg, twp, tbp, tw1, tb1, tw2, tb2) = weights[12:]
    x, xt = image[0], text[0]
    d = x.shape[1]
    row = lambda v: v[None, :]
    m_img, m_txt = modulation(cond_vec, wm, twm)
    m_img = (m_img + bm.astype(F32)).reshape(6, d)
    m_txt = (m_txt + tbm.astype(F32)).reshape(6, d)
    cos, se, so = rope_tables(image_ids)
    o_img, o_txt = attention(x, xt, m_img, m_txt, wqkv, twqkv, row(bqkv), row(tbqkv),
                             jnp.stack([qg, kg]), jnp.stack([tqg, tkg]), cos, se, so)
    image_out, text_out = output(o_img, x, xt, o_txt, m_img, m_txt, wp, w1, w2, twp, tw1, tw2,
                                 row(bp), row(b1), row(b2), row(tbp), row(tb1), row(tb2))
    return image_out[None], text_out[None]


def solution(mesh):
    act = P("dp", "cp", None)
    txt = P("dp", None, None)
    in_specs = (act, txt, P("dp", None), P(("dp", "cp"), None)) + (P(),) * 24
    return jax.shard_map(device_fn, mesh=mesh, in_specs=in_specs, out_specs=(act, txt), check_vma=False)
```

```python
import functools

import jax
import jax.numpy as jnp
from jax import lax
from jax.experimental import pallas as pl
from jax.experimental.pallas import tpu as pltpu
from jax.sharding import PartitionSpec as P

EPS = 1e-6
THETA = 10000.0
F32 = jnp.float32
BF16 = jnp.bfloat16
HD = 128
NCHIP = 8
NDEV = 16
VM = pl.BlockSpec(memory_space=pltpu.VMEM)
ANY = pl.BlockSpec(memory_space=pl.ANY)
MESH = pl.DeviceIdType.MESH
VMEM_LIMIT = 67043328


def dot(a, b):
    return jnp.dot(a, b, preferred_element_type=F32)


def dot_t(a, b):
    return lax.dot_general(a, b, (((1,), (1,)), ((), ())), preferred_element_type=F32)


def bias_row(b_ref, row, n):
    return jnp.concatenate([b_ref[pl.ds(row + i, 1), :] for i in range(n)], axis=1)


def ln_mod_rows(x, scale1p, shift):
    xf = x.astype(F32)
    mean = jnp.mean(xf, axis=-1, keepdims=True)
    cent = xf - mean
    var = jnp.mean(cent * cent, axis=-1, keepdims=True)
    return scale1p * (cent * lax.rsqrt(var + EPS)) + shift


def main_kernel(cfg, boff, x_hbm, xt_hbm, cond_ref, wmi_hbm, wmt_hbm, wi_hbm, wt_hbm, b_ref, g_ref, pos_ref, om_ref,
                o_hbm, ot_ref, g2,
                xs, xm, xt, ks, vs, qs, kb, vb, qb, posm, cos_t, se_t, so_t, mi, mt, g1, mine1, mine2,
                xsem, wsem, wxsem, msend, mrecv, gsend, grecv, ssem, rsem, fssem, frsem, ossem, orsem):
    tok, txt, d_in, heads, ck = cfg
    hd_all = heads * HD
    nj = heads // NCHIP
    quad = 4
    me = lax.axis_index("cp")
    chip, core = me // 2, me % 2
    zh, cl = chip // quad, chip % quad
    plane = cl // 2
    sib = chip * 2 + (1 - core)
    mirror = lax.rem(chip + quad, NCHIP) * 2 + core
    outer = ((chip // 2) == 0) | ((chip // 2) == 3)
    m1 = 2 * tok // 3
    m2 = tok - m1
    sizes = (tok, m1, m2)
    rows0 = (0, tok, tok + m1)
    qpos = (txt, txt + quad * tok, txt + quad * (tok + m1))
    kpos = (txt, txt + 2 * quad * tok, txt + 2 * quad * (tok + m1))

    def same(c_local):
        return {"cp": (zh * quad + c_local) * 2 + core}

    def dev(c):
        return {"cp": c * 2 + core}

    barrier = pltpu.get_barrier_semaphore()
    for r in range(1, NDEV):
        pl.semaphore_signal(barrier, inc=1, device_id={"cp": lax.rem(me + r, NDEV)}, device_id_type=MESH)
    load_x = pltpu.make_async_copy(x_hbm, xs, xsem.at[0])
    load_t = pltpu.make_async_copy(xt_hbm, xt, xsem.at[1])

    def x_copy(part):
        sl = pl.ds(0, m1) if part == 0 else pl.ds(m1, m2)
        return pltpu.make_async_remote_copy(
            src_ref=x_hbm.at[sl, :], dst_ref=xm.at[sl, :], send_sem=msend.at[part], recv_sem=mrecv.at[part],
            device_id={"cp": mirror}, device_id_type=MESH)

    pos_copy = pltpu.make_async_remote_copy(
        src_ref=pos_ref, dst_ref=posm, send_sem=msend.at[2], recv_sem=mrecv.at[2],
        device_id={"cp": mirror}, device_id_type=MESH)

    def qkv_phase(w, wx):
        wide = quad * HD
        wc = wx.shape[2]
        kinds = (1, 2, 0)

        def w_copy(n):
            j, kind = n // 3, kinds[n % 3]
            off = pl.multiple_of(kind * hd_all + j * NCHIP * HD + zh * wide, wide)
            return pltpu.make_async_copy(wi_hbm.at[:, pl.ds(off, wide)], w.at[n], wsem.at[n])

        first = 2 * d_in // NDEV
        rest = 4 * d_in // NDEV
        n1, n2 = first // wc, rest // wc
        side = [(r, i) for r in ("mi1", "mt1") for i in range(n1)] + [("t", kind) for kind in kinds]
        side += [(r, i) for r in ("mi2", "mt2") for i in range(n2)]
        nslot = wx.shape[0]

        def side_copies(n):
            what, i = side[n]
            slot = n % nslot
            if what == "t":
                return [pltpu.make_async_copy(
                    wt_hbm.at[:, pl.ds(pl.multiple_of(i * hd_all + (j * NCHIP + chip) * HD, HD), HD)],
                    wx.at[slot, :, pl.ds(j * HD, HD)], wxsem.at[slot, j]) for j in range(nj)]
            ref = wmi_hbm if what[:2] == "mi" else wmt_hbm
            off = me * first + i * wc if what[2] == "1" else 2 * d_in + me * rest + i * wc
            return [pltpu.make_async_copy(ref.at[:, pl.ds(pl.multiple_of(off, 128), wc)], wx.at[slot], wxsem.at[slot, 0])]

        def side_start(n):
            if n < len(side):
                for c in side_copies(n):
                    c.start()

        def side_get(n):
            side_start(n + nslot - 1)
            for c in side_copies(n):
                c.wait()
            return n % nslot

        for n in range(nslot - 1):
            side_start(n)
        load_x.start()
        for n in range(3 * nj):
            w_copy(n).start()
        load_t.start()

        c = cond_ref[...].astype(F32)
        act = (c * jax.nn.sigmoid(c)).astype(BF16)
        act = jnp.broadcast_to(act, (16, d_in))
        pl.semaphore_wait(barrier, NDEV - 1)

        @pl.when(jnp.logical_not(outer))
        def _():
            x_copy(0).start()
            x_copy(1).start()
        pos_copy.start()

        per = wc // 128

        def mod_rows(n, buf, row):
            r = dot(act, wx[side_get(n)])
            for i in range(per):
                buf[row + i:row + i + 1, :] = r[0:1, i * 128:(i + 1) * 128]

        def spread(buf, dst, k):
            return [pltpu.make_async_remote_copy(
                src_ref=buf, dst_ref=dst.at[me], send_sem=gsend.at[k, r], recv_sem=grecv.at[k, r],
                device_id={"cp": lax.rem(me + r, NDEV)}, device_id_type=MESH) for r in range(1, NDEV)]

        mine1[...] = jnp.zeros_like(mine1)
        for n in range(2 * n1):
            mod_rows(n, mine1, n * per)
        gath1 = spread(mine1, g1, 0)
        for cp in gath1:
            cp.start()
        g1[me] = mine1[...]

        def tables(pos):
            ang = pos.astype(F32) * om_ref[...]
            odd = lax.rem(lax.broadcasted_iota(jnp.int32, ang.shape, 1), 2) == 1
            sin = jnp.sin(ang)
            cos_t[...] = jnp.cos(ang)
            se_t[...] = jnp.where(odd, 0.0, -sin)
            so_t[...] = jnp.where(odd, sin, 0.0)

        tables(pos_ref[...])
        for cp in gath1:
            cp.wait()
        rows1 = n1 * per
        for b, m in ((0, mi), (1, mt)):
            for dv in range(NDEV):
                for r in range(rows1):
                    col = (dv * rows1 + r) * 128
                    v = g1[dv, b * rows1 + r:b * rows1 + r + 1, :] + b_ref[boff[b] + dv * rows1 + r:boff[b] + dv * rows1 + r + 1, :]
                    m[col // d_in:col // d_in + 1, col % d_in:col % d_in + 128] = v

        rb = 16

        def ln_rows(ref, m_ref, lo, n):
            shift = m_ref[0:1, :]
            scale = 1.0 + m_ref[1:2, :]

            def body(i, carry):
                sl = pl.ds(pl.multiple_of(lo + i * rb, rb), rb)
                ref[sl, :] = ln_mod_rows(ref[sl, :], scale, shift).astype(BF16)
                return carry
            lax.fori_loop(0, n // rb, body, 0)

        def norm_rope(y, gain, lo, n):
            ms = jnp.mean(y * y, axis=-1, keepdims=True)
            y = y * lax.rsqrt(ms + EPS) * gain
            if lo is not None:
                sl = slice(lo, lo + n)
                y = y * cos_t[sl, :] + pltpu.roll(y, HD - 1, 1) * se_t[sl, :] + pltpu.roll(y, 1, 1) * so_t[sl, :]
            return y

        def qkv_copy(kind, st, j, c_src, c_dst, sem_i):
            n = sizes[st]
            src, dst = ((qs, qb), (ks, kb), (vs, vb))[kind]
            lo = rows0[st]
            if kind == 0:
                s, t = src.at[j * quad + c_dst, pl.ds(lo, n)], dst.at[j, pl.ds(pl.multiple_of(qpos[st] + c_src * n, 128), n)]
            else:
                at = pl.multiple_of(kpos[st] + core * quad * n + c_src * n, 128)
                if kind == 1:
                    s, t = src.at[j * quad + c_dst, pl.ds(lo, n)], dst.at[j, pl.ds(at, n)]
                else:
                    s, t = src.at[j * quad + c_dst, :, pl.ds(lo, n)], dst.at[j, :, pl.ds(at, n)]
            return pltpu.make_async_remote_copy(
                src_ref=s, dst_ref=t, send_sem=ssem.at[kind, st, j, sem_i], recv_sem=rsem.at[kind, st, j, sem_i],
                device_id=same(c_dst), device_id_type=MESH)

        def own_copy(kind, st, j):
            n, lo = sizes[st], rows0[st]
            h = j * quad + cl
            if kind == 0:
                qb[j, pl.ds(pl.multiple_of(qpos[st] + cl * n, 128), n)] = qs[h, lo:lo + n]
            else:
                at = pl.multiple_of(kpos[st] + core * quad * n + cl * n, 128)
                if kind == 1:
                    kb[j, pl.ds(at, n)] = ks[h, lo:lo + n]
                else:
                    vb[j, :, pl.ds(at, n)] = vs[h, :, lo:lo + n]

        def qkv_set(st, src, src_lo, tab_lo):
            n, lo = sizes[st], rows0[st]

            def per_j(j, carry):
                for i, kind in enumerate(kinds):
                    tile = 3 * j + i
                    if st == 0:
                        pltpu.make_async_copy(wi_hbm.at[:, 0:wide], w.at[tile], wsem.at[tile]).wait()

                    def cols(p, carry):
                        col = pl.multiple_of(p * 2 * HD, 2 * HD)
                        y2 = dot(src[src_lo:src_lo + n, :], w[tile, :, pl.ds(col, 2 * HD)])
                        for hh in range(2):
                            h = 2 * p + hh
                            brow = boff[2] + kind * heads + j * NCHIP + zh * quad + h
                            y = y2[:, hh * HD:(hh + 1) * HD] + b_ref[pl.ds(brow, 1), :]
                            head = j * quad + h
                            if kind == 2:
                                vs[head, :, lo:lo + n] = y.T.astype(BF16)
                            else:
                                y = norm_rope(y, g_ref[kind:kind + 1, :], tab_lo, n).astype(BF16)
                                (qs, ks)[kind][head, lo:lo + n] = y
                        return carry
                    lax.fori_loop(0, 2, cols, 0)
                    own_copy(kind, st, j)
                    for r in range(1, quad):
                        qkv_copy(kind, st, j, cl, lax.rem(cl + r, quad), r).start()
                return carry
            lax.fori_loop(0, nj, per_j, 0)

        def arrived(kind, st, j):
            for r in range(1, quad):
                qkv_copy(kind, st, j, lax.rem(cl + quad - r, quad), cl, r).wait_recv()

        load_x.wait()
        ln_rows(xs, mi, 0, tok)
        qkv_set(0, xs, 0, 0)

        @pl.when(outer)
        def _():
            x_copy(0).start()
            x_copy(1).start()

        load_t.wait()
        ln_rows(xt, mt, 0, txt)
        for i, kind in enumerate(kinds):
            slot = side_get(2 * n1 + i)
            y3 = dot(xt[...], wx[slot, :, 0:nj * HD])
            for j in range(nj):
                brow = boff[3] + kind * heads + j * NCHIP + chip
                y = y3[:, j * HD:(j + 1) * HD] + b_ref[pl.ds(brow, 1), :]
                if kind == 2:
                    vb[j, :, 0:txt] = y.T.astype(BF16)
                else:
                    (qb, kb)[kind][j, 0:txt] = norm_rope(y, g_ref[2 + kind:3 + kind, :], None, txt).astype(BF16)

        mine2[...] = jnp.zeros_like(mine2)
        for n in range(2 * n2):
            mod_rows(2 * n1 + 3 + n, mine2, n * per)
        gath2 = spread(mine2, g2, 1)
        for cp in gath2:
            cp.start()
        g2[me] = mine2[...]

        pos_copy.wait_recv()
        tables(posm[...])
        x_copy(0).wait_recv()
        ln_rows(xm, mi, 0, m1)
        qkv_set(1, xm, 0, 0)

        def to_sibling(kind, st, j):
            n = quad * sizes[st]
            at = pl.multiple_of(kpos[st] + core * n, 128)
            ref = kb.at[j, pl.ds(at, n)] if kind == 1 else vb.at[j, :, pl.ds(at, n)]
            return pltpu.make_async_remote_copy(
                src_ref=ref, dst_ref=ref, send_sem=fssem.at[kind - 1, st, j], recv_sem=frsem.at[kind - 1, st, j],
                device_id={"cp": sib}, device_id_type=MESH)

        for j in range(nj):
            for kind in (1, 2):
                arrived(kind, 0, j)
                to_sibling(kind, 0, j).start()
            arrived(0, 0, j)
        x_copy(1).wait_recv()
        ln_rows(xm, mi, m1, m2)
        qkv_set(2, xm, m1, m1)
        for j in range(nj):
            for kind in (1, 2):
                arrived(kind, 1, j)
                to_sibling(kind, 1, j).start()
            arrived(0, 1, j)
        for j in range(nj):
            for kind in (1, 2):
                arrived(kind, 2, j)
                to_sibling(kind, 2, j).start()
            arrived(0, 2, j)

        for cp in gath2:
            cp.wait()
        for part in range(2):
            x_copy(part).wait_send()
        pos_copy.wait_send()
        for j in range(nj):
            for st in range(3):
                for kind in range(3):
                    for r in range(1, quad):
                        qkv_copy(kind, st, j, cl, lax.rem(cl + r, quad), r).wait_send()
                for kind in (1, 2):
                    to_sibling(kind, st, j).wait()

    pl.run_scoped(qkv_phase, pltpu.VMEM((3 * nj, d_in, quad * HD), BF16), pltpu.VMEM((3, d_in, 2 * d_in // NDEV), BF16))

    scale2 = (HD ** -0.5) * 1.4426950408889634
    qt = 256
    keys = txt + 2 * quad * 2 * tok
    nchunk = keys // ck
    n_own, n_m1, n_m2 = quad * tok // qt, quad * m1 // qt, quad * m2 // qt
    ntile = 1 + n_own + n_m1 + n_m2
    g = n_own // 2

    def attention_phase(s0, s1, mx0, mx1, ost, otmp):
        def tile_start(t):
            own = t - 1 - n_m1 - n_m2
            p = jnp.where(own < g, 1 - plane, plane)
            row_own = txt + p * (2 * tok) + lax.rem(own + 2 * g, g) * qt
            row_mir = txt + quad * tok + (t - 1) * qt
            return pl.multiple_of(jnp.where(t == 0, 0, jnp.where(own < 0, row_mir, row_own)), 128)

        def qk(j, q, i, s_ref, mx):
            sl = pl.ds(pl.multiple_of(i * ck, ck), ck)
            s = dot_t(kb[j, sl], q)
            s_ref[sl, :] = s
            return jnp.maximum(mx, jnp.max(s.reshape(ck // 8, 8, qt), axis=0))

        def sm(j, i, s_ref, m, lsum, acc):
            sl = pl.ds(pl.multiple_of(i * ck, ck), ck)
            p = jnp.exp2((s_ref[sl, :] - m) * scale2)
            lsum = lsum + jnp.sum(p.reshape(ck // 8, 8, qt), axis=0)
            acc = acc + dot(vb[j, :, sl], p.astype(BF16))
            return lsum, acc

        def new_max():
            return jnp.full((8, qt), -jnp.inf, F32)

        def o_copy(j, c_src, c_dst, st):
            n = sizes[st]
            cd = lax.rem(c_dst, quad)
            base = (0, quad * tok, quad * (tok + m1))[st]
            dst_row = (0, 0, m1)[st]
            src = ost.at[j, pl.ds(pl.multiple_of(base + cd * n, 128), n)]
            dst = o_hbm.at[pl.ds(dst_row, n), pl.ds(pl.multiple_of((j * NCHIP + c_src) * HD, HD), HD)]
            return src, dst, dict(send_sem=ossem.at[j, st, cd], recv_sem=orsem.at[j, c_src, 1 if st == 2 else 0],
                                  device_id=dev(c_dst), device_id_type=MESH)

        def o_remote(j, c_src, c_dst, st):
            src, dst, kw = o_copy(j, c_src, c_dst, st)
            return pltpu.make_async_remote_copy(src_ref=src, dst_ref=dst, **kw)

        def o_local(j):
            src, dst, kw = o_copy(j, chip, chip, 0)
            return pltpu.make_async_copy(src, dst, kw["send_sem"])

        def send_own(j, p):
            for y in range(2):
                c = zh * quad + p * 2 + y

                @pl.when(c != chip)
                def _():
                    o_remote(j, chip, c, 0).start()

                @pl.when(c == chip)
                def _():
                    o_local(j).start()

        def finish(j, t, lsum, acc):
            tot = jnp.sum(lsum, axis=0, keepdims=True)
            o = (acc / tot).T.astype(BF16)

            @pl.when(t == 0)
            def _():
                otmp[...] = o
                ot_ref[j] = otmp[pl.ds(pl.multiple_of(core * (txt // 2), 8), txt // 2), :]

            @pl.when(t > 0)
            def _():
                ost[j, pl.ds(pl.multiple_of(tile_start(t) - txt, 128), qt)] = o

            far = (1 - zh) * quad

            @pl.when((t > 0) & (t <= n_m1))
            def _():
                o_remote(j, chip, far + t - 1, 1).start()

            @pl.when((t > n_m1) & (t <= n_m1 + n_m2))
            def _():
                for y in range(2):
                    o_remote(j, chip, far + 2 * (t - 1 - n_m1) + y, 2).start()

            @pl.when(t == n_m1 + n_m2 + g)
            def _():
                send_own(j, 1 - plane)

            @pl.when(t == n_m1 + n_m2 + 2 * g)
            def _():
                send_own(j, plane)

        def pair(j, t, s_cur, mx_cur, s_nxt, mx_nxt, has_next):
            m = jnp.max(mx_cur[...], axis=0, keepdims=True)
            lsum = jnp.zeros((8, qt), F32)
            acc = jnp.zeros((HD, qt), F32)
            if has_next:
                q = qb[j, pl.ds(tile_start(t + 1), qt)]

                def body(i, carry):
                    lsum, acc, mx = carry
                    mx = qk(j, q, i, s_nxt, mx)
                    lsum, acc = sm(j, i, s_cur, m, lsum, acc)
                    return lsum, acc, mx
                lsum, acc, mx = lax.fori_loop(0, nchunk, body, (lsum, acc, new_max()))
                mx_nxt[...] = mx
            else:
                def body(i, carry):
                    return sm(j, i, s_cur, m, *carry)
                lsum, acc = lax.fori_loop(0, nchunk, body, (lsum, acc))
            finish(j, t, lsum, acc)

        def head(j, carry):
            q = qb[j, 0:qt]

            def first(i, mx):
                return qk(j, q, i, s0, mx)
            mx0[...] = lax.fori_loop(0, nchunk, first, new_max())

            def two(i, carry):
                pair(j, 2 * i, s0, mx0, s1, mx1, True)
                pair(j, 2 * i + 1, s1, mx1, s0, mx0, True)
                return carry
            lax.fori_loop(0, (ntile - 1) // 2, two, 0)
            pair(j, jnp.int32(ntile - 1), s0, mx0, s1, mx1, False)
            return carry
        lax.fori_loop(0, nj, head, 0)

        for j in range(nj):
            o_local(j).wait()
            for r in range(1, quad):
                c = zh * quad + lax.rem(cl + r, quad)
                o_remote(j, chip, c, 0).wait_send()
                o_remote(j, c, chip, 0).wait_recv()
            for r in range(quad):
                c = (1 - zh) * quad + r
                for st in (1, 2):
                    o_remote(j, chip, c, st).wait_send()
                    o_remote(j, c, chip, st).wait_recv()

    pl.run_scoped(attention_phase, pltpu.VMEM((keys, qt), F32), pltpu.VMEM((keys, qt), F32), pltpu.VMEM((8, qt), F32),
                  pltpu.VMEM((8, qt), F32), pltpu.VMEM((nj, 2 * quad * tok, HD), BF16), pltpu.VMEM((txt, HD), BF16))


def attention(image, text, cond_vec, wm_img, wm_txt, w_img, w_txt, biases, boff, gains, pos, omega):
    tok, d_in = image.shape
    txt = text.shape[0]
    hd_all = w_img.shape[1] // 3
    heads = hd_all // HD
    nj = heads // NCHIP
    half = tok * NCHIP
    keys = txt + 2 * half
    ck = 1280
    cfg = (tok, txt, d_in, heads, ck)
    dma = pltpu.SemaphoreType.DMA
    flops = 2 * tok * d_in * 3 * hd_all + 4 * nj * HD * (half + txt) * keys
    r1 = 2 * (2 * d_in // NDEV) // 128
    r2 = 2 * (4 * d_in // NDEV) // 128
    r1, r2 = -(-r1 // 8) * 8, -(-r2 // 8) * 8
    return pl.pallas_call(
        functools.partial(main_kernel, cfg, boff),
        out_shape=(jax.ShapeDtypeStruct((tok, hd_all), BF16), jax.ShapeDtypeStruct((nj, txt // 2, HD), BF16),
                   jax.ShapeDtypeStruct((NDEV, r2, 128), F32)),
        in_specs=[ANY, ANY, VM, ANY, ANY, ANY, ANY, VM, VM, VM, VM],
        out_specs=(ANY, VM, VM),
        scratch_shapes=[
            pltpu.VMEM((tok, d_in), BF16),
            pltpu.VMEM((tok, d_in), BF16),
            pltpu.VMEM((txt, d_in), BF16),
            pltpu.VMEM((nj * 4, 2 * tok, HD), BF16),
            pltpu.VMEM((nj * 4, HD, 2 * tok), BF16),
            pltpu.VMEM((nj * 4, 2 * tok, HD), BF16),
            pltpu.VMEM((nj, keys, HD), BF16),
            pltpu.VMEM((nj, HD, keys), BF16),
            pltpu.VMEM((nj, txt + half, HD), BF16),
            pltpu.VMEM((tok, 128), BF16),
            pltpu.VMEM((tok, 128), F32), pltpu.VMEM((tok, 128), F32), pltpu.VMEM((tok, 128), F32),
            pltpu.VMEM((2, d_in), F32), pltpu.VMEM((2, d_in), F32),
            pltpu.VMEM((NDEV, r1, 128), F32), pltpu.VMEM((r1, 128), F32), pltpu.VMEM((r2, 128), F32),
            dma((2,)), dma((3 * nj,)), dma((3, max(nj, 1))), dma((3,)), dma((3,)), dma((2, NDEV)), dma((2, NDEV)),
            dma((3, 3, nj, 4)), dma((3, 3, nj, 4)), dma((2, 3, nj)), dma((2, 3, nj)),
            dma((nj, 3, 4)), dma((nj, NCHIP, 2)),
        ],
        compiler_params=pltpu.CompilerParams(collective_id=1, has_side_effects=True, vmem_limit_bytes=VMEM_LIMIT),
        cost_estimate=pl.CostEstimate(flops=flops, bytes_accessed=2 * d_in * 3 * hd_all, transcendentals=0),
        name="attn",
    )(image, text, cond_vec, wm_img, wm_txt, w_img, w_txt, biases, gains, pos, omega)


def gelu(x):
    return x * (0.5 * (1.0 + jnp.tanh(0.7978845608028654 * (x + 0.044715 * (x * x * x)))))


def out_kernel(cfg, boff, o_hbm, x_hbm, xt_hbm, ot_ref, g2_ref, b_ref, wp_hbm, w1_hbm, w2_hbm, twp_hbm, tw1_hbm, tw2_hbm,
               out_ref, tout_ref, mi_ref, mt_ref,
               wa, wb, o, x, h, z, acc, a0, a1, o_t, x_t, h_t, z_t, a_t, part, rs, row,
               asem, bsem, lsem, ossem, orsem, pssem, prsem, rssem, rrsem, fssem, frsem):
    tok, txt, d, ff, s1, s2 = cfg
    me = lax.axis_index("cp")
    chip, core = me // 2, me % 2
    sib = chip * 2 + (1 - core)
    rows = txt // 2
    piece = rows // NCHIP
    nb = wa.shape[2]
    na = wa.shape[0]
    np_ = d // nb
    nf = ff // nb
    ft = ff // NCHIP
    nt = ft // nb
    nj = ot_ref.shape[0]

    def dev(c):
        return {"cp": c * 2 + core}

    off = pl.multiple_of(chip * ft, nb)
    segs_a = ((np_, wp_hbm, 0), (s1, w1_hbm, 0), (np_, twp_hbm, 0), (nt, tw1_hbm, off), (nf - s1, w1_hbm, s1 * nb))
    segs_b = ((s1, w2_hbm, 0), (nt, tw2_hbm, off), (nf - s1, w2_hbm, s1 * nb))

    def start(p, segs, is_a):
        lo = 0
        for n, ref, base in segs:
            @pl.when((p >= lo) & (p < lo + n))
            def _(lo=lo, ref=ref, base=base):
                sl = pl.ds(pl.multiple_of(base + (p - lo) * nb, nb), nb)
                slot = lax.rem(p, na)
                if is_a:
                    pltpu.make_async_copy(ref.at[:, sl], wa.at[slot], asem.at[slot]).start()
                else:
                    pltpu.make_async_copy(ref.at[sl, :], wb.at[slot], bsem.at[slot]).start()
            lo += n

    def get_a(p):
        start(p + na - 1, segs_a, True)
        slot = lax.rem(p, na)
        pltpu.make_async_copy(w1_hbm.at[:, 0:nb], wa.at[slot], asem.at[slot]).wait()
        return slot

    def get_b(p):
        start(p + na - 1, segs_b, False)
        slot = lax.rem(p, na)
        pltpu.make_async_copy(w2_hbm.at[0:nb, :], wb.at[slot], bsem.at[slot]).wait()
        return slot

    load_o = pltpu.make_async_copy(o_hbm, o, lsem.at[0])
    load_x = pltpu.make_async_copy(x_hbm, x, lsem.at[1])
    load_t = pltpu.make_async_copy(xt_hbm.at[pl.ds(pl.multiple_of(core * rows, 8), rows), :], x_t, lsem.at[2])
    load_o.start()
    start(jnp.int32(0), segs_a, True)
    load_x.start()
    for p in range(1, na - 1):
        start(jnp.int32(p), segs_a, True)
    for p in range(na - 1):
        start(jnp.int32(p), segs_b, False)
    load_t.start()

    barrier = pltpu.get_barrier_semaphore()
    for r in range(1, NCHIP):
        pl.semaphore_signal(barrier, inc=1, device_id=dev(lax.rem(chip + r, NCHIP)), device_id_type=MESH)
    pl.semaphore_signal(barrier, inc=1, device_id={"cp": sib}, device_id_type=MESH)
    pl.semaphore_wait(barrier, NCHIP)

    def o_copy(j, r, c_src, c_dst):
        return pltpu.make_async_remote_copy(
            src_ref=ot_ref.at[j], dst_ref=o_t.at[:, pl.ds(pl.multiple_of((j * NCHIP + c_src) * HD, HD), HD)],
            send_sem=ossem.at[j, r], recv_sem=orsem.at[j, r], device_id=dev(c_dst), device_id_type=MESH)

    for j in range(nj):
        for r in range(1, NCHIP):
            o_copy(j, r, chip, lax.rem(chip + r, NCHIP)).start()
        o_t[:, pl.ds(pl.multiple_of((j * NCHIP + chip) * HD, HD), HD)] = ot_ref[j]

    per = 4 * d // NDEV // 128
    for b, m in ((0, mi_ref), (1, mt_ref)):
        for dv in range(NDEV):
            for r in range(per):
                col = 2 * d + (dv * per + r) * 128
                brow = boff[b] + col // 128
                m[col // d:col // d + 1, col % d:col % d + 128] = g2_ref[dv, b * per + r:b * per + r + 1, :] + b_ref[brow:brow + 1, :]
    n128 = nb // 128

    load_o.wait()
    load_x.wait()

    def proj(p, carry):
        slot = get_a(p)
        sl = pl.ds(pl.multiple_of(p * nb, nb), nb)
        y = dot(o[...], wa[slot]) + bias_row(b_ref, boff[4] + p * n128, n128)
        h[:, sl] = x[:, sl].astype(F32) + mi_ref[2:3, sl] * y
        return carry
    lax.fori_loop(0, np_, proj, 0)

    def ln2(src, dst, m_ref, n):
        shift, scale = m_ref[3:4, :], 1.0 + m_ref[4:5, :]
        rb = 16

        def body(i, carry):
            r = pl.ds(pl.multiple_of(i * rb, rb), rb)
            dst[r, :] = ln_mod_rows(src[r, :], scale, shift).astype(BF16)
            return carry
        lax.fori_loop(0, n // rb, body, 0)

    ln2(h, z, mi_ref, tok)
    acc[...] = jnp.broadcast_to(bias_row(b_ref, boff[8], d // 128), acc.shape)

    def mlp(i, pa, pb, a_new, a_old):
        slot_b = get_b(pb)
        slot_a = get_a(pa)
        a_new[...] = gelu(dot(z[...], wa[slot_a]) + bias_row(b_ref, boff[6] + i * n128, n128)).astype(BF16)
        acc[...] += dot(a_old[...], wb[slot_b])

    def mlp_range(lo, hi, da, db):
        def two(k, carry):
            i = lo + 2 * k
            mlp(i, i + da, i - 1 + db, a1, a0)
            mlp(i + 1, i + 1 + da, i + db, a0, a1)
            return carry
        lax.fori_loop(0, (hi - lo) // 2, two, 0)

    slot = get_a(jnp.int32(np_))
    a0[...] = gelu(dot(z[...], wa[slot]) + bias_row(b_ref, boff[6], n128)).astype(BF16)
    mlp_range(1, s1, np_, 0)
    slot = get_b(jnp.int32(s1 - 1))
    acc[...] += dot(a0[...], wb[slot])

    load_t.wait()
    for j in range(nj):
        for r in range(1, NCHIP):
            o_copy(j, r, lax.rem(chip + NCHIP - r, NCHIP), chip).wait_recv()
    pa = np_ + s1

    def tproj(k, carry):
        slot = get_a(pa + k)
        sl = pl.ds(pl.multiple_of(k * nb, nb), nb)
        y = dot(o_t[...], wa[slot]) + bias_row(b_ref, boff[5] + k * n128, n128)
        h_t[:, sl] = x_t[:, sl].astype(F32) + mt_ref[2:3, sl] * y
        return carry
    lax.fori_loop(0, np_, tproj, 0)
    ln2(h_t, z_t, mt_ref, rows)

    for k in range(nt):
        slot = get_a(jnp.int32(pa + np_ + k))
        y = dot(z_t[...], wa[slot]) + bias_row(b_ref, boff[7] + (chip * nt + k) * n128, n128)
        a_t[:, k * nb:(k + 1) * nb] = gelu(y).astype(BF16)
    for k in range(nt):
        slot = get_b(jnp.int32(s1 + k))
        y = dot(a_t[:, k * nb:(k + 1) * nb], wb[slot])
        part[...] = y if k == 0 else part[...] + y

    def p_copy(r, c_src, c_dst):
        return pltpu.make_async_remote_copy(
            src_ref=part.at[pl.ds(pl.multiple_of(c_dst * piece, 8), piece), :], dst_ref=rs.at[c_src],
            send_sem=pssem.at[r], recv_sem=prsem.at[r], device_id=dev(c_dst), device_id_type=MESH)

    for r in range(1, NCHIP):
        p_copy(r, chip, lax.rem(chip + r, NCHIP)).start()
    mine = pl.ds(pl.multiple_of(chip * piece, 8), piece)
    rs[chip] = part[mine, :]

    da, db = np_ + np_ + nt, nt
    slot = get_a(jnp.int32(s1 + da))
    a0[...] = gelu(dot(z[...], wa[slot]) + bias_row(b_ref, boff[6] + s1 * n128, n128)).astype(BF16)
    mlp_range(s1 + 1, s2, da, db)

    for r in range(1, NCHIP):
        p_copy(r, lax.rem(chip + NCHIP - r, NCHIP), chip).wait_recv()
    tot = rs[0]
    for c in range(1, NCHIP):
        tot = tot + rs[c]
    y = h_t[mine, :] + mt_ref[5:6, :] * (tot + bias_row(b_ref, boff[9], d // 128))
    row[...] = y.astype(BF16)

    def r_copy(r, c_src, c_dst):
        return pltpu.make_async_remote_copy(
            src_ref=row, dst_ref=tout_ref.at[pl.ds(pl.multiple_of(core * rows + c_src * piece, 8), piece), :],
            send_sem=rssem.at[r], recv_sem=rrsem.at[r], device_id=dev(c_dst), device_id_type=MESH)

    for r in range(1, NCHIP):
        r_copy(r, chip, lax.rem(chip + r, NCHIP)).start()
    tout_ref[pl.ds(pl.multiple_of(core * rows + chip * piece, 8), piece), :] = row[...]

    mlp_range(s2, nf, da, db)

    for r in range(1, NCHIP):
        r_copy(r, lax.rem(chip + NCHIP - r, NCHIP), chip).wait_recv()
    ref = tout_ref.at[pl.ds(pl.multiple_of(core * rows, 8), rows), :]
    fwd = pltpu.make_async_remote_copy(src_ref=ref, dst_ref=ref, send_sem=fssem, recv_sem=frsem,
                                       device_id={"cp": sib}, device_id_type=MESH)
    fwd.start()

    slot = get_b(jnp.int32(nf - 1 + db))
    y = acc[...] + dot((a0 if (nf - 1 - s1) % 2 == 0 else a1)[...], wb[slot])
    out_ref[...] = (h[...] + mi_ref[5:6, :] * y).astype(BF16)

    fwd.wait()
    for j in range(nj):
        for r in range(1, NCHIP):
            o_copy(j, r, chip, lax.rem(chip + r, NCHIP)).wait_send()
    for r in range(1, NCHIP):
        c = lax.rem(chip + r, NCHIP)
        p_copy(r, chip, c).wait_send()
        r_copy(r, chip, c).wait_send()


def output(o_img, image, text, o_txt, g2, biases, boff, wp, w1, w2, twp, tw1, tw2):
    tok, d = image.shape
    txt = text.shape[0]
    ff = w1.shape[1]
    nb = 512
    nf = ff // nb
    s1 = 3 if nf > 8 else 1
    s2 = 18 if nf > 8 else 4
    na = 3
    rows = txt // 2
    ft = ff // NCHIP
    nj = o_txt.shape[0]
    dma = pltpu.SemaphoreType.DMA
    flops = 2 * tok * d * (d + 2 * ff) + 2 * rows * d * (d + 2 * ft)
    return pl.pallas_call(
        functools.partial(out_kernel, (tok, txt, d, ff, s1, s2), boff),
        out_shape=(jax.ShapeDtypeStruct((tok, d), BF16), jax.ShapeDtypeStruct((txt, d), BF16)),
        in_specs=[ANY, ANY, ANY, VM, VM, VM] + [ANY] * 6,
        out_specs=(VM, VM),
        scratch_shapes=[
            pltpu.VMEM((6, d), F32), pltpu.VMEM((6, d), F32),
            pltpu.VMEM((na, d, nb), BF16), pltpu.VMEM((na, nb, d), BF16),
            pltpu.VMEM((tok, d), BF16), pltpu.VMEM((tok, d), BF16), pltpu.VMEM((tok, d), F32), pltpu.VMEM((tok, d), BF16),
            pltpu.VMEM((tok, d), F32), pltpu.VMEM((tok, nb), BF16), pltpu.VMEM((tok, nb), BF16),
            pltpu.VMEM((rows, d), BF16), pltpu.VMEM((rows, d), BF16), pltpu.VMEM((rows, d), F32), pltpu.VMEM((rows, d), BF16),
            pltpu.VMEM((rows, ft), BF16), pltpu.VMEM((rows, d), F32), pltpu.VMEM((NCHIP, rows // NCHIP, d), F32),
            pltpu.VMEM((rows // NCHIP, d), BF16),
            dma((na,)), dma((na,)), dma((3,)), dma((nj, NCHIP)), dma((nj, NCHIP)), dma((NCHIP,)), dma((NCHIP,)),
            dma((NCHIP,)), dma((NCHIP,)), dma, dma,
        ],
        compiler_params=pltpu.CompilerParams(collective_id=2, has_side_effects=True, vmem_limit_bytes=VMEM_LIMIT),
        cost_estimate=pl.CostEstimate(flops=flops, bytes_accessed=2 * d * (d + 2 * ff), transcendentals=0),
        name="out",
    )(o_img, image, text, o_txt, g2, biases, wp, w1, w2, twp, tw1, tw2)


def rope_inputs(ids):
    d_t = HD // 8
    d_s = (HD - d_t) // 2
    widths = (d_t, d_s, d_s)
    n = ids.shape[0]
    pos = jnp.concatenate([jnp.broadcast_to(ids[:, a:a + 1], (n, w)) for a, w in enumerate(widths)], axis=1).astype(BF16)
    omega = jnp.concatenate([jnp.repeat(THETA ** (-jnp.arange(0, w, 2, dtype=F32) / w), 2) for w in widths])
    return pos, omega[None, :]


def device_fn(image, text, cond_vec, image_ids, *weights):
    (wm, bm, wqkv, bqkv, qg, kg, wp, bp, w1, b1, w2, b2) = weights[:12]
    (twm, tbm, twqkv, tbqkv, tqg, tkg, twp, tbp, tw1, tb1, tw2, tb2) = weights[12:]
    x, xt = image[0], text[0]
    parts = (bm, tbm, bqkv, tbqkv, bp, tbp, b1, tb1, b2, tb2)
    boff, rows = [], 0
    for b in parts:
        boff.append(rows)
        rows += b.shape[0] // 128
    biases = jnp.concatenate(parts).astype(F32).reshape(rows, 128)
    boff = tuple(boff)
    gains = jnp.stack([qg, kg, tqg, tkg]).astype(F32)
    pos, omega = rope_inputs(image_ids)
    o_img, o_txt, g2 = attention(x, xt, cond_vec, wm, twm, wqkv, twqkv, biases, boff, gains, pos, omega)
    image_out, text_out = output(o_img, x, xt, o_txt, g2, biases, boff, wp, w1, w2, twp, tw1, tw2)
    return image_out[None], text_out[None]


def solution(mesh):
    act = P("dp", "cp", None)
    txt = P("dp", None, None)
    in_specs = (act, txt, P("dp", None), P(("dp", "cp"), None)) + (P(),) * 24
    return jax.shard_map(device_fn, mesh=mesh, in_specs=in_specs, out_specs=(act, txt), check_vma=False)
```

```python
import functools

import jax
import jax.numpy as jnp
import numpy as np
from jax import lax
from jax.experimental import pallas as pl
from jax.experimental.pallas import tpu as pltpu
from jax.sharding import PartitionSpec as P

EPS = 1e-6
THETA = 10000.0
F32 = jnp.float32
BF16 = jnp.bfloat16
HD = 128
NCHIP = 8
NDEV = 16
VM = pl.BlockSpec(memory_space=pltpu.VMEM)
ANY = pl.BlockSpec(memory_space=pl.ANY)
MESH = pl.DeviceIdType.MESH
VMEM_LIMIT = 67043328


def dot(a, b):
    return jnp.dot(a, b, preferred_element_type=F32)


def dot_t(a, b):
    return lax.dot_general(a, b, (((1,), (1,)), ((), ())), preferred_element_type=F32)


def lane_row(b_ref, start, n):
    return b_ref[pl.ds(start, n)].astype(F32).reshape(1, n)


def ln_mod_rows(x, scale1p, shift):
    xf = x.astype(F32)
    mean = jnp.mean(xf, axis=-1, keepdims=True)
    cent = xf - mean
    var = jnp.mean(cent * cent, axis=-1, keepdims=True)
    return scale1p * (cent * lax.rsqrt(var + EPS)) + shift


KINDS = (1, 2, 0)


def main_kernel(cfg, x_hbm, xt_hbm, cond_ref, wmi_hbm, wmt_hbm, wi_hbm, wt_hbm, bmi_ref, bmt_ref, bi_ref, bt_ref,
                qg_ref, kg_ref, tqg_ref, tkg_ref, pos_ref, om_ref,
                o_hbm, ot_ref, g2,
                w, xs, xm, xt, kn, kf, km, vn, vf, vm, qn, qf, qm, kb, vb, qb, posm, cos_t, se_t, so_t,
                mi, mt, g1, mine1, mine2, s0, s1, mx0, mx1, ost, otmp,
                xsem, wsem, msend, mrecv, gsend, grecv, ssem, rsem, fssem, frsem, ossem, orsem):
    tok, txt, d_in, heads, ck, mx = cfg
    nu = tok - mx
    hd_all = heads * HD
    nj = heads // NCHIP
    quad = 4
    wide = quad * HD
    half = tok * NCHIP
    me = lax.axis_index("cp")
    chip, core = me // 2, me % 2
    zh, cl = chip // quad, chip % quad
    sib = chip * 2 + (1 - core)
    mirror_chip = lax.rem(chip + quad, NCHIP)

    def dev(c):
        return {"cp": c * 2 + core}

    barrier = pltpu.get_barrier_semaphore()
    for r in range(1, NDEV):
        pl.semaphore_signal(barrier, inc=1, device_id={"cp": lax.rem(me + r, NDEV)}, device_id_type=MESH)
    load_x = pltpu.make_async_copy(x_hbm, xs, xsem.at[0])
    load_t = pltpu.make_async_copy(xt_hbm, xt, xsem.at[1])

    def x_copy():
        return pltpu.make_async_remote_copy(
            src_ref=x_hbm.at[pl.ds(nu, mx), :], dst_ref=xm, send_sem=msend.at[0], recv_sem=mrecv.at[0],
            device_id=dev(mirror_chip), device_id_type=MESH)

    def pos_copy():
        return pltpu.make_async_remote_copy(
            src_ref=pos_ref.at[pl.ds(nu, mx), :], dst_ref=posm, send_sem=msend.at[1], recv_sem=mrecv.at[1],
            device_id=dev(mirror_chip), device_id_type=MESH)

    mc = 2 * d_in // NDEV

    def tile_copy(what, a, b, slot):
        if what == "mod":
            ref = (wmi_hbm, wmt_hbm)[a]
            off = me * mc if b < 0 else 2 * d_in + me * 2 * mc + b * mc
            return [pltpu.make_async_copy(ref.at[:, pl.ds(pl.multiple_of(off, 128), mc)], w.at[slot, :, pl.ds(0, mc)], wsem.at[slot, 0])]
        if what == "txt":
            return [pltpu.make_async_copy(
                wt_hbm.at[:, pl.ds(pl.multiple_of(a * hd_all + (j * NCHIP + chip) * HD, HD), HD)],
                w.at[slot, :, pl.ds(j * HD, HD)], wsem.at[slot, j]) for j in range(nj)]
        kind, side = a
        off = kind * hd_all + b * NCHIP * HD + (zh if side == 0 else 1 - zh) * wide
        return [pltpu.make_async_copy(wi_hbm.at[:, pl.ds(pl.multiple_of(off, wide), wide)], w.at[slot], wsem.at[slot, 0])]

    def start(*a):
        for c in tile_copy(*a):
            c.start()

    def wait(*a):
        for c in tile_copy(*a):
            c.wait()
        return a[-1]

    def start_own(j, p):
        start("img", (KINDS[p // 2], p % 2), j, (2 + p) % 3)

    def start_txt(t):
        start("txt", KINDS[t], None, (2 + t) % 3)

    def start_mir(j, i):
        start("img", (KINDS[i], 0), j, (2 + i) % 3)

    def start_mod2(t):
        start("mod", t // 2, t % 2, (2 + t) % 3)

    start("mod", 0, -1, 0)
    start("mod", 1, -1, 1)
    load_x.start()
    load_t.start()

    c = cond_ref[...].astype(F32)
    act = (c * jax.nn.sigmoid(c)).astype(BF16)
    act = jnp.broadcast_to(act, (16, d_in))
    per = mc // 128

    def mod_rows(slot, buf, row):
        r = dot(act, w[slot, :, 0:mc])
        for i in range(per):
            buf[row + i:row + i + 1, :] = r[0:1, i * 128:(i + 1) * 128]

    def spread(buf, dst, k):
        return [pltpu.make_async_remote_copy(
            src_ref=buf, dst_ref=dst.at[me], send_sem=gsend.at[k, r], recv_sem=grecv.at[k, r],
            device_id={"cp": lax.rem(me + r, NDEV)}, device_id_type=MESH) for r in range(1, NDEV)]

    mine1[...] = jnp.zeros_like(mine1)
    start_own(0, 0)
    mod_rows(wait("mod", 0, -1, 0), mine1, 0)
    start_own(0, 1)
    mod_rows(wait("mod", 1, -1, 1), mine1, per)
    pl.semaphore_wait(barrier, NDEV - 1)
    gath1 = spread(mine1, g1, 0)
    for cp in gath1:
        cp.start()
    pos_copy().start()
    x_copy().start()
    g1[me] = mine1[...]

    def tables(pos, n):
        ang = pos.astype(F32) * om_ref[...]
        odd = lax.rem(lax.broadcasted_iota(jnp.int32, ang.shape, 1), 2) == 1
        sin = jnp.sin(ang)
        cos_t[0:n, :] = jnp.cos(ang)
        se_t[0:n, :] = jnp.where(odd, 0.0, -sin)
        so_t[0:n, :] = jnp.where(odd, sin, 0.0)

    tables(pos_ref[...], tok)
    for b_ref, m in ((bmi_ref, mi), (bmt_ref, mt)):
        for k in range(2):
            m[k:k + 1, :] = lane_row(b_ref, k * d_in, d_in)
    for cp in gath1:
        cp.wait()
    for b, m in ((0, mi), (1, mt)):
        for dv in range(NDEV):
            for r in range(per):
                col = (dv * per + r) * 128
                at = (slice(col // d_in, col // d_in + 1), slice(col % d_in, col % d_in + 128))
                m[at] = m[at] + g1[dv, b * per + r:b * per + r + 1, :]

    rb = 16

    def ln_rows(ref, m_ref, n):
        shift = m_ref[0:1, :]
        scale = 1.0 + m_ref[1:2, :]

        def body(i, carry):
            sl = pl.ds(pl.multiple_of(i * rb, rb), rb)
            ref[sl, :] = ln_mod_rows(ref[sl, :], scale, shift).astype(BF16)
            return carry
        lax.fori_loop(0, n // rb, body, 0)

    def norm_rope(y, gain, rope):
        ms = jnp.mean(y * y, axis=-1, keepdims=True)
        y = y * lax.rsqrt(ms + EPS) * gain
        if rope:
            n = y.shape[0]
            y = y * cos_t[0:n, :] + pltpu.roll(y, HD - 1, 1) * se_t[0:n, :] + pltpu.roll(y, 1, 1) * so_t[0:n, :]
        return y

    def place(kind, s_chip, row, n, j):
        if kind == 0:
            return qb.at[j, pl.ds(pl.multiple_of(txt + s_chip * tok + row, 128), n)]
        at = pl.multiple_of(txt + core * half + s_chip * tok + row, 128)
        return kb.at[j, pl.ds(at, n)] if kind == 1 else vb.at[j, :, pl.ds(at, n)]

    def qkv_copy(kind, ty, j, src_cl, src_zh, dst_cl, idx):
        buf = ((qn, qf, qm), (kn, kf, km), (vn, vf, vm))[kind][ty]
        n = (tok, nu, mx)[ty]
        s_chip = src_zh * quad + src_cl
        tgt = (1 - src_zh if ty == 1 else src_zh) * quad + dst_cl
        if ty == 2:
            dst = place(kind, lax.rem(s_chip + quad, NCHIP), nu, n, j)
        else:
            dst = place(kind, s_chip, 0, n, j)
        return pltpu.make_async_remote_copy(
            src_ref=buf.at[j * quad + dst_cl], dst_ref=dst, send_sem=ssem.at[kind, ty, j, idx[0]],
            recv_sem=rsem.at[kind, ty, j, idx[1]], device_id=dev(tgt), device_id_type=MESH)

    def out_copies(kind, ty, j):
        if ty == 1:
            return [qkv_copy(kind, 1, j, cl, zh, c, (c, cl)) for c in range(quad)]
        return [qkv_copy(kind, ty, j, cl, zh, lax.rem(cl + r, quad), (r, r)) for r in range(1, quad)]

    def in_copies(kind, ty, j):
        if ty == 1:
            return [qkv_copy(kind, 1, j, c, 1 - zh, cl, (c, c)) for c in range(quad)]
        return [qkv_copy(kind, ty, j, lax.rem(cl + quad - r, quad), zh, cl, (r, r)) for r in range(1, quad)]

    def own_copy(kind, ty, j):
        buf = ((qn, qf, qm), (kn, kf, km), (vn, vf, vm))[kind][ty]
        n = (tok, nu, mx)[ty]
        dst = place(kind, mirror_chip, nu, n, j) if ty == 2 else place(kind, chip, 0, n, j)
        dst[...] = buf[j * quad + cl]

    def make(kind, ty, j, slot):
        src = xm if ty == 2 else xs
        n = (tok, nu, mx)[ty]
        buf = ((qn, qf, qm), (kn, kf, km), (vn, vf, vm))[kind][ty]

        def cols(p, carry):
            col = pl.multiple_of(p * 2 * HD, 2 * HD)
            boff = kind * hd_all + j * NCHIP * HD + (1 - zh if ty == 1 else zh) * wide + col
            y2 = dot(src[0:n, :], w[slot, :, pl.ds(col, 2 * HD)]) + lane_row(bi_ref, pl.multiple_of(boff, 256), 2 * HD)
            for hh in range(2):
                y = y2[:, hh * HD:(hh + 1) * HD]
                if kind == 2:
                    buf[j * quad + 2 * p + hh] = y.T.astype(BF16)
                else:
                    gain = (qg_ref, kg_ref)[kind][...].astype(F32).reshape(1, HD)
                    buf[j * quad + 2 * p + hh] = norm_rope(y, gain, True).astype(BF16)
            return carry
        lax.fori_loop(0, 2, cols, 0)

    load_x.wait()
    ln_rows(xs, mi, tok)

    def own_pass(j, carry):
        for p in range(6):
            kind, side = KINDS[p // 2], p % 2
            if p + 2 < 6:
                start_own(j, p + 2)
            else:
                @pl.when(j < nj - 1)
                def _():
                    start_own(j + 1, p - 4)

                @pl.when(j == nj - 1)
                def _():
                    start_txt(p - 4)
            slot = wait("img", (kind, side), j, (2 + p) % 3)
            make(kind, side, j, slot)
            for cp in out_copies(kind, side, j):
                cp.start()
            if side == 0:
                own_copy(kind, 0, j)
        return carry
    lax.fori_loop(0, nj, own_pass, 0)

    load_t.wait()
    ln_rows(xt, mt, txt)
    for t, kind in enumerate(KINDS):
        if t == 0:
            start_txt(2)
        else:
            start_mir(0, t - 1)
        slot = wait("txt", kind, None, (2 + t) % 3)
        y3 = dot(xt[...], w[slot, :, 0:nj * HD])
        for j in range(nj):
            pair0 = kind * hd_all + (j * NCHIP + chip - lax.rem(chip, 2)) * HD
            b2 = lane_row(bt_ref, pl.multiple_of(pair0, 256), 2 * HD)
            y = y3[:, j * HD:(j + 1) * HD] + jnp.where(lax.rem(chip, 2) == 0, b2[:, 0:HD], b2[:, HD:2 * HD])
            if kind == 2:
                vb[j, :, 0:txt] = y.T.astype(BF16)
            else:
                gain = (tqg_ref, tkg_ref)[kind][...].astype(F32).reshape(1, HD)
                (qb, kb)[kind][j, 0:txt] = norm_rope(y, gain, False).astype(BF16)

    pos_copy().wait_recv()
    tables(posm[...], mx)
    x_copy().wait_recv()
    ln_rows(xm, mi, mx)

    def mir_pass(j, carry):
        for i, kind in enumerate(KINDS):
            if i == 0:
                start_mir(j, 2)
            else:
                @pl.when(j < nj - 1)
                def _():
                    start_mir(j + 1, i - 1)

                @pl.when(j == nj - 1)
                def _():
                    start_mod2(i - 1)
            slot = wait("img", (kind, 0), j, (2 + i) % 3)
            make(kind, 2, j, slot)
            for cp in out_copies(kind, 2, j):
                cp.start()
            own_copy(kind, 2, j)
        return carry
    lax.fori_loop(0, nj, mir_pass, 0)

    mine2[...] = jnp.zeros_like(mine2)
    for t in range(4):
        if t + 2 < 4:
            start_mod2(t + 2)
        mod_rows(wait("mod", t // 2, t % 2, (2 + t) % 3), mine2, t * per)
    gath2 = spread(mine2, g2, 1)
    for cp in gath2:
        cp.start()
    g2[me] = mine2[...]

    scale2 = (HD ** -0.5) * 1.4426950408889634
    keys = txt + 2 * half
    nchunk = keys // ck
    qt = 256
    ntile = (txt + half) // qt
    group = 2 * tok // qt
    ngroup = NCHIP // 2

    def to_sibling(kind, j):
        ref = (kb.at[j, pl.ds(pl.multiple_of(txt + core * half, 128), half)] if kind == 1
               else vb.at[j, :, pl.ds(pl.multiple_of(txt + core * half, 128), half)])
        return pltpu.make_async_remote_copy(
            src_ref=ref, dst_ref=ref, send_sem=fssem.at[kind - 1, j], recv_sem=frsem.at[kind - 1, j],
            device_id={"cp": sib}, device_id_type=MESH)

    def collect(j):
        for kind in KINDS:
            for ty in range(3):
                for cp in in_copies(kind, ty, j):
                    cp.wait_recv()
            if kind != 0:
                to_sibling(kind, j).start()

    def tile_start(t):
        g = (t - 1) // group
        plane = lax.rem(chip // 2 + 1 + g, ngroup)
        row = txt + plane * (2 * tok) + lax.rem(t - 1, group) * qt
        return pl.multiple_of(jnp.where(t == 0, 0, row), 128)

    def qk(j, q, i, s_ref, mxv):
        sl = pl.ds(pl.multiple_of(i * ck, ck), ck)
        s = dot_t(kb[j, sl], q)
        s_ref[sl, :] = s
        return jnp.maximum(mxv, jnp.max(s.reshape(ck // 8, 8, qt), axis=0))

    def sm(j, i, s_ref, m, lsum, acc):
        sl = pl.ds(pl.multiple_of(i * ck, ck), ck)
        p = jnp.exp2((s_ref[sl, :] - m) * scale2)
        lsum = lsum + jnp.sum(p.reshape(ck // 8, 8, qt), axis=0)
        acc = acc + dot(vb[j, :, sl], p.astype(BF16))
        return lsum, acc

    def new_max():
        return jnp.full((8, qt), -jnp.inf, F32)

    def o_remote(j, c_src, c_dst):
        src = ost.at[j, pl.ds(pl.multiple_of(c_dst * tok, 128), tok)]
        dst = o_hbm.at[:, pl.ds(pl.multiple_of((j * NCHIP + c_src) * HD, HD), HD)]
        return pltpu.make_async_remote_copy(
            src_ref=src, dst_ref=dst, send_sem=ossem.at[j, c_dst], recv_sem=orsem.at[j, c_src],
            device_id=dev(c_dst), device_id_type=MESH)

    def o_local(j):
        src = ost.at[j, pl.ds(pl.multiple_of(chip * tok, 128), tok)]
        dst = o_hbm.at[:, pl.ds(pl.multiple_of((j * NCHIP + chip) * HD, HD), HD)]
        return pltpu.make_async_copy(src, dst, ossem.at[j, chip])

    def o_send(j, g):
        plane = lax.rem(chip // 2 + 1 + g, ngroup)
        for y in range(2):
            c = plane * 2 + y

            @pl.when(c != chip)
            def _():
                o_remote(j, chip, c).start()

            @pl.when(c == chip)
            def _():
                o_local(j).start()

    def finish(j, t, lsum, acc):
        tot = jnp.sum(lsum, axis=0, keepdims=True)
        o = (acc / tot).T.astype(BF16)

        @pl.when(t == 0)
        def _():
            otmp[...] = o
            ot_ref[j] = otmp[pl.ds(pl.multiple_of(core * (txt // 2), 8), txt // 2), :]

        @pl.when(t > 0)
        def _():
            ost[j, pl.ds(pl.multiple_of(tile_start(t) - txt, 128), qt)] = o

            @pl.when(lax.rem(t, group) == 0)
            def _():
                o_send(j, t // group - 1)

    def pair(j, t, s_cur, mx_cur, s_nxt, mx_nxt, has_next):
        m = jnp.max(mx_cur[...], axis=0, keepdims=True)
        lsum = jnp.zeros((8, qt), F32)
        acc = jnp.zeros((HD, qt), F32)
        if has_next:
            q = qb[j, pl.ds(tile_start(t + 1), qt)]

            def body(i, carry):
                lsum, acc, mxv = carry
                mxv = qk(j, q, i, s_nxt, mxv)
                lsum, acc = sm(j, i, s_cur, m, lsum, acc)
                return lsum, acc, mxv
            lsum, acc, mxv = lax.fori_loop(0, nchunk, body, (lsum, acc, new_max()))
            mx_nxt[...] = mxv
        else:
            def body(i, carry):
                return sm(j, i, s_cur, m, *carry)
            lsum, acc = lax.fori_loop(0, nchunk, body, (lsum, acc))
        finish(j, t, lsum, acc)

    collect(0)

    def head(j, carry):
        for kind in (1, 2):
            to_sibling(kind, j).wait()
        q = qb[j, 0:qt]

        def first(i, mxv):
            return qk(j, q, i, s0, mxv)
        mx0[...] = lax.fori_loop(0, nchunk, first, new_max())

        def two(i, carry):
            pair(j, 2 * i, s0, mx0, s1, mx1, True)
            pair(j, 2 * i + 1, s1, mx1, s0, mx0, True)
            return carry
        lax.fori_loop(0, (ntile - 1) // 2, two, 0)
        if nj > 1:
            @pl.when(j < nj - 1)
            def _():
                collect(j + 1)
        pair(j, jnp.int32(ntile - 1), s0, mx0, s1, mx1, False)
        return carry
    lax.fori_loop(0, nj, head, 0)

    for cp in gath2:
        cp.wait()
    x_copy().wait_send()
    pos_copy().wait_send()

    def drain(j, carry):
        for kind in KINDS:
            for ty in range(3):
                for cp in out_copies(kind, ty, j):
                    cp.wait_send()
        o_local(j).wait()
        for r in range(1, NCHIP):
            c = lax.rem(chip + r, NCHIP)
            o_remote(j, chip, c).wait_send()
            o_remote(j, c, chip).wait_recv()
        return carry
    lax.fori_loop(0, nj, drain, 0)


def attention(image, text, cond_vec, wm_img, wm_txt, w_img, w_txt, flat, pos, omega):
    tok, d_in = image.shape
    txt = text.shape[0]
    hd_all = w_img.shape[1] // 3
    heads = hd_all // HD
    nj = heads // NCHIP
    half = tok * NCHIP
    keys = txt + 2 * half
    ck = 1280
    mx = 128
    nu = tok - mx
    cfg = (tok, txt, d_in, heads, ck, mx)
    dma = pltpu.SemaphoreType.DMA
    flops = 2 * tok * d_in * 3 * hd_all + 4 * nj * HD * (half + txt) * keys
    per = 2 * d_in // NDEV // 128
    r1, r2 = -(-2 * per // 8) * 8, -(-4 * per // 8) * 8
    row_sets = [pltpu.VMEM((nj * 4, n, HD), BF16) for n in (tok, nu, mx)]
    col_sets = [pltpu.VMEM((nj * 4, HD, n), BF16) for n in (tok, nu, mx)]
    table = pltpu.VMEM((tok, 128), F32)
    return pl.pallas_call(
        functools.partial(main_kernel, cfg),
        out_shape=(jax.ShapeDtypeStruct((tok, hd_all), BF16), jax.ShapeDtypeStruct((nj, txt // 2, HD), BF16),
                   jax.ShapeDtypeStruct((NDEV, r2, 128), F32)),
        in_specs=[ANY, ANY, VM, ANY, ANY, ANY, ANY] + [VM] * 10,
        out_specs=(ANY, VM, VM),
        scratch_shapes=[
            pltpu.VMEM((3, d_in, 4 * HD), BF16),
            pltpu.VMEM((tok, d_in), BF16), pltpu.VMEM((mx, d_in), BF16), pltpu.VMEM((txt, d_in), BF16),
            *row_sets, *col_sets, *row_sets,
            pltpu.VMEM((nj, keys, HD), BF16), pltpu.VMEM((nj, HD, keys), BF16), pltpu.VMEM((nj, txt + half, HD), BF16),
            pltpu.VMEM((mx, 128), BF16), table, table, table,
            pltpu.VMEM((2, d_in), F32), pltpu.VMEM((2, d_in), F32),
            pltpu.VMEM((NDEV, r1, 128), F32), pltpu.VMEM((r1, 128), F32), pltpu.VMEM((r2, 128), F32),
            pltpu.VMEM((keys, 256), F32), pltpu.VMEM((keys, 256), F32), pltpu.VMEM((8, 256), F32), pltpu.VMEM((8, 256), F32),
            pltpu.VMEM((nj, half, HD), BF16), pltpu.VMEM((txt, HD), BF16),
            dma((2,)), dma((3, max(nj, 1))), dma((2,)), dma((2,)), dma((2, NDEV)), dma((2, NDEV)),
            dma((3, 3, nj, 4)), dma((3, 3, nj, 4)), dma((2, nj)), dma((2, nj)), dma((nj, NCHIP)), dma((nj, NCHIP)),
        ],
        compiler_params=pltpu.CompilerParams(collective_id=1, has_side_effects=True, vmem_limit_bytes=VMEM_LIMIT),
        cost_estimate=pl.CostEstimate(flops=flops, bytes_accessed=3 * d_in * 3 * hd_all, transcendentals=0),
        name="attn",
    )(image, text, cond_vec, wm_img, wm_txt, w_img, w_txt, *flat, pos, omega)


def gelu(x):
    return x * (0.5 * (1.0 + jnp.tanh(0.7978845608028654 * (x + 0.044715 * (x * x * x)))))


def out_kernel(cfg, o_hbm, x_hbm, xt_hbm, ot_ref, g2_ref, bmi_ref, bmt_ref, bp_ref, tbp_ref, b1_ref, tb1_ref, b2_ref, tb2_ref, wp_hbm, w1_hbm, w2_hbm, twp_hbm, tw1_hbm, tw2_hbm,
               out_ref, tout_ref, mi_ref, mt_ref,
               wa, wb, o, x, h, z, acc, a0, a1, o_t, x_t, h_t, z_t, a_t, part, rs, row,
               asem, bsem, lsem, ossem, orsem, pssem, prsem, rssem, rrsem, fssem, frsem):
    tok, txt, d, ff, s1, s2 = cfg
    me = lax.axis_index("cp")
    chip, core = me // 2, me % 2
    sib = chip * 2 + (1 - core)
    rows = txt // 2
    piece = rows // NCHIP
    nb = wa.shape[2]
    na = wa.shape[0]
    np_ = d // nb
    nf = ff // nb
    ft = ff // NCHIP
    nt = ft // nb
    nj = ot_ref.shape[0]

    def dev(c):
        return {"cp": c * 2 + core}

    off = pl.multiple_of(chip * ft, nb)
    segs_a = ((np_, wp_hbm, 0), (s1, w1_hbm, 0), (np_, twp_hbm, 0), (nt, tw1_hbm, off), (nf - s1, w1_hbm, s1 * nb))
    segs_b = ((s1, w2_hbm, 0), (nt, tw2_hbm, off), (nf - s1, w2_hbm, s1 * nb))

    def start(p, segs, is_a):
        lo = 0
        for n, ref, base in segs:
            @pl.when((p >= lo) & (p < lo + n))
            def _(lo=lo, ref=ref, base=base):
                sl = pl.ds(pl.multiple_of(base + (p - lo) * nb, nb), nb)
                slot = lax.rem(p, na)
                if is_a:
                    pltpu.make_async_copy(ref.at[:, sl], wa.at[slot], asem.at[slot]).start()
                else:
                    pltpu.make_async_copy(ref.at[sl, :], wb.at[slot], bsem.at[slot]).start()
            lo += n

    def get_a(p):
        start(p + na - 1, segs_a, True)
        slot = lax.rem(p, na)
        pltpu.make_async_copy(w1_hbm.at[:, 0:nb], wa.at[slot], asem.at[slot]).wait()
        return slot

    def get_b(p):
        start(p + na - 1, segs_b, False)
        slot = lax.rem(p, na)
        pltpu.make_async_copy(w2_hbm.at[0:nb, :], wb.at[slot], bsem.at[slot]).wait()
        return slot

    load_o = pltpu.make_async_copy(o_hbm, o, lsem.at[0])
    load_x = pltpu.make_async_copy(x_hbm, x, lsem.at[1])
    load_t = pltpu.make_async_copy(xt_hbm.at[pl.ds(pl.multiple_of(core * rows, 8), rows), :], x_t, lsem.at[2])
    load_o.start()
    start(jnp.int32(0), segs_a, True)
    load_x.start()
    for p in range(1, na - 1):
        start(jnp.int32(p), segs_a, True)
    for p in range(na - 1):
        start(jnp.int32(p), segs_b, False)
    load_t.start()

    barrier = pltpu.get_barrier_semaphore()
    for r in range(1, NCHIP):
        pl.semaphore_signal(barrier, inc=1, device_id=dev(lax.rem(chip + r, NCHIP)), device_id_type=MESH)
    pl.semaphore_signal(barrier, inc=1, device_id={"cp": sib}, device_id_type=MESH)
    pl.semaphore_wait(barrier, NCHIP)

    def o_copy(j, r, c_src, c_dst):
        return pltpu.make_async_remote_copy(
            src_ref=ot_ref.at[j], dst_ref=o_t.at[:, pl.ds(pl.multiple_of((j * NCHIP + c_src) * HD, HD), HD)],
            send_sem=ossem.at[j, r], recv_sem=orsem.at[j, r], device_id=dev(c_dst), device_id_type=MESH)

    for j in range(nj):
        for r in range(1, NCHIP):
            o_copy(j, r, chip, lax.rem(chip + r, NCHIP)).start()
        o_t[:, pl.ds(pl.multiple_of((j * NCHIP + chip) * HD, HD), HD)] = ot_ref[j]

    per = 4 * d // NDEV // 128
    for b, (b_ref, m) in enumerate(((bmi_ref, mi_ref), (bmt_ref, mt_ref))):
        for k in range(2, 6):
            m[k:k + 1, :] = lane_row(b_ref, k * d, d)
        for dv in range(NDEV):
            for r in range(per):
                col = 2 * d + (dv * per + r) * 128
                at = (slice(col // d, col // d + 1), slice(col % d, col % d + 128))
                m[at] = m[at] + g2_ref[dv, b * per + r:b * per + r + 1, :]

    load_o.wait()
    load_x.wait()

    def proj(p, carry):
        slot = get_a(p)
        sl = pl.ds(pl.multiple_of(p * nb, nb), nb)
        y = dot(o[...], wa[slot]) + lane_row(bp_ref, pl.multiple_of(p * nb, nb), nb)
        h[:, sl] = x[:, sl].astype(F32) + mi_ref[2:3, sl] * y
        return carry
    lax.fori_loop(0, np_, proj, 0)

    def ln2(src, dst, m_ref, n):
        shift, scale = m_ref[3:4, :], 1.0 + m_ref[4:5, :]
        rb = 16

        def body(i, carry):
            r = pl.ds(pl.multiple_of(i * rb, rb), rb)
            dst[r, :] = ln_mod_rows(src[r, :], scale, shift).astype(BF16)
            return carry
        lax.fori_loop(0, n // rb, body, 0)

    ln2(h, z, mi_ref, tok)
    acc[...] = jnp.broadcast_to(lane_row(b2_ref, 0, d), acc.shape)

    def mlp(i, pa, pb, a_new, a_old):
        slot_b = get_b(pb)
        slot_a = get_a(pa)
        a_new[...] = gelu(dot(z[...], wa[slot_a]) + lane_row(b1_ref, pl.multiple_of(i * nb, nb), nb)).astype(BF16)
        acc[...] += dot(a_old[...], wb[slot_b])

    def mlp_range(lo, hi, da, db):
        def two(k, carry):
            i = lo + 2 * k
            mlp(i, i + da, i - 1 + db, a1, a0)
            mlp(i + 1, i + 1 + da, i + db, a0, a1)
            return carry
        lax.fori_loop(0, (hi - lo) // 2, two, 0)

    slot = get_a(jnp.int32(np_))
    a0[...] = gelu(dot(z[...], wa[slot]) + lane_row(b1_ref, 0, nb)).astype(BF16)
    mlp_range(1, s1, np_, 0)
    slot = get_b(jnp.int32(s1 - 1))
    acc[...] += dot(a0[...], wb[slot])

    load_t.wait()
    for j in range(nj):
        for r in range(1, NCHIP):
            o_copy(j, r, lax.rem(chip + NCHIP - r, NCHIP), chip).wait_recv()
    pa = np_ + s1

    def tproj(k, carry):
        slot = get_a(pa + k)
        sl = pl.ds(pl.multiple_of(k * nb, nb), nb)
        y = dot(o_t[...], wa[slot]) + lane_row(tbp_ref, pl.multiple_of(k * nb, nb), nb)
        h_t[:, sl] = x_t[:, sl].astype(F32) + mt_ref[2:3, sl] * y
        return carry
    lax.fori_loop(0, np_, tproj, 0)
    ln2(h_t, z_t, mt_ref, rows)

    for k in range(nt):
        slot = get_a(jnp.int32(pa + np_ + k))
        y = dot(z_t[...], wa[slot]) + lane_row(tb1_ref, pl.multiple_of(off + k * nb, nb), nb)
        a_t[:, k * nb:(k + 1) * nb] = gelu(y).astype(BF16)
    for k in range(nt):
        slot = get_b(jnp.int32(s1 + k))
        y = dot(a_t[:, k * nb:(k + 1) * nb], wb[slot])
        part[...] = y if k == 0 else part[...] + y

    def p_copy(r, c_src, c_dst):
        return pltpu.make_async_remote_copy(
            src_ref=part.at[pl.ds(pl.multiple_of(c_dst * piece, 8), piece), :], dst_ref=rs.at[c_src],
            send_sem=pssem.at[r], recv_sem=prsem.at[r], device_id=dev(c_dst), device_id_type=MESH)

    for r in range(1, NCHIP):
        p_copy(r, chip, lax.rem(chip + r, NCHIP)).start()
    mine = pl.ds(pl.multiple_of(chip * piece, 8), piece)
    rs[chip] = part[mine, :]

    da, db = np_ + np_ + nt, nt
    slot = get_a(jnp.int32(s1 + da))
    a0[...] = gelu(dot(z[...], wa[slot]) + lane_row(b1_ref, s1 * nb, nb)).astype(BF16)
    mlp_range(s1 + 1, s2, da, db)

    for r in range(1, NCHIP):
        p_copy(r, lax.rem(chip + NCHIP - r, NCHIP), chip).wait_recv()
    tot = rs[0]
    for c in range(1, NCHIP):
        tot = tot + rs[c]
    y = h_t[mine, :] + mt_ref[5:6, :] * (tot + lane_row(tb2_ref, 0, d))
    row[...] = y.astype(BF16)

    def r_copy(r, c_src, c_dst):
        return pltpu.make_async_remote_copy(
            src_ref=row, dst_ref=tout_ref.at[pl.ds(pl.multiple_of(core * rows + c_src * piece, 8), piece), :],
            send_sem=rssem.at[r], recv_sem=rrsem.at[r], device_id=dev(c_dst), device_id_type=MESH)

    for r in range(1, NCHIP):
        r_copy(r, chip, lax.rem(chip + r, NCHIP)).start()
    tout_ref[pl.ds(pl.multiple_of(core * rows + chip * piece, 8), piece), :] = row[...]

    mlp_range(s2, nf, da, db)

    for r in range(1, NCHIP):
        r_copy(r, lax.rem(chip + NCHIP - r, NCHIP), chip).wait_recv()
    ref = tout_ref.at[pl.ds(pl.multiple_of(core * rows, 8), rows), :]
    fwd = pltpu.make_async_remote_copy(src_ref=ref, dst_ref=ref, send_sem=fssem, recv_sem=frsem,
                                       device_id={"cp": sib}, device_id_type=MESH)
    fwd.start()

    slot = get_b(jnp.int32(nf - 1 + db))
    y = acc[...] + dot((a0 if (nf - 1 - s1) % 2 == 0 else a1)[...], wb[slot])
    out_ref[...] = (h[...] + mi_ref[5:6, :] * y).astype(BF16)

    fwd.wait()
    for j in range(nj):
        for r in range(1, NCHIP):
            o_copy(j, r, chip, lax.rem(chip + r, NCHIP)).wait_send()
    for r in range(1, NCHIP):
        c = lax.rem(chip + r, NCHIP)
        p_copy(r, chip, c).wait_send()
        r_copy(r, chip, c).wait_send()


def output(o_img, image, text, o_txt, g2, flat, wp, w1, w2, twp, tw1, tw2):
    tok, d = image.shape
    txt = text.shape[0]
    ff = w1.shape[1]
    nb = 512
    nf = ff // nb
    s1 = 3 if nf > 8 else 1
    s2 = 18 if nf > 8 else 4
    na = 3
    rows = txt // 2
    ft = ff // NCHIP
    nj = o_txt.shape[0]
    dma = pltpu.SemaphoreType.DMA
    flops = 2 * tok * d * (d + 2 * ff) + 2 * rows * d * (d + 2 * ft)
    return pl.pallas_call(
        functools.partial(out_kernel, (tok, txt, d, ff, s1, s2)),
        out_shape=(jax.ShapeDtypeStruct((tok, d), BF16), jax.ShapeDtypeStruct((txt, d), BF16)),
        in_specs=[ANY, ANY, ANY, VM, VM] + [VM] * 8 + [ANY] * 6,
        out_specs=(VM, VM),
        scratch_shapes=[
            pltpu.VMEM((6, d), F32), pltpu.VMEM((6, d), F32),
            pltpu.VMEM((na, d, nb), BF16), pltpu.VMEM((na, nb, d), BF16),
            pltpu.VMEM((tok, d), BF16), pltpu.VMEM((tok, d), BF16), pltpu.VMEM((tok, d), F32), pltpu.VMEM((tok, d), BF16),
            pltpu.VMEM((tok, d), F32), pltpu.VMEM((tok, nb), BF16), pltpu.VMEM((tok, nb), BF16),
            pltpu.VMEM((rows, d), BF16), pltpu.VMEM((rows, d), BF16), pltpu.VMEM((rows, d), F32), pltpu.VMEM((rows, d), BF16),
            pltpu.VMEM((rows, ft), BF16), pltpu.VMEM((rows, d), F32), pltpu.VMEM((NCHIP, rows // NCHIP, d), F32),
            pltpu.VMEM((rows // NCHIP, d), BF16),
            dma((na,)), dma((na,)), dma((3,)), dma((nj, NCHIP)), dma((nj, NCHIP)), dma((NCHIP,)), dma((NCHIP,)),
            dma((NCHIP,)), dma((NCHIP,)), dma, dma,
        ],
        compiler_params=pltpu.CompilerParams(collective_id=2, has_side_effects=True, vmem_limit_bytes=VMEM_LIMIT),
        cost_estimate=pl.CostEstimate(flops=flops, bytes_accessed=2 * d * (d + 2 * ff), transcendentals=0),
        name="out",
    )(o_img, image, text, o_txt, g2, *flat, wp, w1, w2, twp, tw1, tw2)


def rope_inputs(ids):
    d_t = HD // 8
    d_s = (HD - d_t) // 2
    widths = (d_t, d_s, d_s)
    lane = lax.broadcasted_iota(jnp.int32, (1, HD), 1)
    pos = jnp.where(lane < d_t, ids[:, 0:1], jnp.where(lane < d_t + d_s, ids[:, 1:2], ids[:, 2:3])).astype(BF16)
    omega = np.concatenate([np.repeat(THETA ** (-np.arange(0, w, 2, dtype=np.float32) / np.float32(w)), 2) for w in widths])
    return pos, jnp.asarray(omega.astype(np.float32)[None, :])


def device_fn(image, text, cond_vec, image_ids, *weights):
    (wm, bm, wqkv, bqkv, qg, kg, wp, bp, w1, b1, w2, b2) = weights[:12]
    (twm, tbm, twqkv, tbqkv, tqg, tkg, twp, tbp, tw1, tb1, tw2, tb2) = weights[12:]
    x, xt = image[0], text[0]
    pos, omega = rope_inputs(image_ids)
    o_img, o_txt, g2 = attention(x, xt, cond_vec, wm, twm, wqkv, twqkv, (bm, tbm, bqkv, tbqkv, qg, kg, tqg, tkg), pos, omega)
    image_out, text_out = output(o_img, x, xt, o_txt, g2, (bm, tbm, bp, tbp, b1, tb1, b2, tb2), wp, w1, w2, twp, tw1, tw2)
    return image_out[None], text_out[None]


def solution(mesh):
    act = P("dp", "cp", None)
    txt = P("dp", None, None)
    in_specs = (act, txt, P("dp", None), P(("dp", "cp"), None)) + (P(),) * 24
    return jax.shard_map(device_fn, mesh=mesh, in_specs=in_specs, out_specs=(act, txt), check_vma=False)
```

```python
import functools

import jax
import jax.numpy as jnp
import numpy as np
from jax import lax
from jax.experimental import pallas as pl
from jax.experimental.pallas import tpu as pltpu
from jax.sharding import PartitionSpec as P

EPS = 1e-6
THETA = 10000.0
F32 = jnp.float32
BF16 = jnp.bfloat16
HD = 128
NCHIP = 8
NDEV = 16
VM = pl.BlockSpec(memory_space=pltpu.VMEM)
ANY = pl.BlockSpec(memory_space=pl.ANY)
MESH = pl.DeviceIdType.MESH
VMEM_LIMIT = 67043328


def dot(a, b):
    return jnp.dot(a, b, preferred_element_type=F32)


def dot_t(a, b):
    return lax.dot_general(a, b, (((1,), (1,)), ((), ())), preferred_element_type=F32)


def lane_row(b_ref, start, n):
    return b_ref[pl.ds(start, n)].astype(F32).reshape(1, n)


def ln_mod_rows(x, scale1p, shift):
    xf = x.astype(F32)
    mean = jnp.mean(xf, axis=-1, keepdims=True)
    cent = xf - mean
    var = jnp.mean(cent * cent, axis=-1, keepdims=True)
    return scale1p * (cent * lax.rsqrt(var + EPS)) + shift


KINDS = (1, 2, 0)


def main_kernel(cfg, x_hbm, xt_hbm, cond_ref, wmi_hbm, wmt_hbm, wi_hbm, wt_hbm, bmi_ref, bmt_ref, bi_ref, bt_ref,
                qg_ref, kg_ref, tqg_ref, tkg_ref, pos_ref, om_ref,
                o_hbm, ot_ref, g2,
                w, xs, xm, xt, kn, kf, km, vn, vf, vm, qn, qf, qm, kb, vb, qb, posm, cos_t, se_t, so_t, cos_m, se_m, so_m,
                mi, mt, g1, mine1, mine2, s0, s1, mx0, mx1, ost, otmp,
                xsem, wsem, msend, mrecv, gsend, grecv, ssem, rsem, fssem, frsem, ossem, orsem):
    tok, txt, d_in, heads, ck, mx = cfg
    nu = tok - mx
    hd_all = heads * HD
    nj = heads // NCHIP
    quad = 4
    wide = quad * HD
    half = tok * NCHIP
    me = lax.axis_index("cp")
    chip, core = me // 2, me % 2
    zh, cl = chip // quad, chip % quad
    sib = chip * 2 + (1 - core)
    mirror_chip = lax.rem(chip + quad, NCHIP)

    def dev(c):
        return {"cp": c * 2 + core}

    barrier = pltpu.get_barrier_semaphore()
    for r in range(1, NDEV):
        pl.semaphore_signal(barrier, inc=1, device_id={"cp": lax.rem(me + r, NDEV)}, device_id_type=MESH)
    load_x = pltpu.make_async_copy(x_hbm, xs, xsem.at[0])
    load_t = pltpu.make_async_copy(xt_hbm, xt, xsem.at[1])

    def x_copy():
        return pltpu.make_async_remote_copy(
            src_ref=x_hbm.at[pl.ds(nu, mx), :], dst_ref=xm, send_sem=msend.at[0], recv_sem=mrecv.at[0],
            device_id=dev(mirror_chip), device_id_type=MESH)

    def pos_copy():
        return pltpu.make_async_remote_copy(
            src_ref=pos_ref.at[pl.ds(nu, mx), :], dst_ref=posm, send_sem=msend.at[1], recv_sem=mrecv.at[1],
            device_id=dev(mirror_chip), device_id_type=MESH)

    mc = 2 * d_in // NDEV

    def tile_copy(what, a, b, slot):
        if what == "mod":
            ref = (wmi_hbm, wmt_hbm)[a]
            off = me * mc if b < 0 else 2 * d_in + me * 2 * mc + b * mc
            return [pltpu.make_async_copy(ref.at[:, pl.ds(pl.multiple_of(off, 128), mc)], w.at[slot, :, pl.ds(0, mc)], wsem.at[slot, 0])]
        if what == "txt":
            return [pltpu.make_async_copy(
                wt_hbm.at[:, pl.ds(pl.multiple_of(a * hd_all + (j * NCHIP + chip) * HD, HD), HD)],
                w.at[slot, :, pl.ds(j * HD, HD)], wsem.at[slot, j]) for j in range(nj)]
        kind, side = a
        off = kind * hd_all + b * NCHIP * HD + (zh if side == 0 else 1 - zh) * wide
        return [pltpu.make_async_copy(wi_hbm.at[:, pl.ds(pl.multiple_of(off, wide), wide)], w.at[slot], wsem.at[slot, 0])]

    def start(*a):
        for c in tile_copy(*a):
            c.start()

    def wait(*a):
        for c in tile_copy(*a):
            c.wait()
        return a[-1]

    def start_own(j, p):
        start("img", (KINDS[p // 2], p % 2), j, (2 + p) % 3)

    def start_txt(t):
        start("txt", KINDS[t], None, (2 + t) % 3)

    def start_mir(j, i):
        start("img", (KINDS[i], 0), j, (2 + i) % 3)

    def start_mod2(t):
        start("mod", t // 2, t % 2, (2 + t) % 3)

    start("mod", 0, -1, 0)
    start("mod", 1, -1, 1)
    load_x.start()
    load_t.start()

    c = cond_ref[...].astype(F32)
    act = (c * jax.nn.sigmoid(c)).astype(BF16)
    act = jnp.broadcast_to(act, (16, d_in))
    per = mc // 128

    def mod_rows(slot, buf, row):
        r = dot(act, w[slot, :, 0:mc])
        for i in range(per):
            buf[row + i:row + i + 1, :] = r[0:1, i * 128:(i + 1) * 128]

    def spread(buf, dst, k):
        return [pltpu.make_async_remote_copy(
            src_ref=buf, dst_ref=dst.at[me], send_sem=gsend.at[k, r], recv_sem=grecv.at[k, r],
            device_id={"cp": lax.rem(me + r, NDEV)}, device_id_type=MESH) for r in range(1, NDEV)]

    mine1[...] = jnp.zeros_like(mine1)
    start_own(0, 0)
    mod_rows(wait("mod", 0, -1, 0), mine1, 0)
    start_own(0, 1)
    mod_rows(wait("mod", 1, -1, 1), mine1, per)
    pl.semaphore_wait(barrier, NDEV - 1)
    gath1 = spread(mine1, g1, 0)
    for cp in gath1:
        cp.start()
    pos_copy().start()
    x_copy().start()
    g1[me] = mine1[...]

    def tables(pos, n, cos_t, se_t, so_t):
        ang = pos.astype(F32) * om_ref[...]
        odd = lax.rem(lax.broadcasted_iota(jnp.int32, ang.shape, 1), 2) == 1
        sin = jnp.sin(ang)
        cos_t[0:n, :] = jnp.cos(ang)
        se_t[0:n, :] = jnp.where(odd, 0.0, -sin)
        so_t[0:n, :] = jnp.where(odd, sin, 0.0)

    tables(pos_ref[...], tok, cos_t, se_t, so_t)
    for b_ref, m in ((bmi_ref, mi), (bmt_ref, mt)):
        for k in range(2):
            m[k:k + 1, :] = lane_row(b_ref, k * d_in, d_in)
    for cp in gath1:
        cp.wait()
    for b, m in ((0, mi), (1, mt)):
        for dv in range(NDEV):
            for r in range(per):
                col = (dv * per + r) * 128
                at = (slice(col // d_in, col // d_in + 1), slice(col % d_in, col % d_in + 128))
                m[at] = m[at] + g1[dv, b * per + r:b * per + r + 1, :]

    rb = 16

    def ln_rows(ref, m_ref, n):
        shift = m_ref[0:1, :]
        scale = 1.0 + m_ref[1:2, :]

        def body(i, carry):
            sl = pl.ds(pl.multiple_of(i * rb, rb), rb)
            ref[sl, :] = ln_mod_rows(ref[sl, :], scale, shift).astype(BF16)
            return carry
        lax.fori_loop(0, n // rb, body, 0)

    def norm_rope(y, gain, tabs):
        ms = jnp.mean(y * y, axis=-1, keepdims=True)
        y = y * lax.rsqrt(ms + EPS) * gain
        if tabs is not None:
            n = y.shape[0]
            y = y * tabs[0][0:n, :] + pltpu.roll(y, HD - 1, 1) * tabs[1][0:n, :] + pltpu.roll(y, 1, 1) * tabs[2][0:n, :]
        return y

    def place(kind, s_chip, row, n, j):
        if kind == 0:
            return qb.at[j, pl.ds(pl.multiple_of(txt + s_chip * tok + row, 128), n)]
        at = pl.multiple_of(txt + core * half + s_chip * tok + row, 128)
        return kb.at[j, pl.ds(at, n)] if kind == 1 else vb.at[j, :, pl.ds(at, n)]

    def qkv_copy(kind, ty, j, src_cl, src_zh, dst_cl, idx):
        buf = ((qn, qf, qm), (kn, kf, km), (vn, vf, vm))[kind][ty]
        n = (tok, nu, mx)[ty]
        s_chip = src_zh * quad + src_cl
        tgt = (1 - src_zh if ty == 1 else src_zh) * quad + dst_cl
        if ty == 2:
            dst = place(kind, lax.rem(s_chip + quad, NCHIP), nu, n, j)
        else:
            dst = place(kind, s_chip, 0, n, j)
        return pltpu.make_async_remote_copy(
            src_ref=buf.at[j * quad + dst_cl], dst_ref=dst, send_sem=ssem.at[kind, ty, j, idx[0]],
            recv_sem=rsem.at[kind, ty, j, idx[1]], device_id=dev(tgt), device_id_type=MESH)

    def out_copies(kind, ty, j):
        if ty == 1:
            return [qkv_copy(kind, 1, j, cl, zh, c, (c, cl)) for c in range(quad)]
        return [qkv_copy(kind, ty, j, cl, zh, lax.rem(cl + r, quad), (r, r)) for r in range(1, quad)]

    def in_copies(kind, ty, j):
        if ty == 1:
            return [qkv_copy(kind, 1, j, c, 1 - zh, cl, (c, c)) for c in range(quad)]
        return [qkv_copy(kind, ty, j, lax.rem(cl + quad - r, quad), zh, cl, (r, r)) for r in range(1, quad)]

    def own_copy(kind, ty, j):
        buf = ((qn, qf, qm), (kn, kf, km), (vn, vf, vm))[kind][ty]
        n = (tok, nu, mx)[ty]
        dst = place(kind, mirror_chip, nu, n, j) if ty == 2 else place(kind, chip, 0, n, j)
        dst[...] = buf[j * quad + cl]

    def make(kind, ty, j, slot):
        src = xm if ty == 2 else xs
        n = (tok, nu, mx)[ty]
        buf = ((qn, qf, qm), (kn, kf, km), (vn, vf, vm))[kind][ty]

        def cols(p, carry):
            col = pl.multiple_of(p * 2 * HD, 2 * HD)
            boff = kind * hd_all + j * NCHIP * HD + (1 - zh if ty == 1 else zh) * wide + col
            y2 = dot(src[0:n, :], w[slot, :, pl.ds(col, 2 * HD)]) + lane_row(bi_ref, pl.multiple_of(boff, 256), 2 * HD)
            for hh in range(2):
                y = y2[:, hh * HD:(hh + 1) * HD]
                if kind == 2:
                    buf[j * quad + 2 * p + hh] = y.T.astype(BF16)
                else:
                    gain = (qg_ref, kg_ref)[kind][...].astype(F32).reshape(1, HD)
                    buf[j * quad + 2 * p + hh] = norm_rope(y, gain, (cos_m, se_m, so_m) if ty == 2 else (cos_t, se_t, so_t)).astype(BF16)
            return carry
        lax.fori_loop(0, 2, cols, 0)

    load_x.wait()
    ln_rows(xs, mi, tok)

    def own_pass(j, after):
        for p in range(6):
            kind, side = KINDS[p // 2], p % 2
            if p + 2 < 6:
                start_own(j, p + 2)
            else:
                after(p - 4)
            slot = wait("img", (kind, side), j, (2 + p) % 3)
            make(kind, side, j, slot)
            for cp in out_copies(kind, side, j):
                cp.start()
            if side == 0:
                own_copy(kind, 0, j)

    own_pass(0, start_txt)

    load_t.wait()
    ln_rows(xt, mt, txt)
    for t, kind in enumerate(KINDS):
        if t == 0:
            start_txt(2)
        else:
            start_mir(0, t - 1)
        slot = wait("txt", kind, None, (2 + t) % 3)
        y3 = dot(xt[...], w[slot, :, 0:nj * HD])
        for j in range(nj):
            pair0 = kind * hd_all + (j * NCHIP + chip - lax.rem(chip, 2)) * HD
            b2 = lane_row(bt_ref, pl.multiple_of(pair0, 256), 2 * HD)
            y = y3[:, j * HD:(j + 1) * HD] + jnp.where(lax.rem(chip, 2) == 0, b2[:, 0:HD], b2[:, HD:2 * HD])
            if kind == 2:
                vb[j, :, 0:txt] = y.T.astype(BF16)
            else:
                gain = (tqg_ref, tkg_ref)[kind][...].astype(F32).reshape(1, HD)
                (qb, kb)[kind][j, 0:txt] = norm_rope(y, gain, None).astype(BF16)

    pos_copy().wait_recv()
    tables(posm[...], mx, cos_m, se_m, so_m)
    x_copy().wait_recv()
    ln_rows(xm, mi, mx)

    def after_mir(p):
        if nj > 1:
            start_own(1, p)
        else:
            start_mod2(p)

    def mir_pass(j, carry):
        for i, kind in enumerate(KINDS):
            if i == 0:
                start_mir(j, 2)
            else:
                @pl.when(j < nj - 1)
                def _():
                    start_mir(j + 1, i - 1)

                @pl.when(j == nj - 1)
                def _():
                    after_mir(i - 1)
            slot = wait("img", (kind, 0), j, (2 + i) % 3)
            make(kind, 2, j, slot)
            for cp in out_copies(kind, 2, j):
                cp.start()
            own_copy(kind, 2, j)
        return carry
    lax.fori_loop(0, nj, mir_pass, 0)

    def rest_pass(j, carry):
        def after(p):
            @pl.when(j < nj - 1)
            def _():
                start_own(j + 1, p)

            @pl.when(j == nj - 1)
            def _():
                start_mod2(p)
        own_pass(j, after)
        return carry
    if nj > 1:
        lax.fori_loop(1, nj, rest_pass, 0)

    mine2[...] = jnp.zeros_like(mine2)
    for t in range(4):
        if t + 2 < 4:
            start_mod2(t + 2)
        mod_rows(wait("mod", t // 2, t % 2, (2 + t) % 3), mine2, t * per)
    gath2 = spread(mine2, g2, 1)
    for cp in gath2:
        cp.start()
    g2[me] = mine2[...]

    scale2 = (HD ** -0.5) * 1.4426950408889634
    keys = txt + 2 * half
    nchunk = keys // ck
    qt = 256
    ntile = (txt + half) // qt
    group = 2 * tok // qt
    ngroup = NCHIP // 2

    def to_sibling(kind, j):
        ref = (kb.at[j, pl.ds(pl.multiple_of(txt + core * half, 128), half)] if kind == 1
               else vb.at[j, :, pl.ds(pl.multiple_of(txt + core * half, 128), half)])
        return pltpu.make_async_remote_copy(
            src_ref=ref, dst_ref=ref, send_sem=fssem.at[kind - 1, j], recv_sem=frsem.at[kind - 1, j],
            device_id={"cp": sib}, device_id_type=MESH)

    def collect(j):
        for kind in KINDS:
            for ty in range(3):
                for cp in in_copies(kind, ty, j):
                    cp.wait_recv()
            if kind != 0:
                to_sibling(kind, j).start()

    def tile_start(t):
        g = (t - 1) // group
        plane = lax.rem(chip // 2 + 1 + g, ngroup)
        row = txt + plane * (2 * tok) + lax.rem(t - 1, group) * qt
        return pl.multiple_of(jnp.where(t == 0, 0, row), 128)

    def qk(j, q, i, s_ref, mxv):
        sl = pl.ds(pl.multiple_of(i * ck, ck), ck)
        s = dot_t(kb[j, sl], q)
        s_ref[sl, :] = s
        return jnp.maximum(mxv, jnp.max(s.reshape(ck // 8, 8, qt), axis=0))

    def sm(j, i, s_ref, m, lsum, acc):
        sl = pl.ds(pl.multiple_of(i * ck, ck), ck)
        p = jnp.exp2((s_ref[sl, :] - m) * scale2)
        lsum = lsum + jnp.sum(p.reshape(ck // 8, 8, qt), axis=0)
        acc = acc + dot(vb[j, :, sl], p.astype(BF16))
        return lsum, acc

    def new_max():
        return jnp.full((8, qt), -jnp.inf, F32)

    def o_remote(j, c_src, c_dst):
        src = ost.at[j, pl.ds(pl.multiple_of(c_dst * tok, 128), tok)]
        dst = o_hbm.at[:, pl.ds(pl.multiple_of((j * NCHIP + c_src) * HD, HD), HD)]
        return pltpu.make_async_remote_copy(
            src_ref=src, dst_ref=dst, send_sem=ossem.at[j, c_dst], recv_sem=orsem.at[j, c_src],
            device_id=dev(c_dst), device_id_type=MESH)

    def o_local(j):
        src = ost.at[j, pl.ds(pl.multiple_of(chip * tok, 128), tok)]
        dst = o_hbm.at[:, pl.ds(pl.multiple_of((j * NCHIP + chip) * HD, HD), HD)]
        return pltpu.make_async_copy(src, dst, ossem.at[j, chip])

    def o_send(j, g):
        plane = lax.rem(chip // 2 + 1 + g, ngroup)
        for y in range(2):
            c = plane * 2 + y

            @pl.when(c != chip)
            def _():
                o_remote(j, chip, c).start()

            @pl.when(c == chip)
            def _():
                o_local(j).start()

    def finish(j, t, lsum, acc):
        tot = jnp.sum(lsum, axis=0, keepdims=True)
        o = (acc / tot).T.astype(BF16)

        @pl.when(t == 0)
        def _():
            otmp[...] = o
            ot_ref[j] = otmp[pl.ds(pl.multiple_of(core * (txt // 2), 8), txt // 2), :]

        @pl.when(t > 0)
        def _():
            ost[j, pl.ds(pl.multiple_of(tile_start(t) - txt, 128), qt)] = o

            @pl.when(lax.rem(t, group) == 0)
            def _():
                o_send(j, t // group - 1)

    def pair(j, t, s_cur, mx_cur, s_nxt, mx_nxt, has_next):
        m = jnp.max(mx_cur[...], axis=0, keepdims=True)
        lsum = jnp.zeros((8, qt), F32)
        acc = jnp.zeros((HD, qt), F32)
        if has_next:
            q = qb[j, pl.ds(tile_start(t + 1), qt)]

            def body(i, carry):
                lsum, acc, mxv = carry
                mxv = qk(j, q, i, s_nxt, mxv)
                lsum, acc = sm(j, i, s_cur, m, lsum, acc)
                return lsum, acc, mxv
            lsum, acc, mxv = lax.fori_loop(0, nchunk, body, (lsum, acc, new_max()))
            mx_nxt[...] = mxv
        else:
            def body(i, carry):
                return sm(j, i, s_cur, m, *carry)
            lsum, acc = lax.fori_loop(0, nchunk, body, (lsum, acc))
        finish(j, t, lsum, acc)

    collect(0)

    def head(j, carry):
        for kind in (1, 2):
            to_sibling(kind, j).wait()
        q = qb[j, 0:qt]

        def first(i, mxv):
            return qk(j, q, i, s0, mxv)
        mx0[...] = lax.fori_loop(0, nchunk, first, new_max())

        def two(i, carry):
            pair(j, 2 * i, s0, mx0, s1, mx1, True)
            pair(j, 2 * i + 1, s1, mx1, s0, mx0, True)
            return carry
        lax.fori_loop(0, (ntile - 1) // 2, two, 0)
        if nj > 1:
            @pl.when(j < nj - 1)
            def _():
                collect(j + 1)
        pair(j, jnp.int32(ntile - 1), s0, mx0, s1, mx1, False)
        return carry
    lax.fori_loop(0, nj, head, 0)

    for cp in gath2:
        cp.wait()
    x_copy().wait_send()
    pos_copy().wait_send()

    def drain(j, carry):
        for kind in KINDS:
            for ty in range(3):
                for cp in out_copies(kind, ty, j):
                    cp.wait_send()
        o_local(j).wait()
        for r in range(1, NCHIP):
            c = lax.rem(chip + r, NCHIP)
            o_remote(j, chip, c).wait_send()
            o_remote(j, c, chip).wait_recv()
        return carry
    lax.fori_loop(0, nj, drain, 0)


def attention(image, text, cond_vec, wm_img, wm_txt, w_img, w_txt, flat, pos, omega):
    tok, d_in = image.shape
    txt = text.shape[0]
    hd_all = w_img.shape[1] // 3
    heads = hd_all // HD
    nj = heads // NCHIP
    half = tok * NCHIP
    keys = txt + 2 * half
    ck = 3200
    mx = 128
    nu = tok - mx
    cfg = (tok, txt, d_in, heads, ck, mx)
    dma = pltpu.SemaphoreType.DMA
    flops = 2 * tok * d_in * 3 * hd_all + 4 * nj * HD * (half + txt) * keys
    per = 2 * d_in // NDEV // 128
    r1, r2 = -(-2 * per // 8) * 8, -(-4 * per // 8) * 8
    row_sets = [pltpu.VMEM((nj * 4, n, HD), BF16) for n in (tok, nu, mx)]
    col_sets = [pltpu.VMEM((nj * 4, HD, n), BF16) for n in (tok, nu, mx)]
    table = pltpu.VMEM((tok, 128), F32)
    return pl.pallas_call(
        functools.partial(main_kernel, cfg),
        out_shape=(jax.ShapeDtypeStruct((tok, hd_all), BF16), jax.ShapeDtypeStruct((nj, txt // 2, HD), BF16),
                   jax.ShapeDtypeStruct((NDEV, r2, 128), F32)),
        in_specs=[ANY, ANY, VM, ANY, ANY, ANY, ANY] + [VM] * 10,
        out_specs=(ANY, VM, VM),
        scratch_shapes=[
            pltpu.VMEM((3, d_in, 4 * HD), BF16),
            pltpu.VMEM((tok, d_in), BF16), pltpu.VMEM((mx, d_in), BF16), pltpu.VMEM((txt, d_in), BF16),
            *row_sets, *col_sets, *row_sets,
            pltpu.VMEM((nj, keys, HD), BF16), pltpu.VMEM((nj, HD, keys), BF16), pltpu.VMEM((nj, txt + half, HD), BF16),
            pltpu.VMEM((mx, 128), BF16), table, table, table, *[pltpu.VMEM((mx, 128), F32)] * 3,
            pltpu.VMEM((2, d_in), F32), pltpu.VMEM((2, d_in), F32),
            pltpu.VMEM((NDEV, r1, 128), F32), pltpu.VMEM((r1, 128), F32), pltpu.VMEM((r2, 128), F32),
            pltpu.VMEM((keys, 256), F32), pltpu.VMEM((keys, 256), F32), pltpu.VMEM((8, 256), F32), pltpu.VMEM((8, 256), F32),
            pltpu.VMEM((nj, half, HD), BF16), pltpu.VMEM((txt, HD), BF16),
            dma((2,)), dma((3, max(nj, 1))), dma((2,)), dma((2,)), dma((2, NDEV)), dma((2, NDEV)),
            dma((3, 3, nj, 4)), dma((3, 3, nj, 4)), dma((2, nj)), dma((2, nj)), dma((nj, NCHIP)), dma((nj, NCHIP)),
        ],
        compiler_params=pltpu.CompilerParams(collective_id=1, has_side_effects=True, vmem_limit_bytes=VMEM_LIMIT),
        cost_estimate=pl.CostEstimate(flops=flops, bytes_accessed=3 * d_in * 3 * hd_all, transcendentals=0),
        name="attn",
    )(image, text, cond_vec, wm_img, wm_txt, w_img, w_txt, *flat, pos, omega)


def gelu(x):
    return x * (0.5 * (1.0 + jnp.tanh(0.7978845608028654 * (x + 0.044715 * (x * x * x)))))


def out_kernel(cfg, o_hbm, x_hbm, xt_hbm, ot_ref, g2_ref, bmi_ref, bmt_ref, bp_ref, tbp_ref, b1_ref, tb1_ref, b2_ref, tb2_ref, wp_hbm, w1_hbm, w2_hbm, twp_hbm, tw1_hbm, tw2_hbm,
               out_ref, tout_ref, mi_ref, mt_ref,
               wa, wb, o, x, h, z, acc, a0, a1, o_t, x_t, h_t, z_t, a_t, part, rs, row,
               asem, bsem, lsem, ossem, orsem, pssem, prsem, rssem, rrsem, fssem, frsem):
    tok, txt, d, ff, s1, s2 = cfg
    me = lax.axis_index("cp")
    chip, core = me // 2, me % 2
    sib = chip * 2 + (1 - core)
    rows = txt // 2
    piece = rows // NCHIP
    nb = wa.shape[2]
    na = wa.shape[0]
    np_ = d // nb
    nf = ff // nb
    ft = ff // NCHIP
    nt = ft // nb
    nj = ot_ref.shape[0]

    def dev(c):
        return {"cp": c * 2 + core}

    off = pl.multiple_of(chip * ft, nb)
    segs_a = ((np_, wp_hbm, 0), (s1, w1_hbm, 0), (np_, twp_hbm, 0), (nt, tw1_hbm, off), (nf - s1, w1_hbm, s1 * nb))
    segs_b = ((s1, w2_hbm, 0), (nt, tw2_hbm, off), (nf - s1, w2_hbm, s1 * nb))

    def start(p, segs, is_a):
        lo = 0
        for n, ref, base in segs:
            @pl.when((p >= lo) & (p < lo + n))
            def _(lo=lo, ref=ref, base=base):
                sl = pl.ds(pl.multiple_of(base + (p - lo) * nb, nb), nb)
                slot = lax.rem(p, na)
                if is_a:
                    pltpu.make_async_copy(ref.at[:, sl], wa.at[slot], asem.at[slot]).start()
                else:
                    pltpu.make_async_copy(ref.at[sl, :], wb.at[slot], bsem.at[slot]).start()
            lo += n

    def get_a(p):
        start(p + na - 1, segs_a, True)
        slot = lax.rem(p, na)
        pltpu.make_async_copy(w1_hbm.at[:, 0:nb], wa.at[slot], asem.at[slot]).wait()
        return slot

    def get_b(p):
        start(p + na - 1, segs_b, False)
        slot = lax.rem(p, na)
        pltpu.make_async_copy(w2_hbm.at[0:nb, :], wb.at[slot], bsem.at[slot]).wait()
        return slot

    load_o = pltpu.make_async_copy(o_hbm, o, lsem.at[0])
    load_x = pltpu.make_async_copy(x_hbm, x, lsem.at[1])
    load_t = pltpu.make_async_copy(xt_hbm.at[pl.ds(pl.multiple_of(core * rows, 8), rows), :], x_t, lsem.at[2])
    load_o.start()
    start(jnp.int32(0), segs_a, True)
    load_x.start()
    for p in range(1, na - 1):
        start(jnp.int32(p), segs_a, True)
    for p in range(na - 1):
        start(jnp.int32(p), segs_b, False)
    load_t.start()

    barrier = pltpu.get_barrier_semaphore()
    for r in range(1, NCHIP):
        pl.semaphore_signal(barrier, inc=1, device_id=dev(lax.rem(chip + r, NCHIP)), device_id_type=MESH)
    pl.semaphore_signal(barrier, inc=1, device_id={"cp": sib}, device_id_type=MESH)
    pl.semaphore_wait(barrier, NCHIP)

    def o_copy(j, r, c_src, c_dst):
        return pltpu.make_async_remote_copy(
            src_ref=ot_ref.at[j], dst_ref=o_t.at[:, pl.ds(pl.multiple_of((j * NCHIP + c_src) * HD, HD), HD)],
            send_sem=ossem.at[j, r], recv_sem=orsem.at[j, r], device_id=dev(c_dst), device_id_type=MESH)

    for j in range(nj):
        for r in range(1, NCHIP):
            o_copy(j, r, chip, lax.rem(chip + r, NCHIP)).start()
        o_t[:, pl.ds(pl.multiple_of((j * NCHIP + chip) * HD, HD), HD)] = ot_ref[j]

    per = 4 * d // NDEV // 128
    for b, (b_ref, m) in enumerate(((bmi_ref, mi_ref), (bmt_ref, mt_ref))):
        for k in range(2, 6):
            m[k:k + 1, :] = lane_row(b_ref, k * d, d)
        for dv in range(NDEV):
            for r in range(per):
                col = 2 * d + (dv * per + r) * 128
                at = (slice(col // d, col // d + 1), slice(col % d, col % d + 128))
                m[at] = m[at] + g2_ref[dv, b * per + r:b * per + r + 1, :]

    load_o.wait()
    load_x.wait()

    def proj(p, carry):
        slot = get_a(p)
        sl = pl.ds(pl.multiple_of(p * nb, nb), nb)
        y = dot(o[...], wa[slot]) + lane_row(bp_ref, pl.multiple_of(p * nb, nb), nb)
        h[:, sl] = x[:, sl].astype(F32) + mi_ref[2:3, sl] * y
        return carry
    lax.fori_loop(0, np_, proj, 0)

    def ln2(src, dst, m_ref, n):
        shift, scale = m_ref[3:4, :], 1.0 + m_ref[4:5, :]
        rb = 16

        def body(i, carry):
            r = pl.ds(pl.multiple_of(i * rb, rb), rb)
            dst[r, :] = ln_mod_rows(src[r, :], scale, shift).astype(BF16)
            return carry
        lax.fori_loop(0, n // rb, body, 0)

    ln2(h, z, mi_ref, tok)
    acc[...] = jnp.broadcast_to(lane_row(b2_ref, 0, d), acc.shape)

    def mlp(i, pa, pb, a_new, a_old):
        slot_b = get_b(pb)
        slot_a = get_a(pa)
        a_new[...] = gelu(dot(z[...], wa[slot_a]) + lane_row(b1_ref, pl.multiple_of(i * nb, nb), nb)).astype(BF16)
        acc[...] += dot(a_old[...], wb[slot_b])

    def mlp_range(lo, hi, da, db):
        def two(k, carry):
            i = lo + 2 * k
            mlp(i, i + da, i - 1 + db, a1, a0)
            mlp(i + 1, i + 1 + da, i + db, a0, a1)
            return carry
        lax.fori_loop(0, (hi - lo) // 2, two, 0)

    slot = get_a(jnp.int32(np_))
    a0[...] = gelu(dot(z[...], wa[slot]) + lane_row(b1_ref, 0, nb)).astype(BF16)
    mlp_range(1, s1, np_, 0)
    slot = get_b(jnp.int32(s1 - 1))
    acc[...] += dot(a0[...], wb[slot])

    load_t.wait()
    for j in range(nj):
        for r in range(1, NCHIP):
            o_copy(j, r, lax.rem(chip + NCHIP - r, NCHIP), chip).wait_recv()
    pa = np_ + s1

    def tproj(k, carry):
        slot = get_a(pa + k)
        sl = pl.ds(pl.multiple_of(k * nb, nb), nb)
        y = dot(o_t[...], wa[slot]) + lane_row(tbp_ref, pl.multiple_of(k * nb, nb), nb)
        h_t[:, sl] = x_t[:, sl].astype(F32) + mt_ref[2:3, sl] * y
        return carry
    lax.fori_loop(0, np_, tproj, 0)
    ln2(h_t, z_t, mt_ref, rows)

    for k in range(nt):
        slot = get_a(jnp.int32(pa + np_ + k))
        y = dot(z_t[...], wa[slot]) + lane_row(tb1_ref, pl.multiple_of(off + k * nb, nb), nb)
        a_t[:, k * nb:(k + 1) * nb] = gelu(y).astype(BF16)
    for k in range(nt):
        slot = get_b(jnp.int32(s1 + k))
        y = dot(a_t[:, k * nb:(k + 1) * nb], wb[slot])
        part[...] = y if k == 0 else part[...] + y

    def p_copy(r, c_src, c_dst):
        return pltpu.make_async_remote_copy(
            src_ref=part.at[pl.ds(pl.multiple_of(c_dst * piece, 8), piece), :], dst_ref=rs.at[c_src],
            send_sem=pssem.at[r], recv_sem=prsem.at[r], device_id=dev(c_dst), device_id_type=MESH)

    for r in range(1, NCHIP):
        p_copy(r, chip, lax.rem(chip + r, NCHIP)).start()
    mine = pl.ds(pl.multiple_of(chip * piece, 8), piece)
    rs[chip] = part[mine, :]

    da, db = np_ + np_ + nt, nt
    slot = get_a(jnp.int32(s1 + da))
    a0[...] = gelu(dot(z[...], wa[slot]) + lane_row(b1_ref, s1 * nb, nb)).astype(BF16)
    mlp_range(s1 + 1, s2, da, db)

    for r in range(1, NCHIP):
        p_copy(r, lax.rem(chip + NCHIP - r, NCHIP), chip).wait_recv()
    tot = rs[0]
    for c in range(1, NCHIP):
        tot = tot + rs[c]
    y = h_t[mine, :] + mt_ref[5:6, :] * (tot + lane_row(tb2_ref, 0, d))
    row[...] = y.astype(BF16)

    def r_copy(r, c_src, c_dst):
        return pltpu.make_async_remote_copy(
            src_ref=row, dst_ref=tout_ref.at[pl.ds(pl.multiple_of(core * rows + c_src * piece, 8), piece), :],
            send_sem=rssem.at[r], recv_sem=rrsem.at[r], device_id=dev(c_dst), device_id_type=MESH)

    for r in range(1, NCHIP):
        r_copy(r, chip, lax.rem(chip + r, NCHIP)).start()
    tout_ref[pl.ds(pl.multiple_of(core * rows + chip * piece, 8), piece), :] = row[...]

    mlp_range(s2, nf, da, db)

    for r in range(1, NCHIP):
        r_copy(r, lax.rem(chip + NCHIP - r, NCHIP), chip).wait_recv()
    ref = tout_ref.at[pl.ds(pl.multiple_of(core * rows, 8), rows), :]
    fwd = pltpu.make_async_remote_copy(src_ref=ref, dst_ref=ref, send_sem=fssem, recv_sem=frsem,
                                       device_id={"cp": sib}, device_id_type=MESH)
    fwd.start()

    slot = get_b(jnp.int32(nf - 1 + db))
    y = acc[...] + dot((a0 if (nf - 1 - s1) % 2 == 0 else a1)[...], wb[slot])
    out_ref[...] = (h[...] + mi_ref[5:6, :] * y).astype(BF16)

    fwd.wait()
    for j in range(nj):
        for r in range(1, NCHIP):
            o_copy(j, r, chip, lax.rem(chip + r, NCHIP)).wait_send()
    for r in range(1, NCHIP):
        c = lax.rem(chip + r, NCHIP)
        p_copy(r, chip, c).wait_send()
        r_copy(r, chip, c).wait_send()


def output(o_img, image, text, o_txt, g2, flat, wp, w1, w2, twp, tw1, tw2):
    tok, d = image.shape
    txt = text.shape[0]
    ff = w1.shape[1]
    nb = 512
    nf = ff // nb
    s1 = 3 if nf > 8 else 1
    s2 = 18 if nf > 8 else 4
    na = 3
    rows = txt // 2
    ft = ff // NCHIP
    nj = o_txt.shape[0]
    dma = pltpu.SemaphoreType.DMA
    flops = 2 * tok * d * (d + 2 * ff) + 2 * rows * d * (d + 2 * ft)
    return pl.pallas_call(
        functools.partial(out_kernel, (tok, txt, d, ff, s1, s2)),
        out_shape=(jax.ShapeDtypeStruct((tok, d), BF16), jax.ShapeDtypeStruct((txt, d), BF16)),
        in_specs=[ANY, ANY, ANY, VM, VM] + [VM] * 8 + [ANY] * 6,
        out_specs=(VM, VM),
        scratch_shapes=[
            pltpu.VMEM((6, d), F32), pltpu.VMEM((6, d), F32),
            pltpu.VMEM((na, d, nb), BF16), pltpu.VMEM((na, nb, d), BF16),
            pltpu.VMEM((tok, d), BF16), pltpu.VMEM((tok, d), BF16), pltpu.VMEM((tok, d), F32), pltpu.VMEM((tok, d), BF16),
            pltpu.VMEM((tok, d), F32), pltpu.VMEM((tok, nb), BF16), pltpu.VMEM((tok, nb), BF16),
            pltpu.VMEM((rows, d), BF16), pltpu.VMEM((rows, d), BF16), pltpu.VMEM((rows, d), F32), pltpu.VMEM((rows, d), BF16),
            pltpu.VMEM((rows, ft), BF16), pltpu.VMEM((rows, d), F32), pltpu.VMEM((NCHIP, rows // NCHIP, d), F32),
            pltpu.VMEM((rows // NCHIP, d), BF16),
            dma((na,)), dma((na,)), dma((3,)), dma((nj, NCHIP)), dma((nj, NCHIP)), dma((NCHIP,)), dma((NCHIP,)),
            dma((NCHIP,)), dma((NCHIP,)), dma, dma,
        ],
        compiler_params=pltpu.CompilerParams(collective_id=2, has_side_effects=True, vmem_limit_bytes=VMEM_LIMIT),
        cost_estimate=pl.CostEstimate(flops=flops, bytes_accessed=2 * d * (d + 2 * ff), transcendentals=0),
        name="out",
    )(o_img, image, text, o_txt, g2, *flat, wp, w1, w2, twp, tw1, tw2)


def rope_inputs(ids):
    d_t = HD // 8
    d_s = (HD - d_t) // 2
    widths = (d_t, d_s, d_s)
    lane = lax.broadcasted_iota(jnp.int32, (1, HD), 1)
    pos = jnp.where(lane < d_t, ids[:, 0:1], jnp.where(lane < d_t + d_s, ids[:, 1:2], ids[:, 2:3])).astype(BF16)
    omega = np.concatenate([np.repeat(THETA ** (-np.arange(0, w, 2, dtype=np.float32) / np.float32(w)), 2) for w in widths])
    return pos, jnp.asarray(omega.astype(np.float32)[None, :])


def device_fn(image, text, cond_vec, image_ids, *weights):
    (wm, bm, wqkv, bqkv, qg, kg, wp, bp, w1, b1, w2, b2) = weights[:12]
    (twm, tbm, twqkv, tbqkv, tqg, tkg, twp, tbp, tw1, tb1, tw2, tb2) = weights[12:]
    x, xt = image[0], text[0]
    pos, omega = rope_inputs(image_ids)
    o_img, o_txt, g2 = attention(x, xt, cond_vec, wm, twm, wqkv, twqkv, (bm, tbm, bqkv, tbqkv, qg, kg, tqg, tkg), pos, omega)
    image_out, text_out = output(o_img, x, xt, o_txt, g2, (bm, tbm, bp, tbp, b1, tb1, b2, tb2), wp, w1, w2, twp, tw1, tw2)
    return image_out[None], text_out[None]


def solution(mesh):
    act = P("dp", "cp", None)
    txt = P("dp", None, None)
    in_specs = (act, txt, P("dp", None), P(("dp", "cp"), None)) + (P(),) * 24
    return jax.shard_map(device_fn, mesh=mesh, in_specs=in_specs, out_specs=(act, txt), check_vma=False)
```

```python
import functools

import jax
import jax.numpy as jnp
import numpy as np
from jax import lax
from jax.experimental import pallas as pl
from jax.experimental.pallas import tpu as pltpu
from jax.sharding import PartitionSpec as P

EPS = 1e-6
THETA = 10000.0
F32 = jnp.float32
BF16 = jnp.bfloat16
HD = 128
NCHIP = 8
NDEV = 16
VM = pl.BlockSpec(memory_space=pltpu.VMEM)
ANY = pl.BlockSpec(memory_space=pl.ANY)
MESH = pl.DeviceIdType.MESH
VMEM_LIMIT = 67043328


def dot(a, b):
    return jnp.dot(a, b, preferred_element_type=F32)


def dot_t(a, b):
    return lax.dot_general(a, b, (((1,), (1,)), ((), ())), preferred_element_type=F32)


def lane_row(b_ref, start, n):
    return b_ref[pl.ds(start, n)].astype(F32).reshape(1, n)


def ln_mod_rows(x, scale1p, shift):
    xf = x.astype(F32)
    mean = jnp.mean(xf, axis=-1, keepdims=True)
    cent = xf - mean
    var = jnp.mean(cent * cent, axis=-1, keepdims=True)
    return scale1p * (cent * lax.rsqrt(var + EPS)) + shift


KINDS = (1, 2, 0)


def main_kernel(cfg, x_hbm, xt_hbm, cond_ref, wmi_hbm, wmt_hbm, wi_hbm, wt_hbm, bmi_ref, bmt_ref, bi_ref, bt_ref,
                qg_ref, kg_ref, tqg_ref, tkg_ref, pos_ref, om_ref,
                o_hbm, ot_ref, g2,
                w, xs, xm, xt, kn, kf, km, vn, vf, vm, qn, qf, qm, kb, vb, qb, posm, cos_t, se_t, so_t, cos_m, se_m, so_m,
                mi, mt, g1, mine1, mine2, s0, s1, mx0, mx1, ost, otmp,
                xsem, wsem, msend, mrecv, gsend, grecv, ssem, rsem, fssem, frsem, ossem, orsem):
    tok, txt, d_in, heads, ck, mx = cfg
    nu = tok - mx
    hd_all = heads * HD
    nj = heads // NCHIP
    quad = 4
    wide = quad * HD
    half = tok * NCHIP
    me = lax.axis_index("cp")
    chip, core = me // 2, me % 2
    zh, cl = chip // quad, chip % quad
    sib = chip * 2 + (1 - core)
    mirror_chip = lax.rem(chip + quad, NCHIP)

    def dev(c):
        return {"cp": c * 2 + core}

    barrier = pltpu.get_barrier_semaphore()
    for r in range(1, NDEV):
        pl.semaphore_signal(barrier, inc=1, device_id={"cp": lax.rem(me + r, NDEV)}, device_id_type=MESH)
    load_x = pltpu.make_async_copy(x_hbm, xs, xsem.at[0])
    load_t = pltpu.make_async_copy(xt_hbm, xt, xsem.at[1])

    def x_copy():
        return pltpu.make_async_remote_copy(
            src_ref=x_hbm.at[pl.ds(nu, mx), :], dst_ref=xm, send_sem=msend.at[0], recv_sem=mrecv.at[0],
            device_id=dev(mirror_chip), device_id_type=MESH)

    def pos_copy():
        return pltpu.make_async_remote_copy(
            src_ref=pos_ref.at[pl.ds(nu, mx), :], dst_ref=posm, send_sem=msend.at[1], recv_sem=mrecv.at[1],
            device_id=dev(mirror_chip), device_id_type=MESH)

    mc = 2 * d_in // NDEV

    def tile_copy(what, a, b, slot):
        if what == "mod":
            ref = (wmi_hbm, wmt_hbm)[a]
            off = me * mc if b < 0 else 2 * d_in + me * 2 * mc + b * mc
            return [pltpu.make_async_copy(ref.at[:, pl.ds(pl.multiple_of(off, 128), mc)], w.at[slot, :, pl.ds(0, mc)], wsem.at[slot, 0])]
        if what == "txt":
            return [pltpu.make_async_copy(
                wt_hbm.at[:, pl.ds(pl.multiple_of(a * hd_all + (j * NCHIP + chip) * HD, HD), HD)],
                w.at[slot, :, pl.ds(j * HD, HD)], wsem.at[slot, j]) for j in range(nj)]
        kind, side = a
        off = kind * hd_all + b * NCHIP * HD + (zh if side == 0 else 1 - zh) * wide
        return [pltpu.make_async_copy(wi_hbm.at[:, pl.ds(pl.multiple_of(off, wide), wide)], w.at[slot], wsem.at[slot, 0])]

    def start(*a):
        for c in tile_copy(*a):
            c.start()

    def wait(*a):
        for c in tile_copy(*a):
            c.wait()
        return a[-1]

    def start_own(j, p):
        start("img", (KINDS[p // 2], p % 2), j, (2 + p) % 3)

    def start_txt(t):
        start("txt", KINDS[t], None, (2 + t) % 3)

    def start_mir(j, i):
        start("img", (KINDS[i], 0), j, (2 + i) % 3)

    def start_mod2(t):
        start("mod", t // 2, t % 2, (2 + t) % 3)

    start("mod", 0, -1, 0)
    start("mod", 1, -1, 1)
    load_x.start()
    load_t.start()

    c = cond_ref[...].astype(F32)
    act = (c * jax.nn.sigmoid(c)).astype(BF16)
    act = jnp.broadcast_to(act, (16, d_in))
    per = mc // 128

    def mod_rows(slot, buf, row):
        r = dot(act, w[slot, :, 0:mc])
        for i in range(per):
            buf[row + i:row + i + 1, :] = r[0:1, i * 128:(i + 1) * 128]

    def spread(buf, dst, k):
        return [pltpu.make_async_remote_copy(
            src_ref=buf, dst_ref=dst.at[me], send_sem=gsend.at[k, r], recv_sem=grecv.at[k, r],
            device_id={"cp": lax.rem(me + r, NDEV)}, device_id_type=MESH) for r in range(1, NDEV)]

    mine1[...] = jnp.zeros_like(mine1)
    start_own(0, 0)
    mod_rows(wait("mod", 0, -1, 0), mine1, 0)
    start_own(0, 1)
    mod_rows(wait("mod", 1, -1, 1), mine1, per)
    pl.semaphore_wait(barrier, NDEV - 1)
    gath1 = spread(mine1, g1, 0)
    for cp in gath1:
        cp.start()
    pos_copy().start()
    x_copy().start()
    g1[me] = mine1[...]

    def tables(pos, n, cos_t, se_t, so_t):
        ang = pos.astype(F32) * om_ref[...]
        odd = lax.rem(lax.broadcasted_iota(jnp.int32, ang.shape, 1), 2) == 1
        sin = jnp.sin(ang)
        cos_t[0:n, :] = jnp.cos(ang)
        se_t[0:n, :] = jnp.where(odd, 0.0, -sin)
        so_t[0:n, :] = jnp.where(odd, sin, 0.0)

    tables(pos_ref[...], tok, cos_t, se_t, so_t)
    for b_ref, m in ((bmi_ref, mi), (bmt_ref, mt)):
        for k in range(2):
            m[k:k + 1, :] = lane_row(b_ref, k * d_in, d_in)
    for cp in gath1:
        cp.wait()
    for b, m in ((0, mi), (1, mt)):
        for dv in range(NDEV):
            for r in range(per):
                col = (dv * per + r) * 128
                at = (slice(col // d_in, col // d_in + 1), slice(col % d_in, col % d_in + 128))
                m[at] = m[at] + g1[dv, b * per + r:b * per + r + 1, :]

    rb = 16

    def ln_rows(ref, m_ref, n):
        shift = m_ref[0:1, :]
        scale = 1.0 + m_ref[1:2, :]

        def body(i, carry):
            sl = pl.ds(pl.multiple_of(i * rb, rb), rb)
            ref[sl, :] = ln_mod_rows(ref[sl, :], scale, shift).astype(BF16)
            return carry
        lax.fori_loop(0, n // rb, body, 0)

    def norm_rope(y, gain, tabs):
        ms = jnp.mean(y * y, axis=-1, keepdims=True)
        y = y * lax.rsqrt(ms + EPS) * gain
        if tabs is not None:
            n = y.shape[0]
            y = y * tabs[0][0:n, :] + pltpu.roll(y, HD - 1, 1) * tabs[1][0:n, :] + pltpu.roll(y, 1, 1) * tabs[2][0:n, :]
        return y

    def place(kind, s_chip, row, n, j):
        if kind == 0:
            return qb.at[j, pl.ds(pl.multiple_of(txt + s_chip * tok + row, 128), n)]
        at = pl.multiple_of(txt + core * half + s_chip * tok + row, 128)
        return kb.at[j, pl.ds(at, n)] if kind == 1 else vb.at[j, :, pl.ds(at, n)]

    def qkv_copy(kind, ty, j, src_cl, src_zh, dst_cl, idx):
        buf = ((qn, qf, qm), (kn, kf, km), (vn, vf, vm))[kind][ty]
        n = (tok, nu, mx)[ty]
        s_chip = src_zh * quad + src_cl
        tgt = (1 - src_zh if ty == 1 else src_zh) * quad + dst_cl
        if ty == 2:
            dst = place(kind, lax.rem(s_chip + quad, NCHIP), nu, n, j)
        else:
            dst = place(kind, s_chip, 0, n, j)
        return pltpu.make_async_remote_copy(
            src_ref=buf.at[j * quad + dst_cl], dst_ref=dst, send_sem=ssem.at[kind, ty, j, idx[0]],
            recv_sem=rsem.at[kind, ty, j, idx[1]], device_id=dev(tgt), device_id_type=MESH)

    def out_copies(kind, ty, j):
        if ty == 1:
            return [qkv_copy(kind, 1, j, cl, zh, c, (c, cl)) for c in range(quad)]
        return [qkv_copy(kind, ty, j, cl, zh, lax.rem(cl + r, quad), (r, r)) for r in range(1, quad)]

    def in_copies(kind, ty, j):
        if ty == 1:
            return [qkv_copy(kind, 1, j, c, 1 - zh, cl, (c, c)) for c in range(quad)]
        return [qkv_copy(kind, ty, j, lax.rem(cl + quad - r, quad), zh, cl, (r, r)) for r in range(1, quad)]

    def own_copy(kind, ty, j):
        buf = ((qn, qf, qm), (kn, kf, km), (vn, vf, vm))[kind][ty]
        n = (tok, nu, mx)[ty]
        dst = place(kind, mirror_chip, nu, n, j) if ty == 2 else place(kind, chip, 0, n, j)
        dst[...] = buf[j * quad + cl]

    def make(kind, ty, j, slot):
        src = xm if ty == 2 else xs
        n = (tok, nu, mx)[ty]
        buf = ((qn, qf, qm), (kn, kf, km), (vn, vf, vm))[kind][ty]

        def cols(p, carry):
            col = pl.multiple_of(p * 2 * HD, 2 * HD)
            boff = kind * hd_all + j * NCHIP * HD + (1 - zh if ty == 1 else zh) * wide + col
            y2 = dot(src[0:n, :], w[slot, :, pl.ds(col, 2 * HD)]) + lane_row(bi_ref, pl.multiple_of(boff, 256), 2 * HD)
            for hh in range(2):
                y = y2[:, hh * HD:(hh + 1) * HD]
                if kind == 2:
                    buf[j * quad + 2 * p + hh] = y.T.astype(BF16)
                else:
                    gain = (qg_ref, kg_ref)[kind][...].astype(F32).reshape(1, HD)
                    buf[j * quad + 2 * p + hh] = norm_rope(y, gain, (cos_m, se_m, so_m) if ty == 2 else (cos_t, se_t, so_t)).astype(BF16)
            return carry
        lax.fori_loop(0, 2, cols, 0)

    load_x.wait()
    ln_rows(xs, mi, tok)

    last = nj - 1
    mir_after = min(1, last)

    def text_rows():
        load_t.wait()
        ln_rows(xt, mt, txt)
        for t, kind in enumerate(KINDS):
            if t == 0:
                start_txt(2)
            elif nj > 1:
                start_own(1, t - 1)
            else:
                start_mir(0, t - 1)
            slot = wait("txt", kind, None, (2 + t) % 3)
            y3 = dot(xt[...], w[slot, :, 0:nj * HD])
            for j in range(nj):
                pair0 = kind * hd_all + (j * NCHIP + chip - lax.rem(chip, 2)) * HD
                b2 = lane_row(bt_ref, pl.multiple_of(pair0, 256), 2 * HD)
                y = y3[:, j * HD:(j + 1) * HD] + jnp.where(lax.rem(chip, 2) == 0, b2[:, 0:HD], b2[:, HD:2 * HD])
                if kind == 2:
                    vb[j, :, 0:txt] = y.T.astype(BF16)
                else:
                    gain = (tqg_ref, tkg_ref)[kind][...].astype(F32).reshape(1, HD)
                    (qb, kb)[kind][j, 0:txt] = norm_rope(y, gain, None).astype(BF16)

    def mirror_rows():
        pos_copy().wait_recv()
        tables(posm[...], mx, cos_m, se_m, so_m)
        x_copy().wait_recv()
        ln_rows(xm, mi, mx)

        lax.fori_loop(0, nj, mir_pass, 0)

    def mir_pass(j, carry):
        for i, kind in enumerate(KINDS):
            if i == 0:
                start_mir(j, 2)
            else:
                @pl.when(j < nj - 1)
                def _():
                    start_mir(j + 1, i - 1)

                @pl.when(j == nj - 1)
                def _():
                    if mir_after < last:
                        start_own(mir_after + 1, i - 1)
                    else:
                        start_mod2(i - 1)
            slot = wait("img", (kind, 0), j, (2 + i) % 3)
            make(kind, 2, j, slot)
            for cp in out_copies(kind, 2, j):
                cp.start()
            own_copy(kind, 2, j)
        return carry

    def after_own(j, p):
        @pl.when(j == 0)
        def _():
            start_txt(p)

        if mir_after > 0:
            @pl.when(j == mir_after)
            def _():
                start_mir(0, p)

        @pl.when((j > mir_after) & (j < last))
        def _():
            start_own(j + 1, p)

        if last > mir_after:
            @pl.when(j == last)
            def _():
                start_mod2(p)

    def own_pass(j, carry):
        for p in range(6):
            kind, side = KINDS[p // 2], p % 2
            if p + 2 < 6:
                start_own(j, p + 2)
            else:
                after_own(j, p - 4)
            slot = wait("img", (kind, side), j, (2 + p) % 3)
            make(kind, side, j, slot)
            for cp in out_copies(kind, side, j):
                cp.start()
            if side == 0:
                own_copy(kind, 0, j)

        pl.when(j == 0)(text_rows)
        pl.when(j == mir_after)(mirror_rows)
        return carry
    lax.fori_loop(0, nj, own_pass, 0)

    mine2[...] = jnp.zeros_like(mine2)
    for t in range(4):
        if t + 2 < 4:
            start_mod2(t + 2)
        mod_rows(wait("mod", t // 2, t % 2, (2 + t) % 3), mine2, t * per)
    gath2 = spread(mine2, g2, 1)
    for cp in gath2:
        cp.start()
    g2[me] = mine2[...]

    scale2 = (HD ** -0.5) * 1.4426950408889634
    keys = txt + 2 * half
    nchunk = keys // ck
    qt = 256
    ntile = (txt + half) // qt
    group = 2 * tok // qt
    ngroup = NCHIP // 2

    def to_sibling(kind, j):
        ref = (kb.at[j, pl.ds(pl.multiple_of(txt + core * half, 128), half)] if kind == 1
               else vb.at[j, :, pl.ds(pl.multiple_of(txt + core * half, 128), half)])
        return pltpu.make_async_remote_copy(
            src_ref=ref, dst_ref=ref, send_sem=fssem.at[kind - 1, j], recv_sem=frsem.at[kind - 1, j],
            device_id={"cp": sib}, device_id_type=MESH)

    def collect(j):
        for kind in KINDS:
            for ty in range(3):
                for cp in in_copies(kind, ty, j):
                    cp.wait_recv()
            if kind != 0:
                to_sibling(kind, j).start()

    def tile_start(t):
        g = (t - 1) // group
        plane = lax.rem(chip // 2 + 1 + g, ngroup)
        row = txt + plane * (2 * tok) + lax.rem(t - 1, group) * qt
        return pl.multiple_of(jnp.where(t == 0, 0, row), 128)

    def qk(j, q, i, s_ref, mxv):
        sl = pl.ds(pl.multiple_of(i * ck, ck), ck)
        s = dot_t(kb[j, sl], q)
        s_ref[sl, :] = s
        return jnp.maximum(mxv, jnp.max(s.reshape(ck // 8, 8, qt), axis=0))

    def sm(j, i, s_ref, m, lsum, acc):
        sl = pl.ds(pl.multiple_of(i * ck, ck), ck)
        p = jnp.exp2((s_ref[sl, :] - m) * scale2)
        lsum = lsum + jnp.sum(p.reshape(ck // 8, 8, qt), axis=0)
        acc = acc + dot(vb[j, :, sl], p.astype(BF16))
        return lsum, acc

    def new_max():
        return jnp.full((8, qt), -jnp.inf, F32)

    def o_remote(j, c_src, c_dst):
        src = ost.at[j, pl.ds(pl.multiple_of(c_dst * tok, 128), tok)]
        dst = o_hbm.at[:, pl.ds(pl.multiple_of((j * NCHIP + c_src) * HD, HD), HD)]
        return pltpu.make_async_remote_copy(
            src_ref=src, dst_ref=dst, send_sem=ossem.at[j, c_dst], recv_sem=orsem.at[j, c_src],
            device_id=dev(c_dst), device_id_type=MESH)

    def o_local(j):
        src = ost.at[j, pl.ds(pl.multiple_of(chip * tok, 128), tok)]
        dst = o_hbm.at[:, pl.ds(pl.multiple_of((j * NCHIP + chip) * HD, HD), HD)]
        return pltpu.make_async_copy(src, dst, ossem.at[j, chip])

    def o_send(j, g):
        plane = lax.rem(chip // 2 + 1 + g, ngroup)
        for y in range(2):
            c = plane * 2 + y

            @pl.when(c != chip)
            def _():
                o_remote(j, chip, c).start()

            @pl.when(c == chip)
            def _():
                o_local(j).start()

    def finish(j, t, lsum, acc):
        tot = jnp.sum(lsum, axis=0, keepdims=True)
        o = (acc / tot).T.astype(BF16)

        @pl.when(t == 0)
        def _():
            otmp[...] = o
            ot_ref[j] = otmp[pl.ds(pl.multiple_of(core * (txt // 2), 8), txt // 2), :]

        @pl.when(t > 0)
        def _():
            ost[j, pl.ds(pl.multiple_of(tile_start(t) - txt, 128), qt)] = o

            @pl.when(lax.rem(t, group) == 0)
            def _():
                o_send(j, t // group - 1)

    def pair(j, t, s_cur, mx_cur, s_nxt, mx_nxt, has_next):
        m = jnp.max(mx_cur[...], axis=0, keepdims=True)
        lsum = jnp.zeros((8, qt), F32)
        acc = jnp.zeros((HD, qt), F32)
        if has_next:
            q = qb[j, pl.ds(tile_start(t + 1), qt)]

            def body(i, carry):
                lsum, acc, mxv = carry
                mxv = qk(j, q, i, s_nxt, mxv)
                lsum, acc = sm(j, i, s_cur, m, lsum, acc)
                return lsum, acc, mxv
            lsum, acc, mxv = lax.fori_loop(0, nchunk, body, (lsum, acc, new_max()))
            mx_nxt[...] = mxv
        else:
            def body(i, carry):
                return sm(j, i, s_cur, m, *carry)
            lsum, acc = lax.fori_loop(0, nchunk, body, (lsum, acc))
        finish(j, t, lsum, acc)

    collect(0)

    def head(j, carry):
        for kind in (1, 2):
            to_sibling(kind, j).wait()
        q = qb[j, 0:qt]

        def first(i, mxv):
            return qk(j, q, i, s0, mxv)
        mx0[...] = lax.fori_loop(0, nchunk, first, new_max())

        def two(i, carry):
            pair(j, 2 * i, s0, mx0, s1, mx1, True)
            pair(j, 2 * i + 1, s1, mx1, s0, mx0, True)
            return carry
        lax.fori_loop(0, (ntile - 1) // 2, two, 0)
        if nj > 1:
            @pl.when(j < nj - 1)
            def _():
                collect(j + 1)
        pair(j, jnp.int32(ntile - 1), s0, mx0, s1, mx1, False)
        return carry
    lax.fori_loop(0, nj, head, 0)

    for cp in gath2:
        cp.wait()
    x_copy().wait_send()
    pos_copy().wait_send()

    def drain(j, carry):
        for kind in KINDS:
            for ty in range(3):
                for cp in out_copies(kind, ty, j):
                    cp.wait_send()
        o_local(j).wait()
        for r in range(1, NCHIP):
            c = lax.rem(chip + r, NCHIP)
            o_remote(j, chip, c).wait_send()
            o_remote(j, c, chip).wait_recv()
        return carry
    lax.fori_loop(0, nj, drain, 0)


def attention(image, text, cond_vec, wm_img, wm_txt, w_img, w_txt, flat, pos, omega):
    tok, d_in = image.shape
    txt = text.shape[0]
    hd_all = w_img.shape[1] // 3
    heads = hd_all // HD
    nj = heads // NCHIP
    half = tok * NCHIP
    keys = txt + 2 * half
    ck = 3200
    mx = 2 * tok // 3
    nu = tok - mx
    cfg = (tok, txt, d_in, heads, ck, mx)
    dma = pltpu.SemaphoreType.DMA
    flops = 2 * tok * d_in * 3 * hd_all + 4 * nj * HD * (half + txt) * keys
    per = 2 * d_in // NDEV // 128
    r1, r2 = -(-2 * per // 8) * 8, -(-4 * per // 8) * 8
    row_sets = [pltpu.VMEM((nj * 4, n, HD), BF16) for n in (tok, nu, mx)]
    col_sets = [pltpu.VMEM((nj * 4, HD, n), BF16) for n in (tok, nu, mx)]
    table = pltpu.VMEM((tok, 128), F32)
    return pl.pallas_call(
        functools.partial(main_kernel, cfg),
        out_shape=(jax.ShapeDtypeStruct((tok, hd_all), BF16), jax.ShapeDtypeStruct((nj, txt // 2, HD), BF16),
                   jax.ShapeDtypeStruct((NDEV, r2, 128), F32)),
        in_specs=[ANY, ANY, VM, ANY, ANY, ANY, ANY] + [VM] * 10,
        out_specs=(ANY, VM, VM),
        scratch_shapes=[
            pltpu.VMEM((3, d_in, 4 * HD), BF16),
            pltpu.VMEM((tok, d_in), BF16), pltpu.VMEM((mx, d_in), BF16), pltpu.VMEM((txt, d_in), BF16),
            *row_sets, *col_sets, *row_sets,
            pltpu.VMEM((nj, keys, HD), BF16), pltpu.VMEM((nj, HD, keys), BF16), pltpu.VMEM((nj, txt + half, HD), BF16),
            pltpu.VMEM((mx, 128), BF16), table, table, table, *[pltpu.VMEM((mx, 128), F32)] * 3,
            pltpu.VMEM((2, d_in), F32), pltpu.VMEM((2, d_in), F32),
            pltpu.VMEM((NDEV, r1, 128), F32), pltpu.VMEM((r1, 128), F32), pltpu.VMEM((r2, 128), F32),
            pltpu.VMEM((keys, 256), F32), pltpu.VMEM((keys, 256), F32), pltpu.VMEM((8, 256), F32), pltpu.VMEM((8, 256), F32),
            pltpu.VMEM((nj, half, HD), BF16), pltpu.VMEM((txt, HD), BF16),
            dma((2,)), dma((3, max(nj, 1))), dma((2,)), dma((2,)), dma((2, NDEV)), dma((2, NDEV)),
            dma((3, 3, nj, 4)), dma((3, 3, nj, 4)), dma((2, nj)), dma((2, nj)), dma((nj, NCHIP)), dma((nj, NCHIP)),
        ],
        compiler_params=pltpu.CompilerParams(collective_id=1, has_side_effects=True, vmem_limit_bytes=VMEM_LIMIT),
        cost_estimate=pl.CostEstimate(flops=flops, bytes_accessed=3 * d_in * 3 * hd_all, transcendentals=0),
        name="attn",
    )(image, text, cond_vec, wm_img, wm_txt, w_img, w_txt, *flat, pos, omega)


def gelu(x):
    return x * (0.5 * (1.0 + jnp.tanh(0.7978845608028654 * (x + 0.044715 * (x * x * x)))))


def out_kernel(cfg, o_hbm, x_hbm, xt_hbm, ot_ref, g2_ref, bmi_ref, bmt_ref, bp_ref, tbp_ref, b1_ref, tb1_ref, b2_ref, tb2_ref, wp_hbm, w1_hbm, w2_hbm, twp_hbm, tw1_hbm, tw2_hbm,
               out_ref, tout_ref, mi_ref, mt_ref,
               wa, wb, wc, o, x, h, z, acc, a0, a1, o_t, x_t, h_t, z_t, a_t, part, rs, row,
               asem, bsem, csem, lsem, ossem, orsem, pssem, prsem, rssem, rrsem, fssem, frsem):
    tok, txt, d, ff, k1, k2 = cfg
    me = lax.axis_index("cp")
    chip, core = me // 2, me % 2
    sib = chip * 2 + (1 - core)
    rows = txt // 2
    piece = rows // NCHIP
    nb = wa.shape[2]
    na = wa.shape[0]
    np_ = d // nb
    nf = ff // nb
    ft = ff // NCHIP
    nt = ft // nb
    nj = ot_ref.shape[0]

    def dev(c):
        return {"cp": c * 2 + core}

    off = pl.multiple_of(chip * ft, nb)

    def start_a(p):
        slot = lax.rem(p, na)

        @pl.when(p < np_)
        def _():
            pltpu.make_async_copy(wp_hbm.at[:, pl.ds(pl.multiple_of(p * nb, nb), nb)], wa.at[slot], asem.at[slot]).start()

        @pl.when((p >= np_) & (p < np_ + nf))
        def _():
            pltpu.make_async_copy(w1_hbm.at[:, pl.ds(pl.multiple_of((p - np_) * nb, nb), nb)], wa.at[slot], asem.at[slot]).start()

    def start_b(p):
        slot = lax.rem(p, na)

        @pl.when(p < nf)
        def _():
            pltpu.make_async_copy(w2_hbm.at[pl.ds(pl.multiple_of(p * nb, nb), nb), :], wb.at[slot], bsem.at[slot]).start()

    def c_fc2(p, slot):
        return pltpu.make_async_copy(tw2_hbm.at[pl.ds(off, ft), pl.ds(pl.multiple_of(p * nb, nb), nb)],
                                     wc.at[slot, pl.ds(0, ft), :], csem.at[slot])

    def start_c(p):
        slot = lax.rem(p, na)

        @pl.when(p < np_)
        def _():
            pltpu.make_async_copy(twp_hbm.at[:, pl.ds(pl.multiple_of(p * nb, nb), nb)], wc.at[slot], csem.at[slot]).start()

        @pl.when((p >= np_) & (p < np_ + nt))
        def _():
            pltpu.make_async_copy(tw1_hbm.at[:, pl.ds(pl.multiple_of(off + (p - np_) * nb, nb), nb)], wc.at[slot], csem.at[slot]).start()

        @pl.when((p >= np_ + nt) & (p < np_ + nt + np_))
        def _():
            c_fc2(p - np_ - nt, slot).start()

    def get_a(p):
        start_a(p + na - 1)
        slot = lax.rem(p, na)
        pltpu.make_async_copy(w1_hbm.at[:, 0:nb], wa.at[slot], asem.at[slot]).wait()
        return slot

    def get_b(p):
        start_b(p + na - 1)
        slot = lax.rem(p, na)
        pltpu.make_async_copy(w2_hbm.at[0:nb, :], wb.at[slot], bsem.at[slot]).wait()
        return slot

    def get_c(p, fc2=False):
        start_c(p + na - 1)
        slot = lax.rem(p, na)
        if fc2:
            c_fc2(0, slot).wait()
        else:
            pltpu.make_async_copy(w1_hbm.at[:, 0:nb], wc.at[slot], csem.at[slot]).wait()
        return slot

    load_o = pltpu.make_async_copy(o_hbm, o, lsem.at[0])
    load_x = pltpu.make_async_copy(x_hbm, x, lsem.at[1])
    load_t = pltpu.make_async_copy(xt_hbm.at[pl.ds(pl.multiple_of(core * rows, 8), rows), :], x_t, lsem.at[2])
    load_o.start()
    start_a(jnp.int32(0))
    load_x.start()
    for p in range(1, na - 1):
        start_a(jnp.int32(p))
    load_t.start()
    for p in range(na - 1):
        start_b(jnp.int32(p))
    for p in range(na - 1):
        start_c(jnp.int32(p))

    barrier = pltpu.get_barrier_semaphore()
    for r in range(1, NCHIP):
        pl.semaphore_signal(barrier, inc=1, device_id=dev(lax.rem(chip + r, NCHIP)), device_id_type=MESH)
    pl.semaphore_signal(barrier, inc=1, device_id={"cp": sib}, device_id_type=MESH)
    pl.semaphore_wait(barrier, NCHIP)

    def o_copy(j, r, c_src, c_dst):
        return pltpu.make_async_remote_copy(
            src_ref=ot_ref.at[j], dst_ref=o_t.at[:, pl.ds(pl.multiple_of((j * NCHIP + c_src) * HD, HD), HD)],
            send_sem=ossem.at[j, r], recv_sem=orsem.at[j, r], device_id=dev(c_dst), device_id_type=MESH)

    for j in range(nj):
        for r in range(1, NCHIP):
            o_copy(j, r, chip, lax.rem(chip + r, NCHIP)).start()
        o_t[:, pl.ds(pl.multiple_of((j * NCHIP + chip) * HD, HD), HD)] = ot_ref[j]

    per = 4 * d // NDEV // 128
    for b, (b_ref, m) in enumerate(((bmi_ref, mi_ref), (bmt_ref, mt_ref))):
        for k in range(2, 6):
            m[k:k + 1, :] = lane_row(b_ref, k * d, d)
        for dv in range(NDEV):
            for r in range(per):
                col = 2 * d + (dv * per + r) * 128
                at = (slice(col // d, col // d + 1), slice(col % d, col % d + 128))
                m[at] = m[at] + g2_ref[dv, b * per + r:b * per + r + 1, :]

    load_o.wait()
    load_x.wait()

    def proj(p, carry):
        slot = get_a(p)
        sl = pl.ds(pl.multiple_of(p * nb, nb), nb)
        y = dot(o[...], wa[slot]) + lane_row(bp_ref, pl.multiple_of(p * nb, nb), nb)
        h[:, sl] = x[:, sl].astype(F32) + mi_ref[2:3, sl] * y
        return carry
    lax.fori_loop(0, np_, proj, 0)

    def ln2(src, dst, m_ref, n):
        shift, scale = m_ref[3:4, :], 1.0 + m_ref[4:5, :]
        rb = 16

        def body(i, carry):
            r = pl.ds(pl.multiple_of(i * rb, rb), rb)
            dst[r, :] = ln_mod_rows(src[r, :], scale, shift).astype(BF16)
            return carry
        lax.fori_loop(0, n // rb, body, 0)

    ln2(h, z, mi_ref, tok)
    acc[...] = jnp.broadcast_to(lane_row(b2_ref, 0, d), acc.shape)

    def tproj(p, carry):
        slot = get_c(p)
        sl = pl.ds(pl.multiple_of(p * nb, nb), nb)
        y = dot(o_t[...], wc[slot]) + lane_row(tbp_ref, pl.multiple_of(p * nb, nb), nb)
        h_t[:, sl] = x_t[:, sl].astype(F32) + mt_ref[2:3, sl] * y
        return carry

    def tfc1(p, carry):
        slot = get_c(np_ + p)
        col = pl.multiple_of(p * nb, nb)
        y = dot(z_t[...], wc[slot]) + lane_row(tb1_ref, pl.multiple_of(off + col, nb), nb)
        a_t[:, pl.ds(col, nb)] = gelu(y).astype(BF16)
        return carry

    def tfc2(p, carry):
        slot = get_c(np_ + nt + p, True)
        part[:, pl.ds(pl.multiple_of(p * nb, nb), nb)] = dot(a_t[...], wc[slot, 0:ft, :])
        return carry

    def p_copy(r, c_src, c_dst):
        return pltpu.make_async_remote_copy(
            src_ref=part.at[pl.ds(pl.multiple_of(c_dst * piece, 8), piece), :], dst_ref=rs.at[c_src],
            send_sem=pssem.at[r], recv_sem=prsem.at[r], device_id=dev(c_dst), device_id_type=MESH)

    mine = pl.ds(pl.multiple_of(chip * piece, 8), piece)

    def text0():
        load_t.wait()
        for j in range(nj):
            for r in range(1, NCHIP):
                o_copy(j, r, lax.rem(chip + NCHIP - r, NCHIP), chip).wait_recv()
        lax.fori_loop(0, np_ // 2, tproj, 0)

    def text1():
        lax.fori_loop(np_ // 2, np_, tproj, 0)

    def text2():
        ln2(h_t, z_t, mt_ref, rows)
        lax.fori_loop(0, nt, tfc1, 0)

    def text3():
        lax.fori_loop(0, np_, tfc2, 0)
        for r in range(1, NCHIP):
            p_copy(r, chip, lax.rem(chip + r, NCHIP)).start()
        rs[chip] = part[mine, :]

    def r_copy(r, c_src, c_dst):
        return pltpu.make_async_remote_copy(
            src_ref=row, dst_ref=tout_ref.at[pl.ds(pl.multiple_of(core * rows + c_src * piece, 8), piece), :],
            send_sem=rssem.at[r], recv_sem=rrsem.at[r], device_id=dev(c_dst), device_id_type=MESH)

    def text4():
        for r in range(1, NCHIP):
            p_copy(r, lax.rem(chip + NCHIP - r, NCHIP), chip).wait_recv()
        tot = rs[0]
        for c in range(1, NCHIP):
            tot = tot + rs[c]
        y = h_t[mine, :] + mt_ref[5:6, :] * (tot + lane_row(tb2_ref, 0, d))
        row[...] = y.astype(BF16)
        for r in range(1, NCHIP):
            r_copy(r, chip, lax.rem(chip + r, NCHIP)).start()
        tout_ref[pl.ds(pl.multiple_of(core * rows + chip * piece, 8), piece), :] = row[...]

    def mlp(i, a_new, a_old):
        slot_b = get_b(i - 1)
        slot_a = get_a(np_ + i)
        a_new[...] = gelu(dot(z[...], wa[slot_a]) + lane_row(b1_ref, pl.multiple_of(i * nb, nb), nb)).astype(BF16)
        acc[...] += dot(a_old[...], wb[slot_b])

    slot = get_a(jnp.int32(np_))
    a0[...] = gelu(dot(z[...], wa[slot]) + lane_row(b1_ref, 0, nb)).astype(BF16)

    def two(k, carry):
        mlp(2 * k + 1, a1, a0)
        pl.when(k == k1)(text0)
        pl.when(k == k1 + 1)(text2)
        mlp(2 * k + 2, a0, a1)
        pl.when(k == k1)(text1)
        pl.when(k == k1 + 1)(text3)
        pl.when(k == k2)(text4)
        return carry
    lax.fori_loop(0, nf // 2 - 1, two, 0)
    mlp(jnp.int32(nf - 1), a1, a0)

    for r in range(1, NCHIP):
        r_copy(r, lax.rem(chip + NCHIP - r, NCHIP), chip).wait_recv()
    ref = tout_ref.at[pl.ds(pl.multiple_of(core * rows, 8), rows), :]
    fwd = pltpu.make_async_remote_copy(src_ref=ref, dst_ref=ref, send_sem=fssem, recv_sem=frsem,
                                       device_id={"cp": sib}, device_id_type=MESH)
    fwd.start()

    slot = get_b(jnp.int32(nf - 1))
    y = acc[...] + dot(a1[...], wb[slot])
    out_ref[...] = (h[...] + mi_ref[5:6, :] * y).astype(BF16)

    fwd.wait()
    for j in range(nj):
        for r in range(1, NCHIP):
            o_copy(j, r, chip, lax.rem(chip + r, NCHIP)).wait_send()
    for r in range(1, NCHIP):
        c = lax.rem(chip + r, NCHIP)
        p_copy(r, chip, c).wait_send()
        r_copy(r, chip, c).wait_send()


def output(o_img, image, text, o_txt, g2, flat, wp, w1, w2, twp, tw1, tw2):
    tok, d = image.shape
    txt = text.shape[0]
    ff = w1.shape[1]
    nb = 512
    nf = ff // nb
    k1, k2 = (1, 9) if nf > 8 else (0, 2)
    na = 3
    rows = txt // 2
    ft = ff // NCHIP
    nj = o_txt.shape[0]
    dma = pltpu.SemaphoreType.DMA
    flops = 2 * tok * d * (d + 2 * ff) + 2 * rows * d * (d + 2 * ft)
    return pl.pallas_call(
        functools.partial(out_kernel, (tok, txt, d, ff, k1, k2)),
        out_shape=(jax.ShapeDtypeStruct((tok, d), BF16), jax.ShapeDtypeStruct((txt, d), BF16)),
        in_specs=[ANY, ANY, ANY, VM, VM] + [VM] * 8 + [ANY] * 6,
        out_specs=(VM, VM),
        scratch_shapes=[
            pltpu.VMEM((6, d), F32), pltpu.VMEM((6, d), F32),
            pltpu.VMEM((na, d, nb), BF16), pltpu.VMEM((na, nb, d), BF16), pltpu.VMEM((na, d, nb), BF16),
            pltpu.VMEM((tok, d), BF16), pltpu.VMEM((tok, d), BF16), pltpu.VMEM((tok, d), F32), pltpu.VMEM((tok, d), BF16),
            pltpu.VMEM((tok, d), F32), pltpu.VMEM((tok, nb), BF16), pltpu.VMEM((tok, nb), BF16),
            pltpu.VMEM((rows, d), BF16), pltpu.VMEM((rows, d), BF16), pltpu.VMEM((rows, d), F32), pltpu.VMEM((rows, d), BF16),
            pltpu.VMEM((rows, ft), BF16), pltpu.VMEM((rows, d), F32), pltpu.VMEM((NCHIP, rows // NCHIP, d), F32),
            pltpu.VMEM((rows // NCHIP, d), BF16),
            dma((na,)), dma((na,)), dma((na,)), dma((3,)), dma((nj, NCHIP)), dma((nj, NCHIP)), dma((NCHIP,)), dma((NCHIP,)),
            dma((NCHIP,)), dma((NCHIP,)), dma, dma,
        ],
        compiler_params=pltpu.CompilerParams(collective_id=2, has_side_effects=True, vmem_limit_bytes=VMEM_LIMIT),
        cost_estimate=pl.CostEstimate(flops=flops, bytes_accessed=2 * d * (d + 2 * ff), transcendentals=0),
        name="out",
    )(o_img, image, text, o_txt, g2, *flat, wp, w1, w2, twp, tw1, tw2)


def rope_inputs(ids):
    d_t = HD // 8
    d_s = (HD - d_t) // 2
    widths = (d_t, d_s, d_s)
    lane = lax.broadcasted_iota(jnp.int32, (1, HD), 1)
    pos = jnp.where(lane < d_t, ids[:, 0:1], jnp.where(lane < d_t + d_s, ids[:, 1:2], ids[:, 2:3])).astype(BF16)
    omega = np.concatenate([np.repeat(THETA ** (-np.arange(0, w, 2, dtype=np.float32) / np.float32(w)), 2) for w in widths])
    return pos, jnp.asarray(omega.astype(np.float32)[None, :])


def device_fn(image, text, cond_vec, image_ids, *weights):
    (wm, bm, wqkv, bqkv, qg, kg, wp, bp, w1, b1, w2, b2) = weights[:12]
    (twm, tbm, twqkv, tbqkv, tqg, tkg, twp, tbp, tw1, tb1, tw2, tb2) = weights[12:]
    x, xt = image[0], text[0]
    pos, omega = rope_inputs(image_ids)
    o_img, o_txt, g2 = attention(x, xt, cond_vec, wm, twm, wqkv, twqkv, (bm, tbm, bqkv, tbqkv, qg, kg, tqg, tkg), pos, omega)
    image_out, text_out = output(o_img, x, xt, o_txt, g2, (bm, tbm, bp, tbp, b1, tb1, b2, tb2), wp, w1, w2, twp, tw1, tw2)
    return image_out[None], text_out[None]


def solution(mesh):
    act = P("dp", "cp", None)
    txt = P("dp", None, None)
    in_specs = (act, txt, P("dp", None), P(("dp", "cp"), None)) + (P(),) * 24
    return jax.shard_map(device_fn, mesh=mesh, in_specs=in_specs, out_specs=(act, txt), check_vma=False)
```

```python
import functools

import jax
import jax.numpy as jnp
import numpy as np
from jax import lax
from jax.experimental import pallas as pl
from jax.experimental.pallas import tpu as pltpu
from jax.sharding import PartitionSpec as P

EPS = 1e-6
THETA = 10000.0
F32 = jnp.float32
BF16 = jnp.bfloat16
HD = 128
NCHIP = 8
NDEV = 16
VM = pl.BlockSpec(memory_space=pltpu.VMEM)
ANY = pl.BlockSpec(memory_space=pl.ANY)
MESH = pl.DeviceIdType.MESH
VMEM_LIMIT = 67043328


def dot(a, b):
    return jnp.dot(a, b, preferred_element_type=F32)


def dot_t(a, b):
    return lax.dot_general(a, b, (((1,), (1,)), ((), ())), preferred_element_type=F32)


def lane_row(b_ref, start, n):
    return b_ref[pl.ds(start, n)].astype(F32).reshape(1, n)


def ln_mod_rows(x, scale1p, shift):
    xf = x.astype(F32)
    mean = jnp.mean(xf, axis=-1, keepdims=True)
    cent = xf - mean
    var = jnp.mean(cent * cent, axis=-1, keepdims=True)
    return scale1p * (cent * lax.rsqrt(var + EPS)) + shift


KINDS = (1, 2, 0)


def main_kernel(cfg, x_hbm, xt_hbm, cond_ref, wmi_hbm, wmt_hbm, wi_hbm, wt_hbm, bmi_ref, bmt_ref, bi_ref, bt_ref,
                qg_ref, kg_ref, tqg_ref, tkg_ref, pos_ref, om_ref,
                o_hbm, ot_ref, g2,
                w, xs, xm, xt, kn, kf, km, vn, vf, vm, qn, qf, qm, kb, vb, qb, posm, cos_t, se_t, so_t, cos_m, se_m, so_m,
                mi, mt, g1, mine1, mine2, s0, s1, mx0, mx1, ost, otmp,
                xsem, wsem, msend, mrecv, gsend, grecv, ssem, rsem, fssem, frsem, ossem, orsem):
    tok, txt, d_in, heads, ck, mx = cfg
    nu = tok - mx
    hd_all = heads * HD
    nj = heads // NCHIP
    quad = 4
    wide = quad * HD
    half = tok * NCHIP
    me = lax.axis_index("cp")
    chip, core = me // 2, me % 2
    zh, cl = chip // quad, chip % quad
    sib = chip * 2 + (1 - core)
    mirror_chip = lax.rem(chip + quad, NCHIP)

    def dev(c):
        return {"cp": c * 2 + core}

    barrier = pltpu.get_barrier_semaphore()
    for r in range(1, NDEV):
        pl.semaphore_signal(barrier, inc=1, device_id={"cp": lax.rem(me + r, NDEV)}, device_id_type=MESH)
    load_x = pltpu.make_async_copy(x_hbm, xs, xsem.at[0])
    load_t = pltpu.make_async_copy(xt_hbm, xt, xsem.at[1])

    def x_copy():
        return pltpu.make_async_remote_copy(
            src_ref=x_hbm.at[pl.ds(nu, mx), :], dst_ref=xm, send_sem=msend.at[0], recv_sem=mrecv.at[0],
            device_id=dev(mirror_chip), device_id_type=MESH)

    def pos_copy():
        return pltpu.make_async_remote_copy(
            src_ref=pos_ref.at[pl.ds(nu, mx), :], dst_ref=posm, send_sem=msend.at[1], recv_sem=mrecv.at[1],
            device_id=dev(mirror_chip), device_id_type=MESH)

    mc = 2 * d_in // NDEV

    def tile_copy(what, a, b, slot):
        if what == "mod":
            ref = (wmi_hbm, wmt_hbm)[a]
            off = me * mc if b < 0 else 2 * d_in + me * 2 * mc + b * mc
            return [pltpu.make_async_copy(ref.at[:, pl.ds(pl.multiple_of(off, 128), mc)], w.at[slot, :, pl.ds(0, mc)], wsem.at[slot, 0])]
        if what == "txt":
            return [pltpu.make_async_copy(
                wt_hbm.at[:, pl.ds(pl.multiple_of(a * hd_all + (j * NCHIP + chip) * HD, HD), HD)],
                w.at[slot, :, pl.ds(j * HD, HD)], wsem.at[slot, j]) for j in range(nj)]
        kind, side = a
        off = kind * hd_all + b * NCHIP * HD + (zh if side == 0 else 1 - zh) * wide
        return [pltpu.make_async_copy(wi_hbm.at[:, pl.ds(pl.multiple_of(off, wide), wide)], w.at[slot], wsem.at[slot, 0])]

    def start(*a):
        for c in tile_copy(*a):
            c.start()

    def wait(*a):
        for c in tile_copy(*a):
            c.wait()
        return a[-1]

    def start_own(j, p):
        start("img", (KINDS[p // 2], p % 2), j, (2 + p) % 3)

    def start_txt(t):
        start("txt", KINDS[t], None, (2 + t) % 3)

    def start_mir(j, i):
        start("img", (KINDS[i], 0), j, (2 + i) % 3)

    def start_mod2(t):
        start("mod", t // 2, t % 2, (2 + t) % 3)

    start("mod", 0, -1, 0)
    start("mod", 1, -1, 1)
    load_x.start()
    load_t.start()

    c = cond_ref[...].astype(F32)
    act = (c * jax.nn.sigmoid(c)).astype(BF16)
    act = jnp.broadcast_to(act, (16, d_in))
    per = mc // 128

    def mod_rows(slot, buf, row):
        r = dot(act, w[slot, :, 0:mc])
        for i in range(per):
            buf[row + i:row + i + 1, :] = r[0:1, i * 128:(i + 1) * 128]

    def spread(buf, dst, k):
        return [pltpu.make_async_remote_copy(
            src_ref=buf, dst_ref=dst.at[me], send_sem=gsend.at[k, r], recv_sem=grecv.at[k, r],
            device_id={"cp": lax.rem(me + r, NDEV)}, device_id_type=MESH) for r in range(1, NDEV)]

    mine1[...] = jnp.zeros_like(mine1)
    start_own(0, 0)
    mod_rows(wait("mod", 0, -1, 0), mine1, 0)
    start_own(0, 1)
    mod_rows(wait("mod", 1, -1, 1), mine1, per)
    pl.semaphore_wait(barrier, NDEV - 1)
    gath1 = spread(mine1, g1, 0)
    for cp in gath1:
        cp.start()
    pos_copy().start()
    x_copy().start()
    g1[me] = mine1[...]

    def tables(pos, n, cos_t, se_t, so_t):
        ang = pos.astype(F32) * om_ref[...]
        odd = lax.rem(lax.broadcasted_iota(jnp.int32, ang.shape, 1), 2) == 1
        sin = jnp.sin(ang)
        cos_t[0:n, :] = jnp.cos(ang)
        se_t[0:n, :] = jnp.where(odd, 0.0, -sin)
        so_t[0:n, :] = jnp.where(odd, sin, 0.0)

    tables(pos_ref[...], tok, cos_t, se_t, so_t)
    for b_ref, m in ((bmi_ref, mi), (bmt_ref, mt)):
        for k in range(2):
            m[k:k + 1, :] = lane_row(b_ref, k * d_in, d_in)
    for cp in gath1:
        cp.wait()
    for b, m in ((0, mi), (1, mt)):
        for dv in range(NDEV):
            for r in range(per):
                col = (dv * per + r) * 128
                at = (slice(col // d_in, col // d_in + 1), slice(col % d_in, col % d_in + 128))
                m[at] = m[at] + g1[dv, b * per + r:b * per + r + 1, :]

    rb = 16

    def ln_rows(ref, m_ref, n):
        shift = m_ref[0:1, :]
        scale = 1.0 + m_ref[1:2, :]

        def body(i, carry):
            sl = pl.ds(pl.multiple_of(i * rb, rb), rb)
            ref[sl, :] = ln_mod_rows(ref[sl, :], scale, shift).astype(BF16)
            return carry
        lax.fori_loop(0, n // rb, body, 0)

    def norm_rope(y, gain, tabs):
        ms = jnp.mean(y * y, axis=-1, keepdims=True)
        y = y * lax.rsqrt(ms + EPS) * gain
        if tabs is not None:
            n = y.shape[0]
            y = y * tabs[0][0:n, :] + pltpu.roll(y, HD - 1, 1) * tabs[1][0:n, :] + pltpu.roll(y, 1, 1) * tabs[2][0:n, :]
        return y

    def place(kind, s_chip, row, n, j):
        if kind == 0:
            return qb.at[j, pl.ds(pl.multiple_of(txt + s_chip * tok + row, 128), n)]
        at = pl.multiple_of(txt + core * half + s_chip * tok + row, 128)
        return kb.at[j, pl.ds(at, n)] if kind == 1 else vb.at[j, :, pl.ds(at, n)]

    def qkv_copy(kind, ty, j, src_cl, src_zh, dst_cl, idx):
        buf = ((qn, qf, qm), (kn, kf, km), (vn, vf, vm))[kind][ty]
        n = (tok, nu, mx)[ty]
        s_chip = src_zh * quad + src_cl
        tgt = (1 - src_zh if ty == 1 else src_zh) * quad + dst_cl
        if ty == 2:
            dst = place(kind, lax.rem(s_chip + quad, NCHIP), nu, n, j)
        else:
            dst = place(kind, s_chip, 0, n, j)
        return pltpu.make_async_remote_copy(
            src_ref=buf.at[j * quad + dst_cl], dst_ref=dst, send_sem=ssem.at[kind, ty, j, idx[0]],
            recv_sem=rsem.at[kind, ty, j, idx[1]], device_id=dev(tgt), device_id_type=MESH)

    def out_copies(kind, ty, j):
        if ty == 1:
            return [qkv_copy(kind, 1, j, cl, zh, c, (c, cl)) for c in range(quad)]
        return [qkv_copy(kind, ty, j, cl, zh, lax.rem(cl + r, quad), (r, r)) for r in range(1, quad)]

    def in_copies(kind, ty, j):
        if ty == 1:
            return [qkv_copy(kind, 1, j, c, 1 - zh, cl, (c, c)) for c in range(quad)]
        return [qkv_copy(kind, ty, j, lax.rem(cl + quad - r, quad), zh, cl, (r, r)) for r in range(1, quad)]

    def own_copy(kind, ty, j):
        buf = ((qn, qf, qm), (kn, kf, km), (vn, vf, vm))[kind][ty]
        n = (tok, nu, mx)[ty]
        dst = place(kind, mirror_chip, nu, n, j) if ty == 2 else place(kind, chip, 0, n, j)
        dst[...] = buf[j * quad + cl]

    def make(kind, ty, j, slot):
        src = xm if ty == 2 else xs
        n = (tok, nu, mx)[ty]
        buf = ((qn, qf, qm), (kn, kf, km), (vn, vf, vm))[kind][ty]

        def cols(p, carry):
            col = pl.multiple_of(p * 2 * HD, 2 * HD)
            boff = kind * hd_all + j * NCHIP * HD + (1 - zh if ty == 1 else zh) * wide + col
            y2 = dot(src[0:n, :], w[slot, :, pl.ds(col, 2 * HD)]) + lane_row(bi_ref, pl.multiple_of(boff, 256), 2 * HD)
            for hh in range(2):
                y = y2[:, hh * HD:(hh + 1) * HD]
                if kind == 2:
                    buf[j * quad + 2 * p + hh] = y.T.astype(BF16)
                else:
                    gain = (qg_ref, kg_ref)[kind][...].astype(F32).reshape(1, HD)
                    buf[j * quad + 2 * p + hh] = norm_rope(y, gain, (cos_m, se_m, so_m) if ty == 2 else (cos_t, se_t, so_t)).astype(BF16)
            return carry
        lax.fori_loop(0, 2, cols, 0)

    load_x.wait()
    ln_rows(xs, mi, tok)

    last = nj - 1
    mir_after = 0

    def text_rows():
        load_t.wait()
        ln_rows(xt, mt, txt)
        for t, kind in enumerate(KINDS):
            if t == 0:
                start_txt(2)
            elif mir_after > 0:
                start_own(1, t - 1)
            else:
                start_mir(0, t - 1)
            slot = wait("txt", kind, None, (2 + t) % 3)
            y3 = dot(xt[...], w[slot, :, 0:nj * HD])
            for j in range(nj):
                pair0 = kind * hd_all + (j * NCHIP + chip - lax.rem(chip, 2)) * HD
                b2 = lane_row(bt_ref, pl.multiple_of(pair0, 256), 2 * HD)
                y = y3[:, j * HD:(j + 1) * HD] + jnp.where(lax.rem(chip, 2) == 0, b2[:, 0:HD], b2[:, HD:2 * HD])
                if kind == 2:
                    vb[j, :, 0:txt] = y.T.astype(BF16)
                else:
                    gain = (tqg_ref, tkg_ref)[kind][...].astype(F32).reshape(1, HD)
                    (qb, kb)[kind][j, 0:txt] = norm_rope(y, gain, None).astype(BF16)

    def mirror_rows():
        pos_copy().wait_recv()
        tables(posm[...], mx, cos_m, se_m, so_m)
        x_copy().wait_recv()
        ln_rows(xm, mi, mx)

        lax.fori_loop(0, nj, mir_pass, 0)

    def mir_pass(j, carry):
        for i, kind in enumerate(KINDS):
            if i == 0:
                start_mir(j, 2)
            else:
                @pl.when(j < nj - 1)
                def _():
                    start_mir(j + 1, i - 1)

                @pl.when(j == nj - 1)
                def _():
                    if mir_after < last:
                        start_own(mir_after + 1, i - 1)
                    else:
                        start_mod2(i - 1)
            slot = wait("img", (kind, 0), j, (2 + i) % 3)
            make(kind, 2, j, slot)
            for cp in out_copies(kind, 2, j):
                cp.start()
            own_copy(kind, 2, j)
        return carry

    def after_own(j, p):
        @pl.when(j == 0)
        def _():
            start_txt(p)

        if mir_after > 0:
            @pl.when(j == mir_after)
            def _():
                start_mir(0, p)

        @pl.when((j > mir_after) & (j < last))
        def _():
            start_own(j + 1, p)

        if last > mir_after:
            @pl.when(j == last)
            def _():
                start_mod2(p)

    def own_pass(j, carry):
        for p in range(6):
            kind, side = KINDS[p // 2], p % 2
            if p + 2 < 6:
                start_own(j, p + 2)
            else:
                after_own(j, p - 4)
            slot = wait("img", (kind, side), j, (2 + p) % 3)
            make(kind, side, j, slot)
            for cp in out_copies(kind, side, j):
                cp.start()
            if side == 0:
                own_copy(kind, 0, j)

        pl.when(j == 0)(text_rows)
        pl.when(j == mir_after)(mirror_rows)
        return carry
    lax.fori_loop(0, nj, own_pass, 0)

    mine2[...] = jnp.zeros_like(mine2)
    for t in range(4):
        if t + 2 < 4:
            start_mod2(t + 2)
        mod_rows(wait("mod", t // 2, t % 2, (2 + t) % 3), mine2, t * per)
    gath2 = spread(mine2, g2, 1)
    for cp in gath2:
        cp.start()
    g2[me] = mine2[...]

    scale2 = (HD ** -0.5) * 1.4426950408889634
    keys = txt + 2 * half
    nchunk = keys // ck
    qt = 256
    ntile = (txt + half) // qt
    group = 2 * tok // qt
    ngroup = NCHIP // 2

    def to_sibling(kind, j):
        ref = (kb.at[j, pl.ds(pl.multiple_of(txt + core * half, 128), half)] if kind == 1
               else vb.at[j, :, pl.ds(pl.multiple_of(txt + core * half, 128), half)])
        return pltpu.make_async_remote_copy(
            src_ref=ref, dst_ref=ref, send_sem=fssem.at[kind - 1, j], recv_sem=frsem.at[kind - 1, j],
            device_id={"cp": sib}, device_id_type=MESH)

    def collect(j):
        for kind in KINDS:
            for ty in range(3):
                for cp in in_copies(kind, ty, j):
                    cp.wait_recv()
            if kind != 0:
                to_sibling(kind, j).start()

    def tile_start(t):
        g = (t - 1) // group
        plane = lax.rem(chip // 2 + 1 + g, ngroup)
        row = txt + plane * (2 * tok) + lax.rem(t - 1, group) * qt
        return pl.multiple_of(jnp.where(t == 0, 0, row), 128)

    def qk(j, q, i, s_ref, mxv):
        sl = pl.ds(pl.multiple_of(i * ck, ck), ck)
        s = dot_t(kb[j, sl], q)
        s_ref[sl, :] = s
        return jnp.maximum(mxv, jnp.max(s.reshape(ck // 8, 8, qt), axis=0))

    def sm(j, i, s_ref, m, lsum, acc):
        sl = pl.ds(pl.multiple_of(i * ck, ck), ck)
        p = jnp.exp2((s_ref[sl, :] - m) * scale2)
        lsum = lsum + jnp.sum(p.reshape(ck // 8, 8, qt), axis=0)
        acc = acc + dot(vb[j, :, sl], p.astype(BF16))
        return lsum, acc

    def new_max():
        return jnp.full((8, qt), -jnp.inf, F32)

    def o_remote(j, c_src, c_dst):
        src = ost.at[j, pl.ds(pl.multiple_of(c_dst * tok, 128), tok)]
        dst = o_hbm.at[:, pl.ds(pl.multiple_of((j * NCHIP + c_src) * HD, HD), HD)]
        return pltpu.make_async_remote_copy(
            src_ref=src, dst_ref=dst, send_sem=ossem.at[j, c_dst], recv_sem=orsem.at[j, c_src],
            device_id=dev(c_dst), device_id_type=MESH)

    def o_local(j):
        src = ost.at[j, pl.ds(pl.multiple_of(chip * tok, 128), tok)]
        dst = o_hbm.at[:, pl.ds(pl.multiple_of((j * NCHIP + chip) * HD, HD), HD)]
        return pltpu.make_async_copy(src, dst, ossem.at[j, chip])

    def o_send(j, g):
        plane = lax.rem(chip // 2 + 1 + g, ngroup)
        for y in range(2):
            c = plane * 2 + y

            @pl.when(c != chip)
            def _():
                o_remote(j, chip, c).start()

            @pl.when(c == chip)
            def _():
                o_local(j).start()

    def finish(j, t, lsum, acc):
        tot = jnp.sum(lsum, axis=0, keepdims=True)
        o = (acc / tot).T.astype(BF16)

        @pl.when(t == 0)
        def _():
            otmp[...] = o
            ot_ref[j] = otmp[pl.ds(pl.multiple_of(core * (txt // 2), 8), txt // 2), :]

        @pl.when(t > 0)
        def _():
            ost[j, pl.ds(pl.multiple_of(tile_start(t) - txt, 128), qt)] = o

            @pl.when(lax.rem(t, group) == 0)
            def _():
                o_send(j, t // group - 1)

    def pair(j, t, s_cur, mx_cur, s_nxt, mx_nxt, has_next):
        m = jnp.max(mx_cur[...], axis=0, keepdims=True)
        lsum = jnp.zeros((8, qt), F32)
        acc = jnp.zeros((HD, qt), F32)
        if has_next:
            q = qb[j, pl.ds(tile_start(t + 1), qt)]

            def body(i, carry):
                lsum, acc, mxv = carry
                mxv = qk(j, q, i, s_nxt, mxv)
                lsum, acc = sm(j, i, s_cur, m, lsum, acc)
                return lsum, acc, mxv
            lsum, acc, mxv = lax.fori_loop(0, nchunk, body, (lsum, acc, new_max()))
            mx_nxt[...] = mxv
        else:
            def body(i, carry):
                return sm(j, i, s_cur, m, *carry)
            lsum, acc = lax.fori_loop(0, nchunk, body, (lsum, acc))
        finish(j, t, lsum, acc)

    collect(0)

    def head(j, carry):
        for kind in (1, 2):
            to_sibling(kind, j).wait()
        q = qb[j, 0:qt]

        def first(i, mxv):
            return qk(j, q, i, s0, mxv)
        mx0[...] = lax.fori_loop(0, nchunk, first, new_max())

        def two(i, carry):
            pair(j, 2 * i, s0, mx0, s1, mx1, True)
            pair(j, 2 * i + 1, s1, mx1, s0, mx0, True)
            return carry
        lax.fori_loop(0, (ntile - 1) // 2, two, 0)
        if nj > 1:
            @pl.when(j < nj - 1)
            def _():
                collect(j + 1)
        pair(j, jnp.int32(ntile - 1), s0, mx0, s1, mx1, False)
        return carry
    lax.fori_loop(0, nj, head, 0)

    for cp in gath2:
        cp.wait()
    x_copy().wait_send()
    pos_copy().wait_send()

    def drain(j, carry):
        for kind in KINDS:
            for ty in range(3):
                for cp in out_copies(kind, ty, j):
                    cp.wait_send()
        o_local(j).wait()
        for r in range(1, NCHIP):
            c = lax.rem(chip + r, NCHIP)
            o_remote(j, chip, c).wait_send()
            o_remote(j, c, chip).wait_recv()
        return carry
    lax.fori_loop(0, nj, drain, 0)


def attention(image, text, cond_vec, wm_img, wm_txt, w_img, w_txt, flat, pos, omega):
    tok, d_in = image.shape
    txt = text.shape[0]
    hd_all = w_img.shape[1] // 3
    heads = hd_all // HD
    nj = heads // NCHIP
    half = tok * NCHIP
    keys = txt + 2 * half
    ck = 3200
    mx = tok // 3
    nu = tok - mx
    cfg = (tok, txt, d_in, heads, ck, mx)
    dma = pltpu.SemaphoreType.DMA
    flops = 2 * tok * d_in * 3 * hd_all + 4 * nj * HD * (half + txt) * keys
    per = 2 * d_in // NDEV // 128
    r1, r2 = -(-2 * per // 8) * 8, -(-4 * per // 8) * 8
    row_sets = [pltpu.VMEM((nj * 4, n, HD), BF16) for n in (tok, nu, mx)]
    col_sets = [pltpu.VMEM((nj * 4, HD, n), BF16) for n in (tok, nu, mx)]
    table = pltpu.VMEM((tok, 128), F32)
    return pl.pallas_call(
        functools.partial(main_kernel, cfg),
        out_shape=(jax.ShapeDtypeStruct((tok, hd_all), BF16), jax.ShapeDtypeStruct((nj, txt // 2, HD), BF16),
                   jax.ShapeDtypeStruct((NDEV, r2, 128), F32)),
        in_specs=[ANY, ANY, VM, ANY, ANY, ANY, ANY] + [VM] * 10,
        out_specs=(ANY, VM, VM),
        scratch_shapes=[
            pltpu.VMEM((3, d_in, 4 * HD), BF16),
            pltpu.VMEM((tok, d_in), BF16), pltpu.VMEM((mx, d_in), BF16), pltpu.VMEM((txt, d_in), BF16),
            *row_sets, *col_sets, *row_sets,
            pltpu.VMEM((nj, keys, HD), BF16), pltpu.VMEM((nj, HD, keys), BF16), pltpu.VMEM((nj, txt + half, HD), BF16),
            pltpu.VMEM((mx, 128), BF16), table, table, table, *[pltpu.VMEM((mx, 128), F32)] * 3,
            pltpu.VMEM((2, d_in), F32), pltpu.VMEM((2, d_in), F32),
            pltpu.VMEM((NDEV, r1, 128), F32), pltpu.VMEM((r1, 128), F32), pltpu.VMEM((r2, 128), F32),
            pltpu.VMEM((keys, 256), F32), pltpu.VMEM((keys, 256), F32), pltpu.VMEM((8, 256), F32), pltpu.VMEM((8, 256), F32),
            pltpu.VMEM((nj, half, HD), BF16), pltpu.VMEM((txt, HD), BF16),
            dma((2,)), dma((3, max(nj, 1))), dma((2,)), dma((2,)), dma((2, NDEV)), dma((2, NDEV)),
            dma((3, 3, nj, 4)), dma((3, 3, nj, 4)), dma((2, nj)), dma((2, nj)), dma((nj, NCHIP)), dma((nj, NCHIP)),
        ],
        compiler_params=pltpu.CompilerParams(collective_id=1, has_side_effects=True, vmem_limit_bytes=VMEM_LIMIT),
        cost_estimate=pl.CostEstimate(flops=flops, bytes_accessed=3 * d_in * 3 * hd_all, transcendentals=0),
        name="attn",
    )(image, text, cond_vec, wm_img, wm_txt, w_img, w_txt, *flat, pos, omega)


def gelu(x):
    return x * (0.5 * (1.0 + jnp.tanh(0.7978845608028654 * (x + 0.044715 * (x * x * x)))))


def out_kernel(cfg, o_hbm, x_hbm, xt_hbm, ot_ref, g2_ref, bmi_ref, bmt_ref, bp_ref, tbp_ref, b1_ref, tb1_ref, b2_ref, tb2_ref, wp_hbm, w1_hbm, w2_hbm, twp_hbm, tw1_hbm, tw2_hbm,
               out_ref, tout_ref, mi_ref, mt_ref,
               wa, wb, wc, o, x, h, z, acc, a0, a1, o_t, x_t, h_t, z_t, a_t, part, rs, row,
               asem, bsem, csem, lsem, ossem, orsem, pssem, prsem, rssem, rrsem, fssem, frsem):
    tok, txt, d, ff, k1, k2 = cfg
    me = lax.axis_index("cp")
    chip, core = me // 2, me % 2
    sib = chip * 2 + (1 - core)
    rows = txt // 2
    quad = 4
    cl, zq = chip % quad, chip // quad * quad
    piece = rows // quad
    nb = wa.shape[2]
    na = wa.shape[0]
    np_ = d // nb
    nf = ff // nb
    ft = ff // quad
    nt = ft // nb
    nj = ot_ref.shape[0]

    def dev(c):
        return {"cp": c * 2 + core}

    off = pl.multiple_of(cl * ft, nb)

    def start_a(p):
        slot = lax.rem(p, na)

        @pl.when(p < np_)
        def _():
            pltpu.make_async_copy(wp_hbm.at[:, pl.ds(pl.multiple_of(p * nb, nb), nb)], wa.at[slot], asem.at[slot]).start()

        @pl.when((p >= np_) & (p < np_ + nf))
        def _():
            pltpu.make_async_copy(w1_hbm.at[:, pl.ds(pl.multiple_of((p - np_) * nb, nb), nb)], wa.at[slot], asem.at[slot]).start()

    def start_b(p):
        slot = lax.rem(p, na)

        @pl.when(p < nf)
        def _():
            pltpu.make_async_copy(w2_hbm.at[pl.ds(pl.multiple_of(p * nb, nb), nb), :], wb.at[slot], bsem.at[slot]).start()

    def c_fc2(p, slot):
        return pltpu.make_async_copy(tw2_hbm.at[pl.ds(off, ft), pl.ds(pl.multiple_of(p * nb, nb), nb)],
                                     wc.at[slot, pl.ds(0, ft), :], csem.at[slot])

    def start_c(p):
        slot = lax.rem(p, na)

        @pl.when(p < np_)
        def _():
            pltpu.make_async_copy(twp_hbm.at[:, pl.ds(pl.multiple_of(p * nb, nb), nb)], wc.at[slot], csem.at[slot]).start()

        @pl.when((p >= np_) & (p < np_ + nt))
        def _():
            pltpu.make_async_copy(tw1_hbm.at[:, pl.ds(pl.multiple_of(off + (p - np_) * nb, nb), nb)], wc.at[slot], csem.at[slot]).start()

        @pl.when((p >= np_ + nt) & (p < np_ + nt + np_))
        def _():
            c_fc2(p - np_ - nt, slot).start()

    def get_a(p):
        start_a(p + na - 1)
        slot = lax.rem(p, na)
        pltpu.make_async_copy(w1_hbm.at[:, 0:nb], wa.at[slot], asem.at[slot]).wait()
        return slot

    def get_b(p):
        start_b(p + na - 1)
        slot = lax.rem(p, na)
        pltpu.make_async_copy(w2_hbm.at[0:nb, :], wb.at[slot], bsem.at[slot]).wait()
        return slot

    def get_c(p, fc2=False):
        start_c(p + na - 1)
        slot = lax.rem(p, na)
        if fc2:
            c_fc2(0, slot).wait()
        else:
            pltpu.make_async_copy(w1_hbm.at[:, 0:nb], wc.at[slot], csem.at[slot]).wait()
        return slot

    load_o = pltpu.make_async_copy(o_hbm, o, lsem.at[0])
    load_x = pltpu.make_async_copy(x_hbm, x, lsem.at[1])
    load_t = pltpu.make_async_copy(xt_hbm.at[pl.ds(pl.multiple_of(core * rows, 8), rows), :], x_t, lsem.at[2])
    load_o.start()
    start_a(jnp.int32(0))
    load_x.start()
    for p in range(1, na - 1):
        start_a(jnp.int32(p))
    load_t.start()
    for p in range(na - 1):
        start_b(jnp.int32(p))
    for p in range(na - 1):
        start_c(jnp.int32(p))

    barrier = pltpu.get_barrier_semaphore()
    for r in range(1, NCHIP):
        pl.semaphore_signal(barrier, inc=1, device_id=dev(lax.rem(chip + r, NCHIP)), device_id_type=MESH)
    pl.semaphore_signal(barrier, inc=1, device_id={"cp": sib}, device_id_type=MESH)
    pl.semaphore_wait(barrier, NCHIP)

    def o_copy(j, r, c_src, c_dst):
        return pltpu.make_async_remote_copy(
            src_ref=ot_ref.at[j], dst_ref=o_t.at[:, pl.ds(pl.multiple_of((j * NCHIP + c_src) * HD, HD), HD)],
            send_sem=ossem.at[j, r], recv_sem=orsem.at[j, r], device_id=dev(c_dst), device_id_type=MESH)

    for j in range(nj):
        for r in range(1, NCHIP):
            o_copy(j, r, chip, lax.rem(chip + r, NCHIP)).start()
        o_t[:, pl.ds(pl.multiple_of((j * NCHIP + chip) * HD, HD), HD)] = ot_ref[j]

    per = 4 * d // NDEV // 128
    for b, (b_ref, m) in enumerate(((bmi_ref, mi_ref), (bmt_ref, mt_ref))):
        for k in range(2, 6):
            m[k:k + 1, :] = lane_row(b_ref, k * d, d)
        for dv in range(NDEV):
            for r in range(per):
                col = 2 * d + (dv * per + r) * 128
                at = (slice(col // d, col // d + 1), slice(col % d, col % d + 128))
                m[at] = m[at] + g2_ref[dv, b * per + r:b * per + r + 1, :]

    load_o.wait()
    load_x.wait()

    def proj(p, carry):
        slot = get_a(p)
        sl = pl.ds(pl.multiple_of(p * nb, nb), nb)
        y = dot(o[...], wa[slot]) + lane_row(bp_ref, pl.multiple_of(p * nb, nb), nb)
        h[:, sl] = x[:, sl].astype(F32) + mi_ref[2:3, sl] * y
        return carry
    lax.fori_loop(0, np_, proj, 0)

    def ln2(src, dst, m_ref, n):
        shift, scale = m_ref[3:4, :], 1.0 + m_ref[4:5, :]
        rb = 16

        def body(i, carry):
            r = pl.ds(pl.multiple_of(i * rb, rb), rb)
            dst[r, :] = ln_mod_rows(src[r, :], scale, shift).astype(BF16)
            return carry
        lax.fori_loop(0, n // rb, body, 0)

    ln2(h, z, mi_ref, tok)
    acc[...] = jnp.broadcast_to(lane_row(b2_ref, 0, d), acc.shape)

    def tproj(p, carry):
        slot = get_c(p)
        sl = pl.ds(pl.multiple_of(p * nb, nb), nb)
        y = dot(o_t[...], wc[slot]) + lane_row(tbp_ref, pl.multiple_of(p * nb, nb), nb)
        h_t[:, sl] = x_t[:, sl].astype(F32) + mt_ref[2:3, sl] * y
        return carry

    def tfc1(p, carry):
        slot = get_c(np_ + p)
        col = pl.multiple_of(p * nb, nb)
        y = dot(z_t[...], wc[slot]) + lane_row(tb1_ref, pl.multiple_of(off + col, nb), nb)
        a_t[:, pl.ds(col, nb)] = gelu(y).astype(BF16)
        return carry

    def tfc2(p, carry):
        slot = get_c(np_ + nt + p, True)
        part[:, pl.ds(pl.multiple_of(p * nb, nb), nb)] = dot(a_t[...], wc[slot, 0:ft, :])
        return carry

    def p_copy(r, c_src, c_dst):
        return pltpu.make_async_remote_copy(
            src_ref=part.at[pl.ds(pl.multiple_of(c_dst * piece, 8), piece), :], dst_ref=rs.at[c_src],
            send_sem=pssem.at[r], recv_sem=prsem.at[r], device_id=dev(zq + c_dst), device_id_type=MESH)

    def r_copy(r, c_src, c_dst):
        return pltpu.make_async_remote_copy(
            src_ref=row, dst_ref=tout_ref.at[pl.ds(pl.multiple_of(core * rows + c_src * piece, 8), piece), :],
            send_sem=rssem.at[r], recv_sem=rrsem.at[r], device_id=dev(zq + c_dst), device_id_type=MESH)

    mine = pl.ds(pl.multiple_of(cl * piece, 8), piece)
    n1, n2, n3 = np_ // 2, np_ // 2 + nt // 2, np_ + nt // 2

    def text_step(s):
        @pl.when(s == 0)
        def _():
            load_t.wait()
            for j in range(nj):
                for r in range(1, NCHIP):
                    o_copy(j, r, lax.rem(chip + NCHIP - r, NCHIP), chip).wait_recv()

        @pl.when((s >= 0) & (s < n1))
        def _():
            lax.fori_loop(2 * s, 2 * s + 2, tproj, 0)

        @pl.when(s == n1)
        def _():
            ln2(h_t, z_t, mt_ref, rows)

        @pl.when((s >= n1) & (s < n2))
        def _():
            lax.fori_loop(2 * (s - n1), 2 * (s - n1) + 2, tfc1, 0)

        @pl.when((s >= n2) & (s < n3))
        def _():
            lax.fori_loop(2 * (s - n2), 2 * (s - n2) + 2, tfc2, 0)

        @pl.when(s == n3 - 1)
        def _():
            for r in range(1, quad):
                p_copy(r, cl, lax.rem(cl + r, quad)).start()
            rs[cl] = part[mine, :]

        @pl.when(s == k2)
        def _():
            for r in range(1, quad):
                p_copy(r, lax.rem(cl + quad - r, quad), cl).wait_recv()
            tot = rs[0]
            for c in range(1, quad):
                tot = tot + rs[c]
            y = h_t[mine, :] + mt_ref[5:6, :] * (tot + lane_row(tb2_ref, 0, d))
            row[...] = y.astype(BF16)
            for r in range(1, quad):
                r_copy(r, cl, lax.rem(cl + r, quad)).start()
            tout_ref[pl.ds(pl.multiple_of(core * rows + cl * piece, 8), piece), :] = row[...]

    def mlp(i, a_new, a_old):
        slot_b = get_b(i - 1)
        slot_a = get_a(np_ + i)
        a_new[...] = gelu(dot(z[...], wa[slot_a]) + lane_row(b1_ref, pl.multiple_of(i * nb, nb), nb)).astype(BF16)
        acc[...] += dot(a_old[...], wb[slot_b])

    slot = get_a(jnp.int32(np_))
    a0[...] = gelu(dot(z[...], wa[slot]) + lane_row(b1_ref, 0, nb)).astype(BF16)

    def two(k, carry):
        mlp(2 * k + 1, a1, a0)
        text_step(2 * k - k1)
        mlp(2 * k + 2, a0, a1)
        text_step(2 * k + 1 - k1)
        return carry
    lax.fori_loop(0, nf // 2 - 1, two, 0)
    mlp(jnp.int32(nf - 1), a1, a0)

    for r in range(1, quad):
        r_copy(r, lax.rem(cl + quad - r, quad), cl).wait_recv()
    ref = tout_ref.at[pl.ds(pl.multiple_of(core * rows, 8), rows), :]
    fwd = pltpu.make_async_remote_copy(src_ref=ref, dst_ref=ref, send_sem=fssem, recv_sem=frsem,
                                       device_id={"cp": sib}, device_id_type=MESH)
    fwd.start()

    slot = get_b(jnp.int32(nf - 1))
    y = acc[...] + dot(a1[...], wb[slot])
    out_ref[...] = (h[...] + mi_ref[5:6, :] * y).astype(BF16)

    fwd.wait()
    for j in range(nj):
        for r in range(1, NCHIP):
            o_copy(j, r, chip, lax.rem(chip + r, NCHIP)).wait_send()
    for r in range(1, quad):
        c = lax.rem(cl + r, quad)
        p_copy(r, cl, c).wait_send()
        r_copy(r, cl, c).wait_send()


def output(o_img, image, text, o_txt, g2, flat, wp, w1, w2, twp, tw1, tw2):
    tok, d = image.shape
    txt = text.shape[0]
    ff = w1.shape[1]
    nb = 512
    nf = ff // nb
    k1, k2 = (2, 16) if nf > 8 else (0, 5)
    na = 3
    rows = txt // 2
    ft = ff // 4
    nj = o_txt.shape[0]
    dma = pltpu.SemaphoreType.DMA
    flops = 2 * tok * d * (d + 2 * ff) + 2 * rows * d * (d + 2 * ft)
    return pl.pallas_call(
        functools.partial(out_kernel, (tok, txt, d, ff, k1, k2)),
        out_shape=(jax.ShapeDtypeStruct((tok, d), BF16), jax.ShapeDtypeStruct((txt, d), BF16)),
        in_specs=[ANY, ANY, ANY, VM, VM] + [VM] * 8 + [ANY] * 6,
        out_specs=(VM, VM),
        scratch_shapes=[
            pltpu.VMEM((6, d), F32), pltpu.VMEM((6, d), F32),
            pltpu.VMEM((na, d, nb), BF16), pltpu.VMEM((na, nb, d), BF16), pltpu.VMEM((na, d, nb), BF16),
            pltpu.VMEM((tok, d), BF16), pltpu.VMEM((tok, d), BF16), pltpu.VMEM((tok, d), F32), pltpu.VMEM((tok, d), BF16),
            pltpu.VMEM((tok, d), F32), pltpu.VMEM((tok, nb), BF16), pltpu.VMEM((tok, nb), BF16),
            pltpu.VMEM((rows, d), BF16), pltpu.VMEM((rows, d), BF16), pltpu.VMEM((rows, d), F32), pltpu.VMEM((rows, d), BF16),
            pltpu.VMEM((rows, ft), BF16), pltpu.VMEM((rows, d), F32), pltpu.VMEM((4, rows // 4, d), F32),
            pltpu.VMEM((rows // 4, d), BF16),
            dma((na,)), dma((na,)), dma((na,)), dma((3,)), dma((nj, NCHIP)), dma((nj, NCHIP)), dma((NCHIP,)), dma((NCHIP,)),
            dma((NCHIP,)), dma((NCHIP,)), dma, dma,
        ],
        compiler_params=pltpu.CompilerParams(collective_id=2, has_side_effects=True, vmem_limit_bytes=VMEM_LIMIT),
        cost_estimate=pl.CostEstimate(flops=flops, bytes_accessed=2 * d * (d + 2 * ff), transcendentals=0),
        name="out",
    )(o_img, image, text, o_txt, g2, *flat, wp, w1, w2, twp, tw1, tw2)


def rope_inputs(ids):
    d_t = HD // 8
    d_s = (HD - d_t) // 2
    widths = (d_t, d_s, d_s)
    lane = lax.broadcasted_iota(jnp.int32, (1, HD), 1)
    pos = jnp.where(lane < d_t, ids[:, 0:1], jnp.where(lane < d_t + d_s, ids[:, 1:2], ids[:, 2:3])).astype(BF16)
    omega = np.concatenate([np.repeat(THETA ** (-np.arange(0, w, 2, dtype=np.float32) / np.float32(w)), 2) for w in widths])
    return pos, jnp.asarray(omega.astype(np.float32)[None, :])


def device_fn(image, text, cond_vec, image_ids, *weights):
    (wm, bm, wqkv, bqkv, qg, kg, wp, bp, w1, b1, w2, b2) = weights[:12]
    (twm, tbm, twqkv, tbqkv, tqg, tkg, twp, tbp, tw1, tb1, tw2, tb2) = weights[12:]
    x, xt = image[0], text[0]
    pos, omega = rope_inputs(image_ids)
    o_img, o_txt, g2 = attention(x, xt, cond_vec, wm, twm, wqkv, twqkv, (bm, tbm, bqkv, tbqkv, qg, kg, tqg, tkg), pos, omega)
    image_out, text_out = output(o_img, x, xt, o_txt, g2, (bm, tbm, bp, tbp, b1, tb1, b2, tb2), wp, w1, w2, twp, tw1, tw2)
    return image_out[None], text_out[None]


def solution(mesh):
    act = P("dp", "cp", None)
    txt = P("dp", None, None)
    in_specs = (act, txt, P("dp", None), P(("dp", "cp"), None)) + (P(),) * 24
    return jax.shard_map(device_fn, mesh=mesh, in_specs=in_specs, out_specs=(act, txt), check_vma=False)
```

```python
import functools

import jax
import jax.numpy as jnp
import numpy as np
from jax import lax
from jax.experimental import pallas as pl
from jax.experimental.pallas import tpu as pltpu
from jax.sharding import PartitionSpec as P

EPS = 1e-6
THETA = 10000.0
F32 = jnp.float32
BF16 = jnp.bfloat16
HD = 128
NCHIP = 8
NDEV = 16
VM = pl.BlockSpec(memory_space=pltpu.VMEM)
ANY = pl.BlockSpec(memory_space=pl.ANY)
MESH = pl.DeviceIdType.MESH
VMEM_LIMIT = 67043328


def dot(a, b):
    return jnp.dot(a, b, preferred_element_type=F32)


def dot_t(a, b):
    return lax.dot_general(a, b, (((1,), (1,)), ((), ())), preferred_element_type=F32)


def lane_row(b_ref, start, n):
    return b_ref[pl.ds(start, n)].astype(F32).reshape(1, n)


def ln_mod_rows(x, scale1p, shift):
    xf = x.astype(F32)
    mean = jnp.mean(xf, axis=-1, keepdims=True)
    cent = xf - mean
    var = jnp.mean(cent * cent, axis=-1, keepdims=True)
    return scale1p * (cent * lax.rsqrt(var + EPS)) + shift


KINDS = (1, 2, 0)


def main_kernel(cfg, x_hbm, xt_hbm, cond_ref, wmi_hbm, wmt_hbm, wi_hbm, wt_hbm, bmi_ref, bmt_ref, bi_ref, bt_ref,
                qg_ref, kg_ref, tqg_ref, tkg_ref, pos_ref, om_ref,
                o_hbm, ot_ref, g2,
                w, xs, xm, xt, kn, kf, km, vn, vf, vm, qn, qf, qm, kb, vb, qb, posm, cos_t, se_t, so_t, cos_m, se_m, so_m,
                mi, mt, g1, mine1, mine2, s0, s1, mx0, mx1, ost, otmp,
                xsem, wsem, msend, mrecv, gsend, grecv, ssem, rsem, fssem, frsem, ossem, orsem):
    tok, txt, d_in, heads, ck, mx = cfg
    nu = tok - mx
    hd_all = heads * HD
    nj = heads // NCHIP
    quad = 4
    wide = quad * HD
    half = tok * NCHIP
    me = lax.axis_index("cp")
    chip, core = me // 2, me % 2
    zh, cl = chip // quad, chip % quad
    sib = chip * 2 + (1 - core)
    mirror_chip = lax.rem(chip + quad, NCHIP)

    def dev(c):
        return {"cp": c * 2 + core}

    barrier = pltpu.get_barrier_semaphore()
    for r in range(1, NDEV):
        pl.semaphore_signal(barrier, inc=1, device_id={"cp": lax.rem(me + r, NDEV)}, device_id_type=MESH)
    load_x = pltpu.make_async_copy(x_hbm, xs, xsem.at[0])
    load_t = pltpu.make_async_copy(xt_hbm, xt, xsem.at[1])

    def x_copy():
        return pltpu.make_async_remote_copy(
            src_ref=x_hbm.at[pl.ds(nu, mx), :], dst_ref=xm, send_sem=msend.at[0], recv_sem=mrecv.at[0],
            device_id=dev(mirror_chip), device_id_type=MESH)

    def pos_copy():
        return pltpu.make_async_remote_copy(
            src_ref=pos_ref.at[pl.ds(nu, mx), :], dst_ref=posm, send_sem=msend.at[1], recv_sem=mrecv.at[1],
            device_id=dev(mirror_chip), device_id_type=MESH)

    mc = 2 * d_in // NDEV

    def tile_copy(what, a, b, slot):
        if what == "mod":
            ref = (wmi_hbm, wmt_hbm)[a]
            off = me * mc if b < 0 else 2 * d_in + me * 2 * mc + b * mc
            return [pltpu.make_async_copy(ref.at[:, pl.ds(pl.multiple_of(off, 128), mc)], w.at[slot, :, pl.ds(0, mc)], wsem.at[slot, 0])]
        if what == "txt":
            return [pltpu.make_async_copy(
                wt_hbm.at[:, pl.ds(pl.multiple_of(a * hd_all + (j * NCHIP + chip) * HD, HD), HD)],
                w.at[slot, :, pl.ds(j * HD, HD)], wsem.at[slot, j]) for j in range(nj)]
        kind, side = a
        off = kind * hd_all + b * NCHIP * HD + (zh if side == 0 else 1 - zh) * wide
        return [pltpu.make_async_copy(wi_hbm.at[:, pl.ds(pl.multiple_of(off, wide), wide)], w.at[slot], wsem.at[slot, 0])]

    def start(*a):
        for c in tile_copy(*a):
            c.start()

    def wait(*a):
        for c in tile_copy(*a):
            c.wait()
        return a[-1]

    def start_own(j, p):
        start("img", (KINDS[p // 2], p % 2), j, (2 + p) % 3)

    def start_txt(t):
        start("txt", KINDS[t], None, (2 + t) % 3)

    def start_mir(j, i):
        start("img", (KINDS[i], 0), j, (2 + i) % 3)

    def start_mod2(t):
        start("mod", t // 2, t % 2, (2 + t) % 3)

    start("mod", 0, -1, 0)
    start("mod", 1, -1, 1)

    c = cond_ref[...].astype(F32)
    act = (c * jax.nn.sigmoid(c)).astype(BF16)
    act = jnp.broadcast_to(act, (16, d_in))
    per = mc // 128

    def mod_rows(slot, buf, row):
        r = dot(act, w[slot, :, 0:mc])
        for i in range(per):
            buf[row + i:row + i + 1, :] = r[0:1, i * 128:(i + 1) * 128]

    def spread(buf, dst, k):
        return [pltpu.make_async_remote_copy(
            src_ref=buf, dst_ref=dst.at[me], send_sem=gsend.at[k, r], recv_sem=grecv.at[k, r],
            device_id={"cp": lax.rem(me + r, NDEV)}, device_id_type=MESH) for r in range(1, NDEV)]

    mine1[...] = jnp.zeros_like(mine1)
    slot = wait("mod", 0, -1, 0)
    load_x.start()
    mod_rows(slot, mine1, 0)
    slot = wait("mod", 1, -1, 1)
    start_own(0, 0)
    start_own(0, 1)
    load_t.start()
    mod_rows(slot, mine1, per)
    pl.semaphore_wait(barrier, NDEV - 1)
    gath1 = spread(mine1, g1, 0)
    for cp in gath1:
        cp.start()
    pos_copy().start()
    x_copy().start()
    g1[me] = mine1[...]

    def tables(pos, n, cos_t, se_t, so_t):
        ang = pos.astype(F32) * om_ref[...]
        odd = lax.rem(lax.broadcasted_iota(jnp.int32, ang.shape, 1), 2) == 1
        sin = jnp.sin(ang)
        cos_t[0:n, :] = jnp.cos(ang)
        se_t[0:n, :] = jnp.where(odd, 0.0, -sin)
        so_t[0:n, :] = jnp.where(odd, sin, 0.0)

    tables(pos_ref[...], tok, cos_t, se_t, so_t)
    for b_ref, m in ((bmi_ref, mi), (bmt_ref, mt)):
        for k in range(2):
            m[k:k + 1, :] = lane_row(b_ref, k * d_in, d_in)
    for cp in gath1:
        cp.wait()
    for b, m in ((0, mi), (1, mt)):
        for dv in range(NDEV):
            for r in range(per):
                col = (dv * per + r) * 128
                at = (slice(col // d_in, col // d_in + 1), slice(col % d_in, col % d_in + 128))
                m[at] = m[at] + g1[dv, b * per + r:b * per + r + 1, :]

    rb = 32

    def ln_rows(ref, m_ref, n):
        shift = m_ref[0:1, :]
        scale = 1.0 + m_ref[1:2, :]

        def body(i, carry):
            sl = pl.ds(pl.multiple_of(i * rb, rb), rb)
            ref[sl, :] = ln_mod_rows(ref[sl, :], scale, shift).astype(BF16)
            return carry
        lax.fori_loop(0, n // rb, body, 0)

    def norm_rope(y, gain, tabs):
        ms = jnp.mean(y * y, axis=-1, keepdims=True)
        y = y * lax.rsqrt(ms + EPS) * gain
        if tabs is not None:
            n = y.shape[0]
            y = y * tabs[0][0:n, :] + pltpu.roll(y, HD - 1, 1) * tabs[1][0:n, :] + pltpu.roll(y, 1, 1) * tabs[2][0:n, :]
        return y

    def place(kind, s_chip, row, n, j):
        if kind == 0:
            return qb.at[j, pl.ds(pl.multiple_of(txt + s_chip * tok + row, 128), n)]
        at = pl.multiple_of(txt + core * half + s_chip * tok + row, 128)
        return kb.at[j, pl.ds(at, n)] if kind == 1 else vb.at[j, :, pl.ds(at, n)]

    def qkv_copy(kind, ty, j, src_cl, src_zh, dst_cl, idx):
        buf = ((qn, qf, qm), (kn, kf, km), (vn, vf, vm))[kind][ty]
        n = (tok, nu, mx)[ty]
        s_chip = src_zh * quad + src_cl
        tgt = (1 - src_zh if ty == 1 else src_zh) * quad + dst_cl
        if ty == 2:
            dst = place(kind, lax.rem(s_chip + quad, NCHIP), nu, n, j)
        else:
            dst = place(kind, s_chip, 0, n, j)
        return pltpu.make_async_remote_copy(
            src_ref=buf.at[j * quad + dst_cl], dst_ref=dst, send_sem=ssem.at[kind, ty, j, idx[0]],
            recv_sem=rsem.at[kind, ty, j, idx[1]], device_id=dev(tgt), device_id_type=MESH)

    def out_copies(kind, ty, j):
        if ty == 1:
            return [qkv_copy(kind, 1, j, cl, zh, c, (c, cl)) for c in range(quad)]
        return [qkv_copy(kind, ty, j, cl, zh, lax.rem(cl + r, quad), (r, r)) for r in range(1, quad)]

    def in_copies(kind, ty, j):
        if ty == 1:
            return [qkv_copy(kind, 1, j, c, 1 - zh, cl, (c, c)) for c in range(quad)]
        return [qkv_copy(kind, ty, j, lax.rem(cl + quad - r, quad), zh, cl, (r, r)) for r in range(1, quad)]

    def own_copy(kind, ty, j):
        buf = ((qn, qf, qm), (kn, kf, km), (vn, vf, vm))[kind][ty]
        n = (tok, nu, mx)[ty]
        dst = place(kind, mirror_chip, nu, n, j) if ty == 2 else place(kind, chip, 0, n, j)
        dst[...] = buf[j * quad + cl]

    def make(kind, ty, j, slot):
        src = xm if ty == 2 else xs
        n = (tok, nu, mx)[ty]
        buf = ((qn, qf, qm), (kn, kf, km), (vn, vf, vm))[kind][ty]

        def cols(p, carry):
            col = pl.multiple_of(p * 2 * HD, 2 * HD)
            boff = kind * hd_all + j * NCHIP * HD + (1 - zh if ty == 1 else zh) * wide + col
            y2 = dot(src[0:n, :], w[slot, :, pl.ds(col, 2 * HD)]) + lane_row(bi_ref, pl.multiple_of(boff, 256), 2 * HD)
            for hh in range(2):
                y = y2[:, hh * HD:(hh + 1) * HD]
                if kind == 2:
                    buf[j * quad + 2 * p + hh] = y.T.astype(BF16)
                else:
                    gain = (qg_ref, kg_ref)[kind][...].astype(F32).reshape(1, HD)
                    buf[j * quad + 2 * p + hh] = norm_rope(y, gain, (cos_m, se_m, so_m) if ty == 2 else (cos_t, se_t, so_t)).astype(BF16)
            return carry
        lax.fori_loop(0, 2, cols, 0)

    load_x.wait()
    ln_rows(xs, mi, tok)

    last = nj - 1
    mir_after = 0

    def text_rows():
        load_t.wait()
        ln_rows(xt, mt, txt)
        for t, kind in enumerate(KINDS):
            if t == 0:
                start_txt(2)
            elif mir_after > 0:
                start_own(1, t - 1)
            else:
                start_mir(0, t - 1)
            slot = wait("txt", kind, None, (2 + t) % 3)
            y3 = dot(xt[...], w[slot, :, 0:nj * HD])
            for j in range(nj):
                pair0 = kind * hd_all + (j * NCHIP + chip - lax.rem(chip, 2)) * HD
                b2 = lane_row(bt_ref, pl.multiple_of(pair0, 256), 2 * HD)
                y = y3[:, j * HD:(j + 1) * HD] + jnp.where(lax.rem(chip, 2) == 0, b2[:, 0:HD], b2[:, HD:2 * HD])
                if kind == 2:
                    vb[j, :, 0:txt] = y.T.astype(BF16)
                else:
                    gain = (tqg_ref, tkg_ref)[kind][...].astype(F32).reshape(1, HD)
                    (qb, kb)[kind][j, 0:txt] = norm_rope(y, gain, None).astype(BF16)

    def mirror_rows():
        pos_copy().wait_recv()
        tables(posm[...], mx, cos_m, se_m, so_m)
        x_copy().wait_recv()
        ln_rows(xm, mi, mx)

        lax.fori_loop(0, nj, mir_pass, 0)

    def mir_pass(j, carry):
        for i, kind in enumerate(KINDS):
            if i == 0:
                start_mir(j, 2)
            else:
                @pl.when(j < nj - 1)
                def _():
                    start_mir(j + 1, i - 1)

                @pl.when(j == nj - 1)
                def _():
                    if mir_after < last:
                        start_own(mir_after + 1, i - 1)
                    else:
                        start_mod2(i - 1)
            slot = wait("img", (kind, 0), j, (2 + i) % 3)
            make(kind, 2, j, slot)
            for cp in out_copies(kind, 2, j):
                cp.start()
            own_copy(kind, 2, j)
        return carry

    def after_own(j, p):
        @pl.when(j == 0)
        def _():
            start_txt(p)

        if mir_after > 0:
            @pl.when(j == mir_after)
            def _():
                start_mir(0, p)

        @pl.when((j > mir_after) & (j < last))
        def _():
            start_own(j + 1, p)

        if last > mir_after:
            @pl.when(j == last)
            def _():
                start_mod2(p)

    def own_pass(j, carry):
        for p in range(6):
            kind, side = KINDS[p // 2], p % 2
            if p + 2 < 6:
                start_own(j, p + 2)
            else:
                after_own(j, p - 4)
            slot = wait("img", (kind, side), j, (2 + p) % 3)
            make(kind, side, j, slot)
            for cp in out_copies(kind, side, j):
                cp.start()
            if side == 0:
                own_copy(kind, 0, j)

        pl.when(j == 0)(text_rows)
        pl.when(j == mir_after)(mirror_rows)
        return carry
    lax.fori_loop(0, nj, own_pass, 0)

    mine2[...] = jnp.zeros_like(mine2)
    for t in range(4):
        if t + 2 < 4:
            start_mod2(t + 2)
        mod_rows(wait("mod", t // 2, t % 2, (2 + t) % 3), mine2, t * per)
    gath2 = spread(mine2, g2, 1)
    for cp in gath2:
        cp.start()
    g2[me] = mine2[...]

    scale2 = (HD ** -0.5) * 1.4426950408889634
    keys = txt + 2 * half
    nchunk = keys // ck
    qt = 256
    ntile = (txt + half) // qt
    group = 2 * tok // qt
    ngroup = NCHIP // 2

    def to_sibling(kind, j):
        ref = (kb.at[j, pl.ds(pl.multiple_of(txt + core * half, 128), half)] if kind == 1
               else vb.at[j, :, pl.ds(pl.multiple_of(txt + core * half, 128), half)])
        return pltpu.make_async_remote_copy(
            src_ref=ref, dst_ref=ref, send_sem=fssem.at[kind - 1, j], recv_sem=frsem.at[kind - 1, j],
            device_id={"cp": sib}, device_id_type=MESH)

    def collect(j):
        for kind in KINDS:
            for ty in range(3):
                for cp in in_copies(kind, ty, j):
                    cp.wait_recv()
            if kind != 0:
                to_sibling(kind, j).start()

    def tile_start(t):
        g = (t - 1) // group
        plane = lax.rem(chip // 2 + 1 + g, ngroup)
        row = txt + plane * (2 * tok) + lax.rem(t - 1, group) * qt
        return pl.multiple_of(jnp.where(t == 0, 0, row), 128)

    def qk(j, q, i, s_ref, mxv):
        sl = pl.ds(pl.multiple_of(i * ck, ck), ck)
        s = dot_t(kb[j, sl], q)
        s_ref[sl, :] = s
        return jnp.maximum(mxv, jnp.max(s.reshape(ck // 8, 8, qt), axis=0))

    def sm(j, i, s_ref, m, lsum, acc):
        sl = pl.ds(pl.multiple_of(i * ck, ck), ck)
        p = jnp.exp2((s_ref[sl, :] - m) * scale2)
        lsum = lsum + jnp.sum(p.reshape(ck // 8, 8, qt), axis=0)
        acc = acc + dot(vb[j, :, sl], p.astype(BF16))
        return lsum, acc

    def new_max():
        return jnp.full((8, qt), -jnp.inf, F32)

    def o_remote(j, c_src, c_dst):
        src = ost.at[j, pl.ds(pl.multiple_of(c_dst * tok, 128), tok)]
        dst = o_hbm.at[:, pl.ds(pl.multiple_of((j * NCHIP + c_src) * HD, HD), HD)]
        return pltpu.make_async_remote_copy(
            src_ref=src, dst_ref=dst, send_sem=ossem.at[j, c_dst], recv_sem=orsem.at[j, c_src],
            device_id=dev(c_dst), device_id_type=MESH)

    def o_local(j):
        src = ost.at[j, pl.ds(pl.multiple_of(chip * tok, 128), tok)]
        dst = o_hbm.at[:, pl.ds(pl.multiple_of((j * NCHIP + chip) * HD, HD), HD)]
        return pltpu.make_async_copy(src, dst, ossem.at[j, chip])

    def o_send(j, g):
        plane = lax.rem(chip // 2 + 1 + g, ngroup)
        for y in range(2):
            c = plane * 2 + y

            @pl.when(c != chip)
            def _():
                o_remote(j, chip, c).start()

            @pl.when(c == chip)
            def _():
                o_local(j).start()

    def finish(j, t, lsum, acc):
        tot = jnp.sum(lsum, axis=0, keepdims=True)
        o = (acc / tot).T.astype(BF16)

        @pl.when(t == 0)
        def _():
            otmp[...] = o
            ot_ref[j] = otmp[pl.ds(pl.multiple_of(core * (txt // 2), 8), txt // 2), :]

        @pl.when(t > 0)
        def _():
            ost[j, pl.ds(pl.multiple_of(tile_start(t) - txt, 128), qt)] = o

            @pl.when(lax.rem(t, group) == 0)
            def _():
                o_send(j, t // group - 1)

    def pair(j, t, s_cur, mx_cur, s_nxt, mx_nxt, has_next):
        m = jnp.max(mx_cur[...], axis=0, keepdims=True)
        lsum = jnp.zeros((8, qt), F32)
        acc = jnp.zeros((HD, qt), F32)
        if has_next:
            q = qb[j, pl.ds(tile_start(t + 1), qt)]

            def body(i, carry):
                lsum, acc, mxv = carry
                mxv = qk(j, q, i, s_nxt, mxv)
                lsum, acc = sm(j, i, s_cur, m, lsum, acc)
                return lsum, acc, mxv
            lsum, acc, mxv = lax.fori_loop(0, nchunk, body, (lsum, acc, new_max()))
            mx_nxt[...] = mxv
        else:
            def body(i, carry):
                return sm(j, i, s_cur, m, *carry)
            lsum, acc = lax.fori_loop(0, nchunk, body, (lsum, acc))
        finish(j, t, lsum, acc)

    collect(0)

    def head(j, carry):
        for kind in (1, 2):
            to_sibling(kind, j).wait()
        q = qb[j, 0:qt]

        def first(i, mxv):
            return qk(j, q, i, s0, mxv)
        mx0[...] = lax.fori_loop(0, nchunk, first, new_max())

        def two(i, carry):
            pair(j, 2 * i, s0, mx0, s1, mx1, True)
            pair(j, 2 * i + 1, s1, mx1, s0, mx0, True)
            return carry
        lax.fori_loop(0, (ntile - 1) // 2, two, 0)
        if nj > 1:
            @pl.when(j < nj - 1)
            def _():
                collect(j + 1)
        pair(j, jnp.int32(ntile - 1), s0, mx0, s1, mx1, False)
        return carry
    lax.fori_loop(0, nj, head, 0)

    for cp in gath2:
        cp.wait()
    x_copy().wait_send()
    pos_copy().wait_send()

    def drain(j, carry):
        for kind in KINDS:
            for ty in range(3):
                for cp in out_copies(kind, ty, j):
                    cp.wait_send()
        o_local(j).wait()
        for r in range(1, NCHIP):
            c = lax.rem(chip + r, NCHIP)
            o_remote(j, chip, c).wait_send()
            o_remote(j, c, chip).wait_recv()
        return carry
    lax.fori_loop(0, nj, drain, 0)


def attention(image, text, cond_vec, wm_img, wm_txt, w_img, w_txt, flat, pos, omega):
    tok, d_in = image.shape
    txt = text.shape[0]
    hd_all = w_img.shape[1] // 3
    heads = hd_all // HD
    nj = heads // NCHIP
    half = tok * NCHIP
    keys = txt + 2 * half
    ck = 3200
    mx = tok // 3
    nu = tok - mx
    cfg = (tok, txt, d_in, heads, ck, mx)
    dma = pltpu.SemaphoreType.DMA
    flops = 2 * tok * d_in * 3 * hd_all + 4 * nj * HD * (half + txt) * keys
    per = 2 * d_in // NDEV // 128
    r1, r2 = -(-2 * per // 8) * 8, -(-4 * per // 8) * 8
    row_sets = [pltpu.VMEM((nj * 4, n, HD), BF16) for n in (tok, nu, mx)]
    col_sets = [pltpu.VMEM((nj * 4, HD, n), BF16) for n in (tok, nu, mx)]
    table = pltpu.VMEM((tok, 128), F32)
    return pl.pallas_call(
        functools.partial(main_kernel, cfg),
        out_shape=(jax.ShapeDtypeStruct((tok, hd_all), BF16), jax.ShapeDtypeStruct((nj, txt // 2, HD), BF16),
                   jax.ShapeDtypeStruct((NDEV, r2, 128), F32)),
        in_specs=[ANY, ANY, VM, ANY, ANY, ANY, ANY] + [VM] * 10,
        out_specs=(ANY, VM, VM),
        scratch_shapes=[
            pltpu.VMEM((3, d_in, 4 * HD), BF16),
            pltpu.VMEM((tok, d_in), BF16), pltpu.VMEM((mx, d_in), BF16), pltpu.VMEM((txt, d_in), BF16),
            *row_sets, *col_sets, *row_sets,
            pltpu.VMEM((nj, keys, HD), BF16), pltpu.VMEM((nj, HD, keys), BF16), pltpu.VMEM((nj, txt + half, HD), BF16),
            pltpu.VMEM((mx, 128), BF16), table, table, table, *[pltpu.VMEM((mx, 128), F32)] * 3,
            pltpu.VMEM((2, d_in), F32), pltpu.VMEM((2, d_in), F32),
            pltpu.VMEM((NDEV, r1, 128), F32), pltpu.VMEM((r1, 128), F32), pltpu.VMEM((r2, 128), F32),
            pltpu.VMEM((keys, 256), F32), pltpu.VMEM((keys, 256), F32), pltpu.VMEM((8, 256), F32), pltpu.VMEM((8, 256), F32),
            pltpu.VMEM((nj, half, HD), BF16), pltpu.VMEM((txt, HD), BF16),
            dma((2,)), dma((3, max(nj, 1))), dma((2,)), dma((2,)), dma((2, NDEV)), dma((2, NDEV)),
            dma((3, 3, nj, 4)), dma((3, 3, nj, 4)), dma((2, nj)), dma((2, nj)), dma((nj, NCHIP)), dma((nj, NCHIP)),
        ],
        compiler_params=pltpu.CompilerParams(collective_id=1, has_side_effects=True, vmem_limit_bytes=VMEM_LIMIT),
        cost_estimate=pl.CostEstimate(flops=flops, bytes_accessed=3 * d_in * 3 * hd_all, transcendentals=0),
        name="attn",
    )(image, text, cond_vec, wm_img, wm_txt, w_img, w_txt, *flat, pos, omega)


def gelu(x):
    return x * (0.5 * (1.0 + jnp.tanh(0.7978845608028654 * (x + 0.044715 * (x * x * x)))))


def out_kernel(cfg, o_hbm, x_hbm, xt_hbm, ot_ref, g2_ref, bmi_ref, bmt_ref, bp_ref, tbp_ref, b1_ref, tb1_ref, b2_ref, tb2_ref, wp_hbm, w1_hbm, w2_hbm, twp_hbm, tw1_hbm, tw2_hbm,
               out_ref, tout_ref, mi_ref, mt_ref,
               wa, wb, wc, o, x, h, z, acc, a0, a1, o_t, x_t, h_t, z_t, a_t, part, rs, row,
               asem, bsem, csem, lsem, ossem, orsem, pssem, prsem, rssem, rrsem, fssem, frsem):
    tok, txt, d, ff, k1, k2 = cfg
    me = lax.axis_index("cp")
    chip, core = me // 2, me % 2
    sib = chip * 2 + (1 - core)
    rows = txt // 2
    quad = 4
    cl, zq = chip % quad, chip // quad * quad
    piece = rows // quad
    nb = wa.shape[2]
    na = wa.shape[0]
    np_ = d // nb
    nf = ff // nb
    ft = ff // quad
    nt = ft // nb
    nj = ot_ref.shape[0]

    def dev(c):
        return {"cp": c * 2 + core}

    off = pl.multiple_of(cl * ft, nb)

    def start_a(p):
        slot = lax.rem(p, na)

        @pl.when(p < np_)
        def _():
            pltpu.make_async_copy(wp_hbm.at[:, pl.ds(pl.multiple_of(p * nb, nb), nb)], wa.at[slot], asem.at[slot]).start()

        @pl.when((p >= np_) & (p < np_ + nf))
        def _():
            pltpu.make_async_copy(w1_hbm.at[:, pl.ds(pl.multiple_of((p - np_) * nb, nb), nb)], wa.at[slot], asem.at[slot]).start()

    def start_b(p):
        slot = lax.rem(p, na)

        @pl.when(p < nf)
        def _():
            pltpu.make_async_copy(w2_hbm.at[pl.ds(pl.multiple_of(p * nb, nb), nb), :], wb.at[slot], bsem.at[slot]).start()

    def c_fc2(p, slot):
        return pltpu.make_async_copy(tw2_hbm.at[pl.ds(off, ft), pl.ds(pl.multiple_of(p * nb, nb), nb)],
                                     wc.at[slot, pl.ds(0, ft), :], csem.at[slot])

    def start_c(p):
        slot = lax.rem(p, na)

        @pl.when(p < np_)
        def _():
            pltpu.make_async_copy(twp_hbm.at[:, pl.ds(pl.multiple_of(p * nb, nb), nb)], wc.at[slot], csem.at[slot]).start()

        @pl.when((p >= np_) & (p < np_ + nt))
        def _():
            pltpu.make_async_copy(tw1_hbm.at[:, pl.ds(pl.multiple_of(off + (p - np_) * nb, nb), nb)], wc.at[slot], csem.at[slot]).start()

        @pl.when((p >= np_ + nt) & (p < np_ + nt + np_))
        def _():
            c_fc2(p - np_ - nt, slot).start()

    def get_a(p):
        start_a(p + na - 1)
        slot = lax.rem(p, na)
        pltpu.make_async_copy(w1_hbm.at[:, 0:nb], wa.at[slot], asem.at[slot]).wait()
        return slot

    def get_b(p):
        start_b(p + na - 1)
        slot = lax.rem(p, na)
        pltpu.make_async_copy(w2_hbm.at[0:nb, :], wb.at[slot], bsem.at[slot]).wait()
        return slot

    def get_c(p, fc2=False):
        start_c(p + na - 1)
        slot = lax.rem(p, na)
        if fc2:
            c_fc2(0, slot).wait()
        else:
            pltpu.make_async_copy(w1_hbm.at[:, 0:nb], wc.at[slot], csem.at[slot]).wait()
        return slot

    load_o = pltpu.make_async_copy(o_hbm, o, lsem.at[0])
    load_x = pltpu.make_async_copy(x_hbm, x, lsem.at[1])
    load_t = pltpu.make_async_copy(xt_hbm.at[pl.ds(pl.multiple_of(core * rows, 8), rows), :], x_t, lsem.at[2])
    load_o.start()
    start_a(jnp.int32(0))
    load_x.start()
    for p in range(1, na - 1):
        start_a(jnp.int32(p))

    barrier = pltpu.get_barrier_semaphore()
    for r in range(1, NCHIP):
        pl.semaphore_signal(barrier, inc=1, device_id=dev(lax.rem(chip + r, NCHIP)), device_id_type=MESH)
    pl.semaphore_signal(barrier, inc=1, device_id={"cp": sib}, device_id_type=MESH)
    pl.semaphore_wait(barrier, NCHIP)

    def o_copy(j, r, c_src, c_dst):
        return pltpu.make_async_remote_copy(
            src_ref=ot_ref.at[j], dst_ref=o_t.at[:, pl.ds(pl.multiple_of((j * NCHIP + c_src) * HD, HD), HD)],
            send_sem=ossem.at[j, r], recv_sem=orsem.at[j, r], device_id=dev(c_dst), device_id_type=MESH)

    for j in range(nj):
        for r in range(1, NCHIP):
            o_copy(j, r, chip, lax.rem(chip + r, NCHIP)).start()
        o_t[:, pl.ds(pl.multiple_of((j * NCHIP + chip) * HD, HD), HD)] = ot_ref[j]

    per = 4 * d // NDEV // 128
    for b, (b_ref, m) in enumerate(((bmi_ref, mi_ref), (bmt_ref, mt_ref))):
        for k in range(2, 6):
            m[k:k + 1, :] = lane_row(b_ref, k * d, d)
        for dv in range(NDEV):
            for r in range(per):
                col = 2 * d + (dv * per + r) * 128
                at = (slice(col // d, col // d + 1), slice(col % d, col % d + 128))
                m[at] = m[at] + g2_ref[dv, b * per + r:b * per + r + 1, :]

    load_o.wait()
    load_x.wait()

    def proj(p, carry):
        slot = get_a(p)
        sl = pl.ds(pl.multiple_of(p * nb, nb), nb)

        @pl.when(p == 0)
        def _():
            load_t.start()

        @pl.when((p > 0) & (p < na))
        def _():
            start_b(p - 1)

        @pl.when((p >= na) & (p < 2 * na - 1))
        def _():
            start_c(p - na)
        y = dot(o[...], wa[slot]) + lane_row(bp_ref, pl.multiple_of(p * nb, nb), nb)
        h[:, sl] = x[:, sl].astype(F32) + mi_ref[2:3, sl] * y
        acc[:, sl] = jnp.broadcast_to(lane_row(b2_ref, pl.multiple_of(p * nb, nb), nb), (tok, nb))
        return carry
    lax.fori_loop(0, np_, proj, 0)

    def ln2(src, dst, m_ref, n):
        shift, scale = m_ref[3:4, :], 1.0 + m_ref[4:5, :]
        rb = 32

        def body(i, carry):
            r = pl.ds(pl.multiple_of(i * rb, rb), rb)
            dst[r, :] = ln_mod_rows(src[r, :], scale, shift).astype(BF16)
            return carry
        lax.fori_loop(0, n // rb, body, 0)

    ln2(h, z, mi_ref, tok)

    def tproj(p, carry):
        slot = get_c(p)
        sl = pl.ds(pl.multiple_of(p * nb, nb), nb)
        y = dot(o_t[...], wc[slot]) + lane_row(tbp_ref, pl.multiple_of(p * nb, nb), nb)
        h_t[:, sl] = x_t[:, sl].astype(F32) + mt_ref[2:3, sl] * y
        return carry

    def tfc1(p, carry):
        slot = get_c(np_ + p)
        col = pl.multiple_of(p * nb, nb)
        y = dot(z_t[...], wc[slot]) + lane_row(tb1_ref, pl.multiple_of(off + col, nb), nb)
        a_t[:, pl.ds(col, nb)] = gelu(y).astype(BF16)
        return carry

    def tfc2(p, carry):
        slot = get_c(np_ + nt + p, True)
        part[:, pl.ds(pl.multiple_of(p * nb, nb), nb)] = dot(a_t[...], wc[slot, 0:ft, :])
        return carry

    def p_copy(r, c_src, c_dst):
        return pltpu.make_async_remote_copy(
            src_ref=part.at[pl.ds(pl.multiple_of(c_dst * piece, 8), piece), :], dst_ref=rs.at[c_src],
            send_sem=pssem.at[r], recv_sem=prsem.at[r], device_id=dev(zq + c_dst), device_id_type=MESH)

    def r_copy(r, c_src, c_dst):
        return pltpu.make_async_remote_copy(
            src_ref=row, dst_ref=tout_ref.at[pl.ds(pl.multiple_of(core * rows + c_src * piece, 8), piece), :],
            send_sem=rssem.at[r], recv_sem=rrsem.at[r], device_id=dev(zq + c_dst), device_id_type=MESH)

    mine = pl.ds(pl.multiple_of(cl * piece, 8), piece)
    n1, n2, n3 = np_ // 2, np_ // 2 + nt // 2, np_ + nt // 2

    def text_step(s):
        @pl.when(s == 0)
        def _():
            load_t.wait()
            for j in range(nj):
                for r in range(1, NCHIP):
                    o_copy(j, r, lax.rem(chip + NCHIP - r, NCHIP), chip).wait_recv()

        @pl.when((s >= 0) & (s < n1))
        def _():
            lax.fori_loop(2 * s, 2 * s + 2, tproj, 0)

        @pl.when(s == n1)
        def _():
            ln2(h_t, z_t, mt_ref, rows)

        @pl.when((s >= n1) & (s < n2))
        def _():
            lax.fori_loop(2 * (s - n1), 2 * (s - n1) + 2, tfc1, 0)

        @pl.when((s >= n2) & (s < n3))
        def _():
            lax.fori_loop(2 * (s - n2), 2 * (s - n2) + 2, tfc2, 0)

        @pl.when(s == n3 - 1)
        def _():
            for r in range(1, quad):
                p_copy(r, cl, lax.rem(cl + r, quad)).start()
            rs[cl] = part[mine, :]

        @pl.when(s == k2)
        def _():
            for r in range(1, quad):
                p_copy(r, lax.rem(cl + quad - r, quad), cl).wait_recv()
            tot = rs[0]
            for c in range(1, quad):
                tot = tot + rs[c]
            y = h_t[mine, :] + mt_ref[5:6, :] * (tot + lane_row(tb2_ref, 0, d))
            row[...] = y.astype(BF16)
            for r in range(1, quad):
                r_copy(r, cl, lax.rem(cl + r, quad)).start()
            tout_ref[pl.ds(pl.multiple_of(core * rows + cl * piece, 8), piece), :] = row[...]

    def mlp(i, a_new, a_old):
        slot_b = get_b(i - 1)
        slot_a = get_a(np_ + i)
        hn, hd = nb // 2, d // 2
        for s in range(2):
            c1, c2 = slice(s * hn, (s + 1) * hn), slice(s * hd, (s + 1) * hd)
            b1 = lane_row(b1_ref, pl.multiple_of(i * nb + s * hn, hn), hn)
            a_new[:, c1] = gelu(dot(z[...], wa[slot_a, :, c1]) + b1).astype(BF16)
            acc[:, c2] += dot(a_old[...], wb[slot_b, :, c2])

    slot = get_a(jnp.int32(np_))
    a0[...] = gelu(dot(z[...], wa[slot]) + lane_row(b1_ref, 0, nb)).astype(BF16)

    def two(k, carry):
        mlp(2 * k + 1, a1, a0)
        text_step(2 * k - k1)
        mlp(2 * k + 2, a0, a1)
        text_step(2 * k + 1 - k1)
        return carry
    lax.fori_loop(0, nf // 2 - 1, two, 0)
    mlp(jnp.int32(nf - 1), a1, a0)

    for r in range(1, quad):
        r_copy(r, lax.rem(cl + quad - r, quad), cl).wait_recv()
    ref = tout_ref.at[pl.ds(pl.multiple_of(core * rows, 8), rows), :]
    fwd = pltpu.make_async_remote_copy(src_ref=ref, dst_ref=ref, send_sem=fssem, recv_sem=frsem,
                                       device_id={"cp": sib}, device_id_type=MESH)
    fwd.start()

    slot = get_b(jnp.int32(nf - 1))
    y = acc[...] + dot(a1[...], wb[slot])
    out_ref[...] = (h[...] + mi_ref[5:6, :] * y).astype(BF16)

    fwd.wait()
    for j in range(nj):
        for r in range(1, NCHIP):
            o_copy(j, r, chip, lax.rem(chip + r, NCHIP)).wait_send()
    for r in range(1, quad):
        c = lax.rem(cl + r, quad)
        p_copy(r, cl, c).wait_send()
        r_copy(r, cl, c).wait_send()


def output(o_img, image, text, o_txt, g2, flat, wp, w1, w2, twp, tw1, tw2):
    tok, d = image.shape
    txt = text.shape[0]
    ff = w1.shape[1]
    nb = 512
    nf = ff // nb
    k1, k2 = (2, 16) if nf > 8 else (0, 5)
    na = 3
    rows = txt // 2
    ft = ff // 4
    nj = o_txt.shape[0]
    dma = pltpu.SemaphoreType.DMA
    flops = 2 * tok * d * (d + 2 * ff) + 2 * rows * d * (d + 2 * ft)
    return pl.pallas_call(
        functools.partial(out_kernel, (tok, txt, d, ff, k1, k2)),
        out_shape=(jax.ShapeDtypeStruct((tok, d), BF16), jax.ShapeDtypeStruct((txt, d), BF16)),
        in_specs=[ANY, ANY, ANY, VM, VM] + [VM] * 8 + [ANY] * 6,
        out_specs=(VM, VM),
        scratch_shapes=[
            pltpu.VMEM((6, d), F32), pltpu.VMEM((6, d), F32),
            pltpu.VMEM((na, d, nb), BF16), pltpu.VMEM((na, nb, d), BF16), pltpu.VMEM((na, d, nb), BF16),
            pltpu.VMEM((tok, d), BF16), pltpu.VMEM((tok, d), BF16), pltpu.VMEM((tok, d), F32), pltpu.VMEM((tok, d), BF16),
            pltpu.VMEM((tok, d), F32), pltpu.VMEM((tok, nb), BF16), pltpu.VMEM((tok, nb), BF16),
            pltpu.VMEM((rows, d), BF16), pltpu.VMEM((rows, d), BF16), pltpu.VMEM((rows, d), F32), pltpu.VMEM((rows, d), BF16),
            pltpu.VMEM((rows, ft), BF16), pltpu.VMEM((rows, d), F32), pltpu.VMEM((4, rows // 4, d), F32),
            pltpu.VMEM((rows // 4, d), BF16),
            dma((na,)), dma((na,)), dma((na,)), dma((3,)), dma((nj, NCHIP)), dma((nj, NCHIP)), dma((NCHIP,)), dma((NCHIP,)),
            dma((NCHIP,)), dma((NCHIP,)), dma, dma,
        ],
        compiler_params=pltpu.CompilerParams(collective_id=2, has_side_effects=True, vmem_limit_bytes=VMEM_LIMIT),
        cost_estimate=pl.CostEstimate(flops=flops, bytes_accessed=2 * d * (d + 2 * ff), transcendentals=0),
        name="out",
    )(o_img, image, text, o_txt, g2, *flat, wp, w1, w2, twp, tw1, tw2)


def pass_kernel(parts, a_hbm, b_hbm, oa_hbm, ob_hbm, a, b, isem, osem):
    moves = []
    for k, (src, dst, buf) in enumerate(((a_hbm, oa_hbm, a), (b_hbm, ob_hbm, b))):
        n = src.shape[0] // parts
        for i in range(parts):
            sl = pl.ds(i * n, n)
            moves.append((pltpu.make_async_copy(src.at[sl, :], buf.at[sl, :], isem.at[k, i]),
                          pltpu.make_async_copy(buf.at[sl, :], dst.at[sl, :], osem.at[k, i])))
    for load, _ in moves:
        load.start()
    for load, store in moves:
        load.wait()
        store.start()
    for _, store in moves:
        store.wait()


def pass_results(a, b):
    parts = 4
    dma = pltpu.SemaphoreType.DMA
    return pl.pallas_call(
        functools.partial(pass_kernel, parts),
        out_shape=(jax.ShapeDtypeStruct(a.shape, a.dtype), jax.ShapeDtypeStruct(b.shape, b.dtype)),
        in_specs=[ANY, ANY],
        out_specs=(ANY, ANY),
        scratch_shapes=[pltpu.VMEM(a.shape, a.dtype), pltpu.VMEM(b.shape, b.dtype), dma((2, parts)), dma((2, parts))],
        compiler_params=pltpu.CompilerParams(vmem_limit_bytes=VMEM_LIMIT),
        name="results",
    )(a, b)


def rope_inputs(ids):
    d_t = HD // 8
    d_s = (HD - d_t) // 2
    widths = (d_t, d_s, d_s)
    lane = lax.broadcasted_iota(jnp.int32, (1, HD), 1)
    pos = jnp.where(lane < d_t, ids[:, 0:1], jnp.where(lane < d_t + d_s, ids[:, 1:2], ids[:, 2:3])).astype(BF16)
    omega = np.concatenate([np.repeat(THETA ** (-np.arange(0, w, 2, dtype=np.float32) / np.float32(w)), 2) for w in widths])
    return pos, jnp.asarray(omega.astype(np.float32)[None, :])


def device_fn(image, text, cond_vec, image_ids, *weights):
    (wm, bm, wqkv, bqkv, qg, kg, wp, bp, w1, b1, w2, b2) = weights[:12]
    (twm, tbm, twqkv, tbqkv, tqg, tkg, twp, tbp, tw1, tb1, tw2, tb2) = weights[12:]
    x, xt = image[0], text[0]
    pos, omega = rope_inputs(image_ids)
    o_img, o_txt, g2 = attention(x, xt, cond_vec, wm, twm, wqkv, twqkv, (bm, tbm, bqkv, tbqkv, qg, kg, tqg, tkg), pos, omega)
    image_out, text_out = output(o_img, x, xt, o_txt, g2, (bm, tbm, bp, tbp, b1, tb1, b2, tb2), wp, w1, w2, twp, tw1, tw2)
    image_out, text_out = pass_results(image_out, text_out)
    return image_out[None], text_out[None]


def solution(mesh):
    act = P("dp", "cp", None)
    txt = P("dp", None, None)
    in_specs = (act, txt, P("dp", None), P(("dp", "cp"), None)) + (P(),) * 24
    return jax.shard_map(device_fn, mesh=mesh, in_specs=in_specs, out_specs=(act, txt), check_vma=False)
```

```python
import functools

import jax
import jax.numpy as jnp
import numpy as np
from jax import lax
from jax.experimental import pallas as pl
from jax.experimental.pallas import tpu as pltpu
from jax.sharding import PartitionSpec as P

EPS = 1e-6
THETA = 10000.0
F32 = jnp.float32
BF16 = jnp.bfloat16
HD = 128
NCHIP = 8
NDEV = 16
VM = pl.BlockSpec(memory_space=pltpu.VMEM)
ANY = pl.BlockSpec(memory_space=pl.ANY)
MESH = pl.DeviceIdType.MESH
VMEM_LIMIT = 67043328


def dot(a, b):
    return jnp.dot(a, b, preferred_element_type=F32)


def dot_t(a, b):
    return lax.dot_general(a, b, (((1,), (1,)), ((), ())), preferred_element_type=F32)


def lane_row(b_ref, start, n):
    return b_ref[pl.ds(start, n)].astype(F32).reshape(1, n)


def ln_mod_rows(x, scale1p, shift):
    xf = x.astype(F32)
    mean = jnp.mean(xf, axis=-1, keepdims=True)
    cent = xf - mean
    var = jnp.mean(cent * cent, axis=-1, keepdims=True)
    return scale1p * (cent * lax.rsqrt(var + EPS)) + shift


KINDS = (1, 2, 0)


def main_kernel(cfg, x_hbm, xt_hbm, cond_ref, wmi_hbm, wmt_hbm, wi_hbm, wt_hbm, bmi_ref, bmt_ref, bi_ref, bt_ref,
                qg_ref, kg_ref, tqg_ref, tkg_ref, pos_ref, om_ref,
                o_hbm, ot_ref, g2,
                w, xs, xm, xt, kn, kf, km, vn, vf, vm, qn, qf, qm, kb, vb, qb, posm, cos_t, se_t, so_t, cos_m, se_m, so_m,
                mi, mt, g1, mine1, mine2, s0, s1, mx0, mx1, ost, otmp,
                xsem, wsem, msend, mrecv, gsend, grecv, ssem, rsem, fssem, frsem, ossem, orsem):
    tok, txt, d_in, heads, ck, mx = cfg
    nu = tok - mx
    hd_all = heads * HD
    nj = heads // NCHIP
    quad = 4
    wide = quad * HD
    half = tok * NCHIP
    me = lax.axis_index("cp")
    chip, core = me // 2, me % 2
    zh, cl = chip // quad, chip % quad
    sib = chip * 2 + (1 - core)
    mirror_chip = lax.rem(chip + quad, NCHIP)

    def dev(c):
        return {"cp": c * 2 + core}

    barrier = pltpu.get_barrier_semaphore()
    for r in range(1, NDEV):
        pl.semaphore_signal(barrier, inc=1, device_id={"cp": lax.rem(me + r, NDEV)}, device_id_type=MESH)
    load_x = pltpu.make_async_copy(x_hbm, xs, xsem.at[0])
    load_t = pltpu.make_async_copy(xt_hbm, xt, xsem.at[1])

    early = 16

    def x_copy(part):
        lo, n = ((0, early), (early, mx - early))[part]
        return pltpu.make_async_remote_copy(
            src_ref=x_hbm.at[pl.ds(nu + lo, n), :], dst_ref=xm.at[pl.ds(lo, n), :], send_sem=msend.at[2 * part],
            recv_sem=mrecv.at[2 * part], device_id=dev(mirror_chip), device_id_type=MESH)

    def pos_copy():
        return pltpu.make_async_remote_copy(
            src_ref=pos_ref.at[pl.ds(nu, mx), :], dst_ref=posm, send_sem=msend.at[1], recv_sem=mrecv.at[1],
            device_id=dev(mirror_chip), device_id_type=MESH)

    mc = 2 * d_in // NDEV

    def tile_copy(what, a, b, slot):
        if what == "mod":
            ref = (wmi_hbm, wmt_hbm)[a]
            off = me * mc if b < 0 else 2 * d_in + me * 2 * mc + b * mc
            return [pltpu.make_async_copy(ref.at[:, pl.ds(pl.multiple_of(off, 128), mc)], w.at[slot, :, pl.ds(0, mc)], wsem.at[slot, 0])]
        if what == "txt":
            return [pltpu.make_async_copy(
                wt_hbm.at[:, pl.ds(pl.multiple_of(a * hd_all + (j * NCHIP + chip) * HD, HD), HD)],
                w.at[slot, :, pl.ds(j * HD, HD)], wsem.at[slot, j]) for j in range(nj)]
        kind, side = a
        off = kind * hd_all + b * NCHIP * HD + (zh if side == 0 else 1 - zh) * wide
        return [pltpu.make_async_copy(wi_hbm.at[:, pl.ds(pl.multiple_of(off, wide), wide)], w.at[slot], wsem.at[slot, 0])]

    def start(*a):
        for c in tile_copy(*a):
            c.start()

    def wait(*a):
        for c in tile_copy(*a):
            c.wait()
        return a[-1]

    def start_own(j, p):
        start("img", (KINDS[p // 2], p % 2), j, (2 + p) % 3)

    def start_txt(t):
        start("txt", KINDS[t], None, (2 + t) % 3)

    def start_mir(j, i):
        start("img", (KINDS[i], 0), j, (2 + i) % 3)

    def start_mod2(t):
        start("mod", t // 2, t % 2, (2 + t) % 3)

    start("mod", 0, -1, 0)
    start("mod", 1, -1, 1)

    c = cond_ref[...].astype(F32)
    act = (c * jax.nn.sigmoid(c)).astype(BF16)
    act = jnp.broadcast_to(act, (16, d_in))
    per = mc // 128

    def mod_rows(slot, buf, row):
        r = dot(act, w[slot, :, 0:mc])
        for i in range(per):
            buf[row + i:row + i + 1, :] = r[0:1, i * 128:(i + 1) * 128]

    def spread(buf, dst, k):
        return [pltpu.make_async_remote_copy(
            src_ref=buf, dst_ref=dst.at[me], send_sem=gsend.at[k, r], recv_sem=grecv.at[k, r],
            device_id={"cp": lax.rem(me + r, NDEV)}, device_id_type=MESH) for r in range(1, NDEV)]

    mine1[...] = jnp.zeros_like(mine1)
    pl.semaphore_wait(barrier, NDEV - 1)
    x_copy(0).start()
    slot = wait("mod", 0, -1, 0)
    load_x.start()
    mod_rows(slot, mine1, 0)
    slot = wait("mod", 1, -1, 1)
    start_own(0, 0)
    start_own(0, 1)
    load_t.start()
    mod_rows(slot, mine1, per)
    gath1 = spread(mine1, g1, 0)
    for cp in gath1:
        cp.start()
    pos_copy().start()
    x_copy(1).start()
    g1[me] = mine1[...]

    def tables(pos, n, cos_t, se_t, so_t):
        ang = pos.astype(F32) * om_ref[...]
        odd = lax.rem(lax.broadcasted_iota(jnp.int32, ang.shape, 1), 2) == 1
        sin = jnp.sin(ang)
        cos_t[0:n, :] = jnp.cos(ang)
        se_t[0:n, :] = jnp.where(odd, 0.0, -sin)
        so_t[0:n, :] = jnp.where(odd, sin, 0.0)

    tables(pos_ref[...], tok, cos_t, se_t, so_t)
    for b_ref, m in ((bmi_ref, mi), (bmt_ref, mt)):
        for k in range(2):
            m[k:k + 1, :] = lane_row(b_ref, k * d_in, d_in)
    for cp in gath1:
        cp.wait()
    for b, m in ((0, mi), (1, mt)):
        for dv in range(NDEV):
            for r in range(per):
                col = (dv * per + r) * 128
                at = (slice(col // d_in, col // d_in + 1), slice(col % d_in, col % d_in + 128))
                m[at] = m[at] + g1[dv, b * per + r:b * per + r + 1, :]

    rb = 32

    def ln_rows(ref, m_ref, n):
        shift = m_ref[0:1, :]
        scale = 1.0 + m_ref[1:2, :]

        def body(i, carry):
            sl = pl.ds(pl.multiple_of(i * rb, rb), rb)
            ref[sl, :] = ln_mod_rows(ref[sl, :], scale, shift).astype(BF16)
            return carry
        lax.fori_loop(0, n // rb, body, 0)

    def norm_rope(y, gain, tabs):
        ms = jnp.mean(y * y, axis=-1, keepdims=True)
        y = y * lax.rsqrt(ms + EPS) * gain
        if tabs is not None:
            n = y.shape[0]
            y = y * tabs[0][0:n, :] + pltpu.roll(y, HD - 1, 1) * tabs[1][0:n, :] + pltpu.roll(y, 1, 1) * tabs[2][0:n, :]
        return y

    def place(kind, s_chip, row, n, j):
        if kind == 0:
            return qb.at[j, pl.ds(pl.multiple_of(txt + s_chip * tok + row, 128), n)]
        at = pl.multiple_of(txt + core * half + s_chip * tok + row, 128)
        return kb.at[j, pl.ds(at, n)] if kind == 1 else vb.at[j, :, pl.ds(at, n)]

    def qkv_copy(kind, ty, j, src_cl, src_zh, dst_cl, idx):
        buf = ((qn, qf, qm), (kn, kf, km), (vn, vf, vm))[kind][ty]
        n = (tok, nu, mx)[ty]
        s_chip = src_zh * quad + src_cl
        tgt = (1 - src_zh if ty == 1 else src_zh) * quad + dst_cl
        if ty == 2:
            dst = place(kind, lax.rem(s_chip + quad, NCHIP), nu, n, j)
        else:
            dst = place(kind, s_chip, 0, n, j)
        return pltpu.make_async_remote_copy(
            src_ref=buf.at[j * quad + dst_cl], dst_ref=dst, send_sem=ssem.at[kind, ty, j, idx[0]],
            recv_sem=rsem.at[kind, ty, j, idx[1]], device_id=dev(tgt), device_id_type=MESH)

    def out_copies(kind, ty, j):
        if ty == 1:
            return [qkv_copy(kind, 1, j, cl, zh, c, (c, cl)) for c in range(quad)]
        return [qkv_copy(kind, ty, j, cl, zh, lax.rem(cl + r, quad), (r, r)) for r in range(1, quad)]

    def in_copies(kind, ty, j):
        if ty == 1:
            return [qkv_copy(kind, 1, j, c, 1 - zh, cl, (c, c)) for c in range(quad)]
        return [qkv_copy(kind, ty, j, lax.rem(cl + quad - r, quad), zh, cl, (r, r)) for r in range(1, quad)]

    def own_copy(kind, ty, j):
        buf = ((qn, qf, qm), (kn, kf, km), (vn, vf, vm))[kind][ty]
        n = (tok, nu, mx)[ty]
        dst = place(kind, mirror_chip, nu, n, j) if ty == 2 else place(kind, chip, 0, n, j)
        dst[...] = buf[j * quad + cl]

    def make(kind, ty, j, slot):
        src = xm if ty == 2 else xs
        n = (tok, nu, mx)[ty]
        buf = ((qn, qf, qm), (kn, kf, km), (vn, vf, vm))[kind][ty]

        def cols(p, carry):
            col = pl.multiple_of(p * 2 * HD, 2 * HD)
            boff = kind * hd_all + j * NCHIP * HD + (1 - zh if ty == 1 else zh) * wide + col
            y2 = dot(src[0:n, :], w[slot, :, pl.ds(col, 2 * HD)]) + lane_row(bi_ref, pl.multiple_of(boff, 256), 2 * HD)
            for hh in range(2):
                y = y2[:, hh * HD:(hh + 1) * HD]
                if kind == 2:
                    buf[j * quad + 2 * p + hh] = y.T.astype(BF16)
                else:
                    gain = (qg_ref, kg_ref)[kind][...].astype(F32).reshape(1, HD)
                    buf[j * quad + 2 * p + hh] = norm_rope(y, gain, (cos_m, se_m, so_m) if ty == 2 else (cos_t, se_t, so_t)).astype(BF16)
            return carry
        lax.fori_loop(0, 2, cols, 0)

    load_x.wait()
    ln_rows(xs, mi, tok)

    last = nj - 1
    mir_after = 0

    def text_rows():
        load_t.wait()
        ln_rows(xt, mt, txt)
        for t, kind in enumerate(KINDS):
            if t == 0:
                start_txt(2)
            elif mir_after > 0:
                start_own(1, t - 1)
            else:
                start_mir(0, t - 1)
            slot = wait("txt", kind, None, (2 + t) % 3)
            y3 = dot(xt[...], w[slot, :, 0:nj * HD])
            for j in range(nj):
                pair0 = kind * hd_all + (j * NCHIP + chip - lax.rem(chip, 2)) * HD
                b2 = lane_row(bt_ref, pl.multiple_of(pair0, 256), 2 * HD)
                y = y3[:, j * HD:(j + 1) * HD] + jnp.where(lax.rem(chip, 2) == 0, b2[:, 0:HD], b2[:, HD:2 * HD])
                if kind == 2:
                    vb[j, :, 0:txt] = y.T.astype(BF16)
                else:
                    gain = (tqg_ref, tkg_ref)[kind][...].astype(F32).reshape(1, HD)
                    (qb, kb)[kind][j, 0:txt] = norm_rope(y, gain, None).astype(BF16)

    def mirror_rows():
        pos_copy().wait_recv()
        tables(posm[...], mx, cos_m, se_m, so_m)
        for part in range(2):
            x_copy(part).wait_recv()
        ln_rows(xm, mi, mx)

        lax.fori_loop(0, nj, mir_pass, 0)

    def mir_pass(j, carry):
        for i, kind in enumerate(KINDS):
            if i == 0:
                start_mir(j, 2)
            else:
                @pl.when(j < nj - 1)
                def _():
                    start_mir(j + 1, i - 1)

                @pl.when(j == nj - 1)
                def _():
                    if mir_after < last:
                        start_own(mir_after + 1, i - 1)
                    else:
                        start_mod2(i - 1)
            slot = wait("img", (kind, 0), j, (2 + i) % 3)
            make(kind, 2, j, slot)
            for cp in out_copies(kind, 2, j):
                cp.start()
            own_copy(kind, 2, j)
        return carry

    def after_own(j, p):
        @pl.when(j == 0)
        def _():
            start_txt(p)

        if mir_after > 0:
            @pl.when(j == mir_after)
            def _():
                start_mir(0, p)

        @pl.when((j > mir_after) & (j < last))
        def _():
            start_own(j + 1, p)

        if last > mir_after:
            @pl.when(j == last)
            def _():
                start_mod2(p)

    def own_pass(j, carry):
        for p in range(6):
            kind, side = KINDS[p // 2], p % 2
            if p + 2 < 6:
                start_own(j, p + 2)
            else:
                after_own(j, p - 4)
            slot = wait("img", (kind, side), j, (2 + p) % 3)
            make(kind, side, j, slot)
            for cp in out_copies(kind, side, j):
                cp.start()
            if side == 0:
                own_copy(kind, 0, j)

        pl.when(j == 0)(text_rows)
        pl.when(j == mir_after)(mirror_rows)
        return carry
    lax.fori_loop(0, nj, own_pass, 0)

    mine2[...] = jnp.zeros_like(mine2)
    for t in range(4):
        if t + 2 < 4:
            start_mod2(t + 2)
        mod_rows(wait("mod", t // 2, t % 2, (2 + t) % 3), mine2, t * per)
    gath2 = spread(mine2, g2, 1)
    for cp in gath2:
        cp.start()
    g2[me] = mine2[...]

    scale2 = (HD ** -0.5) * 1.4426950408889634
    keys = txt + 2 * half
    nchunk = keys // ck
    qt = 256
    ntile = (txt + half) // qt
    group = 2 * tok // qt

    def to_sibling(kind, j):
        ref = (kb.at[j, pl.ds(pl.multiple_of(txt + core * half, 128), half)] if kind == 1
               else vb.at[j, :, pl.ds(pl.multiple_of(txt + core * half, 128), half)])
        return pltpu.make_async_remote_copy(
            src_ref=ref, dst_ref=ref, send_sem=fssem.at[kind - 1, j], recv_sem=frsem.at[kind - 1, j],
            device_id={"cp": sib}, device_id_type=MESH)

    def collect(j):
        for kind in KINDS:
            for ty in range(3):
                for cp in in_copies(kind, ty, j):
                    cp.wait_recv()
            if kind != 0:
                to_sibling(kind, j).start()

    def plane_of(g):
        p = (chip // 2) % 2
        same = (g == 0) | (g == 3)
        return jnp.where(g < 2, 1 - zh, zh) * 2 + jnp.where(same, p, 1 - p)

    def tile_start(t):
        g = (t - 1) // group
        plane = plane_of(g)
        row = txt + plane * (2 * tok) + lax.rem(t - 1, group) * qt
        return pl.multiple_of(jnp.where(t == 0, 0, row), 128)

    def qk(j, q, i, s_ref, mxv):
        sl = pl.ds(pl.multiple_of(i * ck, ck), ck)
        s = dot_t(kb[j, sl], q)
        s_ref[sl, :] = s
        return jnp.maximum(mxv, jnp.max(s.reshape(ck // 8, 8, qt), axis=0))

    def sm(j, i, s_ref, m, lsum, acc):
        sl = pl.ds(pl.multiple_of(i * ck, ck), ck)
        p = jnp.exp2((s_ref[sl, :] - m) * scale2)
        lsum = lsum + jnp.sum(p.reshape(ck // 8, 8, qt), axis=0)
        acc = acc + dot(vb[j, :, sl], p.astype(BF16))
        return lsum, acc

    def new_max():
        return jnp.full((8, qt), -jnp.inf, F32)

    def o_remote(j, c_src, c_dst):
        src = ost.at[j, pl.ds(pl.multiple_of(c_dst * tok, 128), tok)]
        dst = o_hbm.at[:, pl.ds(pl.multiple_of((j * NCHIP + c_src) * HD, HD), HD)]
        return pltpu.make_async_remote_copy(
            src_ref=src, dst_ref=dst, send_sem=ossem.at[j, c_dst], recv_sem=orsem.at[j, c_src],
            device_id=dev(c_dst), device_id_type=MESH)

    def o_local(j):
        src = ost.at[j, pl.ds(pl.multiple_of(chip * tok, 128), tok)]
        dst = o_hbm.at[:, pl.ds(pl.multiple_of((j * NCHIP + chip) * HD, HD), HD)]
        return pltpu.make_async_copy(src, dst, ossem.at[j, chip])

    def o_send(j, g):
        plane = plane_of(g)
        for y in range(2):
            c = plane * 2 + y

            @pl.when(c != chip)
            def _():
                o_remote(j, chip, c).start()

            @pl.when(c == chip)
            def _():
                o_local(j).start()

    def finish(j, t, lsum, acc):
        tot = jnp.sum(lsum, axis=0, keepdims=True)
        o = (acc / tot).T.astype(BF16)

        @pl.when(t == 0)
        def _():
            otmp[...] = o
            ot_ref[j] = otmp[pl.ds(pl.multiple_of(core * (txt // 2), 8), txt // 2), :]

        @pl.when(t > 0)
        def _():
            ost[j, pl.ds(pl.multiple_of(tile_start(t) - txt, 128), qt)] = o

            @pl.when(lax.rem(t, group) == 0)
            def _():
                o_send(j, t // group - 1)

    def pair(j, t, s_cur, mx_cur, s_nxt, mx_nxt, has_next):
        m = jnp.max(mx_cur[...], axis=0, keepdims=True)
        lsum = jnp.zeros((8, qt), F32)
        acc = jnp.zeros((HD, qt), F32)
        if has_next:
            q = qb[j, pl.ds(tile_start(t + 1), qt)]

            def body(i, carry):
                lsum, acc, mxv = carry
                mxv = qk(j, q, i, s_nxt, mxv)
                lsum, acc = sm(j, i, s_cur, m, lsum, acc)
                return lsum, acc, mxv
            lsum, acc, mxv = lax.fori_loop(0, nchunk, body, (lsum, acc, new_max()))
            mx_nxt[...] = mxv
        else:
            def body(i, carry):
                return sm(j, i, s_cur, m, *carry)
            lsum, acc = lax.fori_loop(0, nchunk, body, (lsum, acc))
        finish(j, t, lsum, acc)

    collect(0)

    def head(j, carry):
        for kind in (1, 2):
            to_sibling(kind, j).wait()
        q = qb[j, 0:qt]

        def first(i, mxv):
            return qk(j, q, i, s0, mxv)
        mx0[...] = lax.fori_loop(0, nchunk, first, new_max())

        def two(i, carry):
            pair(j, 2 * i, s0, mx0, s1, mx1, True)
            pair(j, 2 * i + 1, s1, mx1, s0, mx0, True)
            return carry
        lax.fori_loop(0, (ntile - 1) // 2, two, 0)
        if nj > 1:
            @pl.when(j < nj - 1)
            def _():
                collect(j + 1)
        pair(j, jnp.int32(ntile - 1), s0, mx0, s1, mx1, False)
        return carry
    lax.fori_loop(0, nj, head, 0)

    for cp in gath2:
        cp.wait()
    for part in range(2):
        x_copy(part).wait_send()
    pos_copy().wait_send()

    def drain(j, carry):
        for kind in KINDS:
            for ty in range(3):
                for cp in out_copies(kind, ty, j):
                    cp.wait_send()
        o_local(j).wait()
        for r in range(1, NCHIP):
            c = lax.rem(chip + r, NCHIP)
            o_remote(j, chip, c).wait_send()
            o_remote(j, c, chip).wait_recv()
        return carry
    lax.fori_loop(0, nj, drain, 0)


def attention(image, text, cond_vec, wm_img, wm_txt, w_img, w_txt, flat, pos, omega):
    tok, d_in = image.shape
    txt = text.shape[0]
    hd_all = w_img.shape[1] // 3
    heads = hd_all // HD
    nj = heads // NCHIP
    half = tok * NCHIP
    keys = txt + 2 * half
    ck = 3200
    mx = tok // 3
    nu = tok - mx
    cfg = (tok, txt, d_in, heads, ck, mx)
    dma = pltpu.SemaphoreType.DMA
    flops = 2 * tok * d_in * 3 * hd_all + 4 * nj * HD * (half + txt) * keys
    per = 2 * d_in // NDEV // 128
    r1, r2 = -(-2 * per // 8) * 8, -(-4 * per // 8) * 8
    row_sets = [pltpu.VMEM((nj * 4, n, HD), BF16) for n in (tok, nu, mx)]
    col_sets = [pltpu.VMEM((nj * 4, HD, n), BF16) for n in (tok, nu, mx)]
    table = pltpu.VMEM((tok, 128), F32)
    return pl.pallas_call(
        functools.partial(main_kernel, cfg),
        out_shape=(jax.ShapeDtypeStruct((tok, hd_all), BF16), jax.ShapeDtypeStruct((nj, txt // 2, HD), BF16),
                   jax.ShapeDtypeStruct((NDEV, r2, 128), F32)),
        in_specs=[ANY, ANY, VM, ANY, ANY, ANY, ANY] + [VM] * 10,
        out_specs=(ANY, VM, VM),
        scratch_shapes=[
            pltpu.VMEM((3, d_in, 4 * HD), BF16),
            pltpu.VMEM((tok, d_in), BF16), pltpu.VMEM((mx, d_in), BF16), pltpu.VMEM((txt, d_in), BF16),
            *row_sets, *col_sets, *row_sets,
            pltpu.VMEM((nj, keys, HD), BF16), pltpu.VMEM((nj, HD, keys), BF16), pltpu.VMEM((nj, txt + half, HD), BF16),
            pltpu.VMEM((mx, 128), BF16), table, table, table, *[pltpu.VMEM((mx, 128), F32)] * 3,
            pltpu.VMEM((2, d_in), F32), pltpu.VMEM((2, d_in), F32),
            pltpu.VMEM((NDEV, r1, 128), F32), pltpu.VMEM((r1, 128), F32), pltpu.VMEM((r2, 128), F32),
            pltpu.VMEM((keys, 256), F32), pltpu.VMEM((keys, 256), F32), pltpu.VMEM((8, 256), F32), pltpu.VMEM((8, 256), F32),
            pltpu.VMEM((nj, half, HD), BF16), pltpu.VMEM((txt, HD), BF16),
            dma((2,)), dma((3, max(nj, 1))), dma((3,)), dma((3,)), dma((2, NDEV)), dma((2, NDEV)),
            dma((3, 3, nj, 4)), dma((3, 3, nj, 4)), dma((2, nj)), dma((2, nj)), dma((nj, NCHIP)), dma((nj, NCHIP)),
        ],
        compiler_params=pltpu.CompilerParams(collective_id=1, has_side_effects=True, vmem_limit_bytes=VMEM_LIMIT),
        cost_estimate=pl.CostEstimate(flops=flops, bytes_accessed=3 * d_in * 3 * hd_all, transcendentals=0),
        name="attn",
    )(image, text, cond_vec, wm_img, wm_txt, w_img, w_txt, *flat, pos, omega)


def gelu(x):
    return x * (0.5 * (1.0 + jnp.tanh(0.7978845608028654 * (x + 0.044715 * (x * x * x)))))


def out_kernel(cfg, o_hbm, x_hbm, xt_hbm, ot_ref, g2_ref, bmi_ref, bmt_ref, bp_ref, tbp_ref, b1_ref, tb1_ref, b2_ref, tb2_ref, wp_hbm, w1_hbm, w2_hbm, twp_hbm, tw1_hbm, tw2_hbm,
               out_ref, tout_ref, mi_ref, mt_ref,
               wa, wb, wc, o, x, h, z, acc, a0, a1, o_t, x_t, h_t, z_t, a_t, part, rs, row,
               asem, bsem, csem, lsem, ossem, orsem, pssem, prsem, rssem, rrsem, fssem, frsem):
    tok, txt, d, ff, k1, k2 = cfg
    me = lax.axis_index("cp")
    chip, core = me // 2, me % 2
    sib = chip * 2 + (1 - core)
    rows = txt // 2
    quad = 4
    cl, zq = chip % quad, chip // quad * quad
    piece = rows // quad
    nb = wa.shape[2]
    na = wa.shape[0]
    np_ = d // nb
    nf = ff // nb
    ft = ff // quad
    nt = ft // nb
    nj = ot_ref.shape[0]

    def dev(c):
        return {"cp": c * 2 + core}

    off = pl.multiple_of(cl * ft, nb)

    def start_a(p):
        slot = lax.rem(p, na)

        @pl.when(p < np_)
        def _():
            pltpu.make_async_copy(wp_hbm.at[:, pl.ds(pl.multiple_of(p * nb, nb), nb)], wa.at[slot], asem.at[slot]).start()

        @pl.when((p >= np_) & (p < np_ + nf))
        def _():
            pltpu.make_async_copy(w1_hbm.at[:, pl.ds(pl.multiple_of((p - np_) * nb, nb), nb)], wa.at[slot], asem.at[slot]).start()

    def start_b(p):
        slot = lax.rem(p, na)

        @pl.when(p < nf)
        def _():
            pltpu.make_async_copy(w2_hbm.at[pl.ds(pl.multiple_of(p * nb, nb), nb), :], wb.at[slot], bsem.at[slot]).start()

    def c_fc2(p, slot):
        return pltpu.make_async_copy(tw2_hbm.at[pl.ds(off, ft), pl.ds(pl.multiple_of(p * nb, nb), nb)],
                                     wc.at[slot, pl.ds(0, ft), :], csem.at[slot])

    def start_c(p):
        slot = lax.rem(p, na)

        @pl.when(p < np_)
        def _():
            pltpu.make_async_copy(twp_hbm.at[:, pl.ds(pl.multiple_of(p * nb, nb), nb)], wc.at[slot], csem.at[slot]).start()

        @pl.when((p >= np_) & (p < np_ + nt))
        def _():
            pltpu.make_async_copy(tw1_hbm.at[:, pl.ds(pl.multiple_of(off + (p - np_) * nb, nb), nb)], wc.at[slot], csem.at[slot]).start()

        @pl.when((p >= np_ + nt) & (p < np_ + nt + np_))
        def _():
            c_fc2(p - np_ - nt, slot).start()

    def get_a(p):
        start_a(p + na - 1)
        slot = lax.rem(p, na)
        pltpu.make_async_copy(w1_hbm.at[:, 0:nb], wa.at[slot], asem.at[slot]).wait()
        return slot

    def get_b(p):
        start_b(p + na - 1)
        slot = lax.rem(p, na)
        pltpu.make_async_copy(w2_hbm.at[0:nb, :], wb.at[slot], bsem.at[slot]).wait()
        return slot

    def get_c(p, fc2=False):
        start_c(p + na - 1)
        slot = lax.rem(p, na)
        if fc2:
            c_fc2(0, slot).wait()
        else:
            pltpu.make_async_copy(w1_hbm.at[:, 0:nb], wc.at[slot], csem.at[slot]).wait()
        return slot

    load_o = pltpu.make_async_copy(o_hbm, o, lsem.at[0])
    load_x = pltpu.make_async_copy(x_hbm, x, lsem.at[1])
    load_t = pltpu.make_async_copy(xt_hbm.at[pl.ds(pl.multiple_of(core * rows, 8), rows), :], x_t, lsem.at[2])
    load_o.start()
    start_a(jnp.int32(0))
    load_x.start()
    for p in range(1, na - 1):
        start_a(jnp.int32(p))

    barrier = pltpu.get_barrier_semaphore()
    for r in range(1, NCHIP):
        pl.semaphore_signal(barrier, inc=1, device_id=dev(lax.rem(chip + r, NCHIP)), device_id_type=MESH)
    pl.semaphore_signal(barrier, inc=1, device_id={"cp": sib}, device_id_type=MESH)
    pl.semaphore_wait(barrier, NCHIP)

    def o_copy(j, r, c_src, c_dst):
        return pltpu.make_async_remote_copy(
            src_ref=ot_ref.at[j], dst_ref=o_t.at[:, pl.ds(pl.multiple_of((j * NCHIP + c_src) * HD, HD), HD)],
            send_sem=ossem.at[j, r], recv_sem=orsem.at[j, r], device_id=dev(c_dst), device_id_type=MESH)

    for j in range(nj):
        for r in range(1, NCHIP):
            o_copy(j, r, chip, lax.rem(chip + r, NCHIP)).start()
        o_t[:, pl.ds(pl.multiple_of((j * NCHIP + chip) * HD, HD), HD)] = ot_ref[j]

    per = 4 * d // NDEV // 128
    for b, (b_ref, m) in enumerate(((bmi_ref, mi_ref), (bmt_ref, mt_ref))):
        for k in range(2, 6):
            m[k:k + 1, :] = lane_row(b_ref, k * d, d)
        for dv in range(NDEV):
            for r in range(per):
                col = 2 * d + (dv * per + r) * 128
                at = (slice(col // d, col // d + 1), slice(col % d, col % d + 128))
                m[at] = m[at] + g2_ref[dv, b * per + r:b * per + r + 1, :]

    load_o.wait()
    load_x.wait()

    def proj(p, carry):
        slot = get_a(p)
        sl = pl.ds(pl.multiple_of(p * nb, nb), nb)

        @pl.when(p == 0)
        def _():
            load_t.start()

        @pl.when((p > 0) & (p < na))
        def _():
            start_b(p - 1)

        @pl.when((p >= na) & (p < 2 * na - 1))
        def _():
            start_c(p - na)
        y = dot(o[...], wa[slot]) + lane_row(bp_ref, pl.multiple_of(p * nb, nb), nb)
        h[:, sl] = x[:, sl].astype(F32) + mi_ref[2:3, sl] * y
        acc[:, sl] = jnp.broadcast_to(lane_row(b2_ref, pl.multiple_of(p * nb, nb), nb), (tok, nb))
        return carry
    lax.fori_loop(0, np_, proj, 0)

    def ln2(src, dst, m_ref, n):
        shift, scale = m_ref[3:4, :], 1.0 + m_ref[4:5, :]
        rb = 32

        def body(i, carry):
            r = pl.ds(pl.multiple_of(i * rb, rb), rb)
            dst[r, :] = ln_mod_rows(src[r, :], scale, shift).astype(BF16)
            return carry
        lax.fori_loop(0, n // rb, body, 0)

    ln2(h, z, mi_ref, tok)

    def tproj(p, carry):
        slot = get_c(p)
        sl = pl.ds(pl.multiple_of(p * nb, nb), nb)
        y = dot(o_t[...], wc[slot]) + lane_row(tbp_ref, pl.multiple_of(p * nb, nb), nb)
        h_t[:, sl] = x_t[:, sl].astype(F32) + mt_ref[2:3, sl] * y
        return carry

    def tfc1(p, carry):
        slot = get_c(np_ + p)
        col = pl.multiple_of(p * nb, nb)
        y = dot(z_t[...], wc[slot]) + lane_row(tb1_ref, pl.multiple_of(off + col, nb), nb)
        a_t[:, pl.ds(col, nb)] = gelu(y).astype(BF16)
        return carry

    def tfc2(p, carry):
        slot = get_c(np_ + nt + p, True)
        part[:, pl.ds(pl.multiple_of(p * nb, nb), nb)] = dot(a_t[...], wc[slot, 0:ft, :])
        return carry

    def p_copy(r, c_src, c_dst):
        return pltpu.make_async_remote_copy(
            src_ref=part.at[pl.ds(pl.multiple_of(c_dst * piece, 8), piece), :], dst_ref=rs.at[c_src],
            send_sem=pssem.at[r], recv_sem=prsem.at[r], device_id=dev(zq + c_dst), device_id_type=MESH)

    def r_copy(r, c_src, c_dst):
        return pltpu.make_async_remote_copy(
            src_ref=row, dst_ref=tout_ref.at[pl.ds(pl.multiple_of(core * rows + c_src * piece, 8), piece), :],
            send_sem=rssem.at[r], recv_sem=rrsem.at[r], device_id=dev(zq + c_dst), device_id_type=MESH)

    mine = pl.ds(pl.multiple_of(cl * piece, 8), piece)
    n1, n2, n3 = np_ // 2, np_ // 2 + nt // 2, np_ + nt // 2

    def text_step(s):
        @pl.when(s == 0)
        def _():
            load_t.wait()
            for j in range(nj):
                for r in range(1, NCHIP):
                    o_copy(j, r, lax.rem(chip + NCHIP - r, NCHIP), chip).wait_recv()

        @pl.when((s >= 0) & (s < n1))
        def _():
            lax.fori_loop(2 * s, 2 * s + 2, tproj, 0)

        @pl.when(s == n1)
        def _():
            ln2(h_t, z_t, mt_ref, rows)

        @pl.when((s >= n1) & (s < n2))
        def _():
            lax.fori_loop(2 * (s - n1), 2 * (s - n1) + 2, tfc1, 0)

        @pl.when((s >= n2) & (s < n3))
        def _():
            lax.fori_loop(2 * (s - n2), 2 * (s - n2) + 2, tfc2, 0)

        @pl.when(s == n3 - 1)
        def _():
            for r in range(1, quad):
                p_copy(r, cl, lax.rem(cl + r, quad)).start()
            rs[cl] = part[mine, :]

        @pl.when(s == k2)
        def _():
            for r in range(1, quad):
                p_copy(r, lax.rem(cl + quad - r, quad), cl).wait_recv()
            tot = rs[0]
            for c in range(1, quad):
                tot = tot + rs[c]
            y = h_t[mine, :] + mt_ref[5:6, :] * (tot + lane_row(tb2_ref, 0, d))
            row[...] = y.astype(BF16)
            for r in range(1, quad):
                r_copy(r, cl, lax.rem(cl + r, quad)).start()
            tout_ref[pl.ds(pl.multiple_of(core * rows + cl * piece, 8), piece), :] = row[...]

    def mlp(i, a_new, a_old):
        slot_b = get_b(i - 1)
        slot_a = get_a(np_ + i)
        hn, hd = nb // 2, d // 2
        for s in range(2):
            c1, c2 = slice(s * hn, (s + 1) * hn), slice(s * hd, (s + 1) * hd)
            b1 = lane_row(b1_ref, pl.multiple_of(i * nb + s * hn, hn), hn)
            a_new[:, c1] = gelu(dot(z[...], wa[slot_a, :, c1]) + b1).astype(BF16)
            acc[:, c2] += dot(a_old[...], wb[slot_b, :, c2])

    slot = get_a(jnp.int32(np_))
    a0[...] = gelu(dot(z[...], wa[slot]) + lane_row(b1_ref, 0, nb)).astype(BF16)

    def two(k, carry):
        mlp(2 * k + 1, a1, a0)
        text_step(2 * k - k1)
        mlp(2 * k + 2, a0, a1)
        text_step(2 * k + 1 - k1)
        return carry
    lax.fori_loop(0, nf // 2 - 1, two, 0)
    mlp(jnp.int32(nf - 1), a1, a0)

    for r in range(1, quad):
        r_copy(r, lax.rem(cl + quad - r, quad), cl).wait_recv()
    ref = tout_ref.at[pl.ds(pl.multiple_of(core * rows, 8), rows), :]
    fwd = pltpu.make_async_remote_copy(src_ref=ref, dst_ref=ref, send_sem=fssem, recv_sem=frsem,
                                       device_id={"cp": sib}, device_id_type=MESH)
    fwd.start()

    slot = get_b(jnp.int32(nf - 1))
    y = acc[...] + dot(a1[...], wb[slot])
    out_ref[...] = (h[...] + mi_ref[5:6, :] * y).astype(BF16)

    fwd.wait()
    for j in range(nj):
        for r in range(1, NCHIP):
            o_copy(j, r, chip, lax.rem(chip + r, NCHIP)).wait_send()
    for r in range(1, quad):
        c = lax.rem(cl + r, quad)
        p_copy(r, cl, c).wait_send()
        r_copy(r, cl, c).wait_send()


def output(o_img, image, text, o_txt, g2, flat, wp, w1, w2, twp, tw1, tw2):
    tok, d = image.shape
    txt = text.shape[0]
    ff = w1.shape[1]
    nb = 512
    nf = ff // nb
    k1, k2 = (2, 16) if nf > 8 else (0, 5)
    na = 3
    rows = txt // 2
    ft = ff // 4
    nj = o_txt.shape[0]
    dma = pltpu.SemaphoreType.DMA
    flops = 2 * tok * d * (d + 2 * ff) + 2 * rows * d * (d + 2 * ft)
    return pl.pallas_call(
        functools.partial(out_kernel, (tok, txt, d, ff, k1, k2)),
        out_shape=(jax.ShapeDtypeStruct((tok, d), BF16), jax.ShapeDtypeStruct((txt, d), BF16)),
        in_specs=[ANY, ANY, ANY, VM, VM] + [VM] * 8 + [ANY] * 6,
        out_specs=(VM, VM),
        scratch_shapes=[
            pltpu.VMEM((6, d), F32), pltpu.VMEM((6, d), F32),
            pltpu.VMEM((na, d, nb), BF16), pltpu.VMEM((na, nb, d), BF16), pltpu.VMEM((na, d, nb), BF16),
            pltpu.VMEM((tok, d), BF16), pltpu.VMEM((tok, d), BF16), pltpu.VMEM((tok, d), F32), pltpu.VMEM((tok, d), BF16),
            pltpu.VMEM((tok, d), F32), pltpu.VMEM((tok, nb), BF16), pltpu.VMEM((tok, nb), BF16),
            pltpu.VMEM((rows, d), BF16), pltpu.VMEM((rows, d), BF16), pltpu.VMEM((rows, d), F32), pltpu.VMEM((rows, d), BF16),
            pltpu.VMEM((rows, ft), BF16), pltpu.VMEM((rows, d), F32), pltpu.VMEM((4, rows // 4, d), F32),
            pltpu.VMEM((rows // 4, d), BF16),
            dma((na,)), dma((na,)), dma((na,)), dma((3,)), dma((nj, NCHIP)), dma((nj, NCHIP)), dma((NCHIP,)), dma((NCHIP,)),
            dma((NCHIP,)), dma((NCHIP,)), dma, dma,
        ],
        compiler_params=pltpu.CompilerParams(collective_id=2, has_side_effects=True, vmem_limit_bytes=VMEM_LIMIT),
        cost_estimate=pl.CostEstimate(flops=flops, bytes_accessed=2 * d * (d + 2 * ff), transcendentals=0),
        name="out",
    )(o_img, image, text, o_txt, g2, *flat, wp, w1, w2, twp, tw1, tw2)


def pass_kernel(parts, a_hbm, b_hbm, oa_hbm, ob_hbm, a, b, isem, osem):
    moves = []
    for k, (src, dst, buf) in enumerate(((a_hbm, oa_hbm, a), (b_hbm, ob_hbm, b))):
        n = src.shape[0] // parts
        for i in range(parts):
            sl = pl.ds(i * n, n)
            moves.append((pltpu.make_async_copy(src.at[sl, :], buf.at[sl, :], isem.at[k, i]),
                          pltpu.make_async_copy(buf.at[sl, :], dst.at[sl, :], osem.at[k, i])))
    for load, _ in moves:
        load.start()
    for load, store in moves:
        load.wait()
        store.start()
    for _, store in moves:
        store.wait()


def pass_results(a, b):
    parts = 4
    dma = pltpu.SemaphoreType.DMA
    return pl.pallas_call(
        functools.partial(pass_kernel, parts),
        out_shape=(jax.ShapeDtypeStruct(a.shape, a.dtype), jax.ShapeDtypeStruct(b.shape, b.dtype)),
        in_specs=[ANY, ANY],
        out_specs=(ANY, ANY),
        scratch_shapes=[pltpu.VMEM(a.shape, a.dtype), pltpu.VMEM(b.shape, b.dtype), dma((2, parts)), dma((2, parts))],
        compiler_params=pltpu.CompilerParams(vmem_limit_bytes=VMEM_LIMIT),
        name="results",
    )(a, b)


def rope_inputs(ids):
    d_t = HD // 8
    d_s = (HD - d_t) // 2
    widths = (d_t, d_s, d_s)
    lane = lax.broadcasted_iota(jnp.int32, (1, HD), 1)
    pos = jnp.where(lane < d_t, ids[:, 0:1], jnp.where(lane < d_t + d_s, ids[:, 1:2], ids[:, 2:3])).astype(BF16)
    omega = np.concatenate([np.repeat(THETA ** (-np.arange(0, w, 2, dtype=np.float32) / np.float32(w)), 2) for w in widths])
    return pos, jnp.asarray(omega.astype(np.float32)[None, :])


def device_fn(image, text, cond_vec, image_ids, *weights):
    (wm, bm, wqkv, bqkv, qg, kg, wp, bp, w1, b1, w2, b2) = weights[:12]
    (twm, tbm, twqkv, tbqkv, tqg, tkg, twp, tbp, tw1, tb1, tw2, tb2) = weights[12:]
    x, xt = image[0], text[0]
    pos, omega = rope_inputs(image_ids)
    o_img, o_txt, g2 = attention(x, xt, cond_vec, wm, twm, wqkv, twqkv, (bm, tbm, bqkv, tbqkv, qg, kg, tqg, tkg), pos, omega)
    image_out, text_out = output(o_img, x, xt, o_txt, g2, (bm, tbm, bp, tbp, b1, tb1, b2, tb2), wp, w1, w2, twp, tw1, tw2)
    image_out, text_out = pass_results(image_out, text_out)
    return image_out[None], text_out[None]


def solution(mesh):
    act = P("dp", "cp", None)
    txt = P("dp", None, None)
    in_specs = (act, txt, P("dp", None), P(("dp", "cp"), None)) + (P(),) * 24
    return jax.shard_map(device_fn, mesh=mesh, in_specs=in_specs, out_specs=(act, txt), check_vma=False)
```
